16 devices in a mesh: dp: 2 (over z), tp: 8 (over y, x, core).
Axes of the slice: x: 2, y: 2, z: 2, core: 2. Of those that a mesh axis runs over, the one named last changes fastest.
Arguments:
- x_norm: bfloat16 [2048, 4096], P(('dp', 'tp')), parts along dimension 0
- w_gate: bfloat16 [4096, 11008], P(None, 'tp')
- w_up: bfloat16 [4096, 11008], P(None, 'tp')
- w_down: bfloat16 [11008, 4096], P('tp')
- u_gate: bfloat16 [2048, 11008], P('dp', 'tp'), parts along dimension 0
- u_up: bfloat16 [2048, 11008], P('dp', 'tp'), parts along dimension 0
- grad_out: bfloat16 [2048, 4096], P(('dp', 'tp')), parts along dimension 0
Outputs:
- output 1: bfloat16 [2048, 4096], P(('dp', 'tp')), parts along dimension 0
- output 2: float32 [8192, 11008], P('dp', 'tp'), parts along dimension 0
- output 3: float32 [8192, 11008], P('dp', 'tp'), parts along dimension 0
- output 4: float32 [22016, 4096], P(('dp', 'tp')), parts along dimension 0
There are 2 independent parts. The reference program is written for one: setup_inputs(seed, part) draws one part's arguments, and reference() takes and returns one part's arrays. A program takes and returns all parts, laid end to end along the dimension named above; an argument that names none is the same for every part.
All inputs are finite; a program needn't handle non-finite values.
Results may differ from the reference program's by a relative error of at most 0.0116485.
Values are sent between devices in bfloat16 or wider.
A program may use at most 1 GiB of HBM per device.

```python
import jax
import jax.numpy as jnp

TOKENS = 1024
HIDDEN = 4096
FFN_DIM = 11008


def setup_inputs(seed: int = 0, part: int = 0) -> dict:
    shared_keys = jax.random.split(jax.random.key(seed + 1), 3)
    own_keys = jax.random.split(jax.random.fold_in(jax.random.key(seed), part), 4)
    x_norm = jax.random.normal(own_keys[0], (TOKENS, HIDDEN), jnp.float32)
    w_gate = jax.random.normal(shared_keys[0], (HIDDEN, FFN_DIM), jnp.float32) * HIDDEN ** -0.5
    w_up = jax.random.normal(shared_keys[1], (HIDDEN, FFN_DIM), jnp.float32) * HIDDEN ** -0.5
    w_down = jax.random.normal(shared_keys[2], (FFN_DIM, HIDDEN), jnp.float32) * FFN_DIM ** -0.5
    u_gate = jax.random.normal(own_keys[1], (TOKENS, FFN_DIM), jnp.float32)
    u_up = jax.random.normal(own_keys[2], (TOKENS, FFN_DIM), jnp.float32)
    grad_out = jax.random.normal(own_keys[3], (TOKENS, HIDDEN), jnp.float32)
    return {
        'x_norm': x_norm.astype(jnp.bfloat16),
        'w_gate': w_gate.astype(jnp.bfloat16),
        'w_up': w_up.astype(jnp.bfloat16),
        'w_down': w_down.astype(jnp.bfloat16),
        'u_gate': u_gate.astype(jnp.bfloat16),
        'u_up': u_up.astype(jnp.bfloat16),
        'grad_out': grad_out.astype(jnp.bfloat16),
    }


def reference(x_norm, w_gate, w_up, w_down, u_gate, u_up, grad_out):
    gate_pre = u_gate.astype(jnp.float32)
    up_pre = u_up.astype(jnp.float32)
    sig_gate = jax.nn.sigmoid(gate_pre)
    gate_act = gate_pre * sig_gate
    z_act = (gate_act * up_pre).astype(jnp.bfloat16)
    grad_down = jnp.dot(z_act.T, grad_out, preferred_element_type=jnp.float32)
    grad_hid = jnp.dot(grad_out, w_down.T, preferred_element_type=jnp.float32)
    grad_up = (grad_hid * gate_act).astype(jnp.bfloat16)
    silu_prime = sig_gate * (1.0 + gate_pre * (1.0 - sig_gate))
    grad_gate = (grad_hid * up_pre * silu_prime).astype(jnp.bfloat16)
    grad_x = (jnp.dot(grad_gate, w_gate.T, preferred_element_type=jnp.float32)
              + jnp.dot(grad_up, w_up.T, preferred_element_type=jnp.float32)).astype(jnp.bfloat16)
    grad_wg = jnp.dot(x_norm.T, grad_gate, preferred_element_type=jnp.float32)
    grad_wu = jnp.dot(x_norm.T, grad_up, preferred_element_type=jnp.float32)
    return (grad_x, grad_wg, grad_wu, grad_down)
```

```python
import functools

import jax
import jax.numpy as jnp
from jax import lax
from jax.experimental import pallas as pl
from jax.experimental.pallas import tpu as pltpu
from jax.sharding import PartitionSpec as P

MESH = pl.DeviceIdType.MESH
BF16 = jnp.bfloat16
F32 = jnp.float32
NH = 8
NT = (((1,), (1,)), ((), ()))


def _lanes(n):
    return (n + 127) // 128 * 128


def _comm_kernel(x_ref, dy_ref, wd_ref, wg_ref, wu_ref, ug_ref, uu_ref,
                 dx_ref, zt_ref, dgt_ref, dut_ref, dya_ref, xa_ref,
                 dyv, gv, av, spv, utv, duv, wbuf, ugv, uuv, r0v, r1v, r2v, dxv, xov,
                 ys, yr, xs, xr, rs, rr, yl, xl, wl, ul, ol, dl):
    tok, hid = dy_ref.shape
    ff = wd_ref.shape[0]
    fp = _lanes(ff)
    nfull, rest = ff // 128, ff % 128
    hc = hid // NH
    tall = 8 * tok

    t = lax.axis_index("tp")
    ty, tx, tc = t // 4, (t // 2) % 2, t % 2
    tq = t // 2
    xn = t + 2 - 4 * tx
    yn = t + 4 - 8 * ty
    dg = xn + yn - t
    pn = t + 1 - 2 * tc

    def n1(k):
        return xn + (yn - xn) * (k % 2)

    def n2(k):
        return yn + (xn - yn) * (k % 2)

    def cols(k):
        return pl.ds(pl.multiple_of(k * hc, hc), hc)

    def blk(ref, owner, k):
        return ref.at[owner // 2, owner % 2, :, cols(k)]

    def rcopy(src, dst, ss, rs_, dev):
        return pltpu.make_async_remote_copy(src_ref=src, dst_ref=dst, send_sem=ss, recv_sem=rs_,
                                            device_id={"tp": dev}, device_id_type=MESH)

    def ag(buf, ss, sr, k, j, owner, dev):
        return rcopy(blk(buf, owner, k), blk(buf, owner, k), ss.at[k, j], sr.at[k, j], dev)

    def ag_own(buf, ss, sr, k):
        ag(buf, ss, sr, k, 0, t, n1(k)).start()
        ag(buf, ss, sr, k, 1, t, n2(k)).start()
        ag(buf, ss, sr, k, 3, t, pn).start()

    def ag_mid(buf, ss, sr, k):
        ag(buf, ss, sr, k, 0, n1(k), n1(k)).wait_recv()
        ag(buf, ss, sr, k, 2, n1(k), n2(k)).start()
        ag(buf, ss, sr, k, 4, n1(k), pn).start()

    def ag_last(buf, ss, sr, k):
        ag(buf, ss, sr, k, 1, n2(k), n2(k)).wait_recv()
        ag(buf, ss, sr, k, 5, n2(k), pn).start()
        ag(buf, ss, sr, k, 2, dg, n2(k)).wait_recv()
        ag(buf, ss, sr, k, 6, dg, pn).start()

    def ag_end(buf, ss, sr, k):
        pc = 1 - 2 * tc
        ag(buf, ss, sr, k, 3, t + pc, pn).wait_recv()
        ag(buf, ss, sr, k, 4, n1(k) + pc, pn).wait_recv()
        ag(buf, ss, sr, k, 5, n2(k) + pc, pn).wait_recv()
        ag(buf, ss, sr, k, 6, dg + pc, pn).wait_recv()

    def ag_sent(buf, ss, sr, k):
        ag(buf, ss, sr, k, 0, t, n1(k)).wait_send()
        ag(buf, ss, sr, k, 1, t, n2(k)).wait_send()
        ag(buf, ss, sr, k, 2, n1(k), n2(k)).wait_send()
        ag(buf, ss, sr, k, 3, t, pn).wait_send()
        ag(buf, ss, sr, k, 4, n1(k), pn).wait_send()
        ag(buf, ss, sr, k, 5, n2(k), pn).wait_send()
        ag(buf, ss, sr, k, 6, dg, pn).wait_send()

    def y_local(k):
        return pltpu.make_async_copy(dy_ref.at[:, cols(k)], blk(dyv, t, k), yl.at[k])

    def x_local(k):
        return pltpu.make_async_copy(x_ref.at[:, cols(k)], xov.at[:, cols(k)], xl.at[k])

    def x_put(k):
        return pltpu.make_async_copy(xov.at[:, cols(k)], blk(xa_ref, t, k), xl.at[k])

    def wd_load(k):
        return pltpu.make_async_copy(wd_ref.at[:, cols(k)], wbuf.at[0, k % 2, pl.ds(0, ff), :], wl.at[0, k % 2])

    def w_load(k, j):
        src = (wg_ref, wu_ref)[j]
        return pltpu.make_async_copy(src.at[:, cols(k)], wbuf.at[(k + 1) % 2, j, pl.ds(0, ff), :],
                                     wl.at[(k + 1) % 2, j])

    def dy_out(k):
        return pltpu.make_async_copy(dyv.at[:, :, :, cols(k)], dya_ref.at[:, :, :, cols(k)], dl.at[k])

    ug_in = pltpu.make_async_copy(ug_ref, ugv, ul.at[0])
    uu_in = pltpu.make_async_copy(uu_ref, uuv, ul.at[1])
    for k in range(NH):
        y_local(k).start()
    wd_load(0).start()
    wd_load(1).start()
    ug_in.start()
    uu_in.start()
    for k in range(NH):
        x_local(k).start()

    barrier = pltpu.get_barrier_semaphore()
    for dev in (xn, yn, pn):
        pl.semaphore_signal(barrier, inc=1, device_id={"tp": dev}, device_id_type=MESH)
    pl.semaphore_wait(barrier, 3)

    for k in range(2):
        y_local(k).wait()
        ag_own(dyv, ys, yr, k)

    for a in range(2):
        for b in range(2):
            wbuf[a, b, ff:, :] = jnp.zeros((fp - ff, hc), BF16)
    gv[...] = jnp.zeros_like(gv)
    ug_in.wait()
    uu_in.wait()

    def u_block(r0, n):
        rows = pl.ds(r0, n)
        ug = ugv[rows, :].astype(F32)
        ub = uuv[rows, :]
        uu = ub.astype(F32)
        s = jax.nn.sigmoid(ug)
        a = ug * s
        sp = s * (1.0 + ug * (1.0 - s))
        ugv[rows, :] = (a * uu).astype(BF16)
        if n < 128:
            pad = jnp.zeros((128 - n, tall), F32)
            a = jnp.concatenate([a, pad], axis=0)
            sp = jnp.concatenate([sp, pad], axis=0)
            uu = jnp.concatenate([uu, pad], axis=0)
        lanes = pl.ds(r0, 128)
        av[:, lanes] = a.T
        spv[:, lanes] = sp.T
        utv[:, lanes] = uu.T.astype(BF16)

    def phase1(i, carry):
        @pl.when(i < NH - 2)
        def _():
            y_local(i + 2).wait()
            ag_own(dyv, ys, yr, i + 2)

        @pl.when(i < NH)
        def _():
            ag_mid(dyv, ys, yr, i)

        @pl.when(i < nfull)
        def _():
            u_block(pl.multiple_of(i * 128, 128), 128)

        @pl.when((i >= 1) & (i <= NH))
        def _():
            ag_last(dyv, ys, yr, i - 1)

        @pl.when(i >= 2)
        def _():
            k = i - 2
            ag_end(dyv, ys, yr, k)
            dy_out(k).start()
            wd_load(k).wait()
            dyc = dyv[:, :, :, cols(k)].reshape(tall, hc)
            for n in range(0, fp, 256):
                w = min(256, fp - n)
                gv[:, n:n + w] += lax.dot_general(dyc, wbuf[0, k % 2, n:n + w, :], NT, preferred_element_type=F32)

            @pl.when(k + 2 < NH)
            def _():
                wd_load(k + 2).start()

        return carry

    w_load(0, 0).start()
    w_load(0, 1).start()
    lax.fori_loop(0, NH + 2, phase1, 0)
    w_load(1, 0).start()
    w_load(1, 1).start()
    for k in range(NH):
        x_local(k).wait()
        x_put(k).start()
    if rest:
        u_block(nfull * 128, rest)
    zt_out = pltpu.make_async_copy(ugv, zt_ref, ol.at[0])
    zt_out.start()
    for k in range(NH):
        x_put(k).wait()
    for k in range(2):
        ag_own(xa_ref, xs, xr, k)

    def gates(i, carry):
        rows = pl.ds(pl.multiple_of(i * 128, 128), 128)
        g = gv[rows, :]
        duv[rows, :fp] = (g * utv[rows, :].astype(F32) * spv[rows, :]).astype(BF16)
        duv[rows, fp:] = (g * av[rows, :]).astype(BF16)
        return carry

    lax.fori_loop(0, tall // 128, gates, 0)

    def sent(k, carry):
        ag_sent(dyv, ys, yr, k)
        dy_out(k).wait()
        return carry

    lax.fori_loop(0, NH, sent, 0)
    zt_out.wait()

    def rs0(k, c):
        return rcopy(dyv.at[:, c, :, cols(k)], r0v.at[k], rs.at[k, 0], rr.at[k, 0], pn)

    def rs1(k, j, owner):
        return rcopy(blk(dyv, owner, k), r1v.at[k, j], rs.at[k, 1 + j], rr.at[k, 1 + j], n1(k))

    def rs2(k):
        return rcopy(blk(dyv, n2(k), k), r2v.at[k], rs.at[k, 3], rr.at[k, 3], n2(k))

    def add(owner, k, other):
        b = blk(dyv, owner, k)
        b[...] = (b[...].astype(F32) + other.astype(F32)).astype(BF16)

    def t_block(r0, n):
        lanes = pl.ds(r0, 128)
        rows = pl.ds(r0, n)
        ugv[rows, :] = duv[:, lanes].T[:n]
        uuv[rows, :] = duv[:, pl.ds(fp + r0, 128)].T[:n]

    def phase2(i, carry):
        @pl.when(i < NH - 2)
        def _():
            ag_own(xa_ref, xs, xr, i + 2)

        @pl.when(i < NH)
        def _():
            ag_mid(xa_ref, xs, xr, i)
            w_load(i, 0).wait()
            w_load(i, 1).wait()
            slot = (i + 1) % 2
            for n in range(0, hc, 256):
                p = lax.dot_general(duv[:, :fp], wbuf[slot, 0, :, n:n + 256], (((1,), (0,)), ((), ())),
                                    preferred_element_type=F32)
                p = p + lax.dot_general(duv[:, fp:], wbuf[slot, 1, :, n:n + 256], (((1,), (0,)), ((), ())),
                                        preferred_element_type=F32)
                dyv[:, :, :, pl.ds(pl.multiple_of(i * hc + n, 256), 256)] = p.astype(BF16).reshape(4, 2, tok, 256)

            @pl.when(i + 2 < NH)
            def _():
                w_load(i + 2, 0).start()
                w_load(i + 2, 1).start()

        @pl.when(i < nfull)
        def _():
            t_block(pl.multiple_of(i * 128, 128), 128)

        @pl.when(i < NH)
        def _():
            rs0(i, 1 - tc).start()

        @pl.when((i >= 1) & (i <= NH))
        def _():
            k = i - 1
            ag_last(xa_ref, xs, xr, k)
            rs0(k, tc).wait_recv()
            for q in range(4):
                add(2 * q + tc, k, r0v[k, q])
            rs1(k, 0, n1(k)).start()
            rs1(k, 1, dg).start()

        @pl.when((i >= 2) & (i <= NH + 1))
        def _():
            k = i - 2
            rs1(k, 0, t).wait_recv()
            rs1(k, 1, n2(k)).wait_recv()
            add(n2(k), k, r1v[k, 1])
            add(t, k, r1v[k, 0])
            rs2(k).start()

        @pl.when(i >= 3)
        def _():
            k = i - 3
            rs2(k).wait_recv()
            dxv[:, cols(k)] = (blk(dyv, t, k)[...].astype(F32) + r2v[k].astype(F32)).astype(BF16)

        return carry

    lax.fori_loop(0, NH + 3, phase2, 0)
    if rest:
        t_block(nfull * 128, rest)
    outs = [pltpu.make_async_copy(ugv, dgt_ref, ol.at[0]), pltpu.make_async_copy(uuv, dut_ref, ol.at[1]),
            pltpu.make_async_copy(dxv, dx_ref, ol.at[2])]
    for o in outs:
        o.start()

    def drain(k, carry):
        ag_end(xa_ref, xs, xr, k)
        ag_sent(xa_ref, xs, xr, k)
        rs0(k, 1 - tc).wait_send()
        rs1(k, 0, n1(k)).wait_send()
        rs1(k, 1, dg).wait_send()
        rs2(k).wait_send()
        return carry

    lax.fori_loop(0, NH, drain, 0)
    for o in outs:
        o.wait()


def _weight_kernel(zt_ref, dgt_ref, dut_ref, dy_ref, x_ref, dd_ref, dg_ref, du_ref):
    j = pl.program_id(0)
    n = pl.num_programs(0) // 3

    @pl.when(j < n)
    def _():
        dd_ref[...] = jnp.dot(zt_ref[...], dy_ref[...], preferred_element_type=F32)

    @pl.when((j >= n) & ((j - n) % 2 == 0))
    def _():
        dg_ref[...] = jnp.dot(dgt_ref[...], x_ref[...], preferred_element_type=F32)

    @pl.when((j >= n) & ((j - n) % 2 == 1))
    def _():
        du_ref[...] = jnp.dot(dut_ref[...], x_ref[...], preferred_element_type=F32)


def solution(mesh):
    def local_backward(x, wg, wu, wd, ug, uu, dy):
        tok, hid = dy.shape
        ff = wd.shape[0]
        fp = _lanes(ff)
        tall = 8 * tok
        hc = hid // NH
        any_ = pl.BlockSpec(memory_space=pl.ANY)
        sem = pltpu.SemaphoreType.DMA
        full = jax.ShapeDtypeStruct((4, 2, tok, hid), BF16)
        act = jax.ShapeDtypeStruct((ff, tall), BF16)
        dx, zt, dgt, dut, dya, xa = pl.pallas_call(
            _comm_kernel,
            out_shape=(jax.ShapeDtypeStruct((tok, hid), BF16), act, act, act, full, full),
            in_specs=[any_] * 7,
            out_specs=(any_,) * 6,
            scratch_shapes=[
                pltpu.VMEM((4, 2, tok, hid), BF16),
                pltpu.VMEM((tall, fp), F32),
                pltpu.VMEM((tall, fp), F32),
                pltpu.VMEM((tall, fp), F32),
                pltpu.VMEM((tall, fp), BF16),
                pltpu.VMEM((tall, 2 * fp), BF16),
                pltpu.VMEM((2, 2, fp, hc), BF16),
                pltpu.VMEM((ff, tall), BF16),
                pltpu.VMEM((ff, tall), BF16),
                pltpu.VMEM((NH, 4, tok, hc), BF16),
                pltpu.VMEM((NH, 2, tok, hc), BF16),
                pltpu.VMEM((NH, tok, hc), BF16),
                pltpu.VMEM((tok, hid), BF16),
                pltpu.VMEM((tok, hid), BF16),
                sem((NH, 7)), sem((NH, 7)), sem((NH, 7)), sem((NH, 7)), sem((NH, 4)), sem((NH, 4)),
                sem((NH,)), sem((NH,)), sem((2, 2)), sem((2,)), sem((3,)), sem((NH,)),
            ],
            compiler_params=pltpu.CompilerParams(collective_id=0, has_side_effects=True, vmem_limit_bytes=67043328),
            name="gather_reduce",
        )(x, dy, wd, wg.T, wu.T, ug.T, uu.T)

        nb = 512
        n = hid // nb
        res = pl.BlockSpec((ff, tall), lambda j: (0, 0))
        grad = jax.ShapeDtypeStruct((ff, hid), F32)
        dwd, dwg, dwu = pl.pallas_call(
            _weight_kernel,
            grid=(3 * n,),
            out_shape=(grad, grad, grad),
            in_specs=[res, res, res,
                      pl.BlockSpec((tall, nb), lambda j: (0, jnp.minimum(j, n - 1))),
                      pl.BlockSpec((tall, nb), lambda j: (0, jnp.maximum(j - n, 0) // 2))],
            out_specs=(pl.BlockSpec((ff, nb), lambda j: (0, jnp.minimum(j, n - 1))),
                       pl.BlockSpec((ff, nb), lambda j: (0, jnp.maximum(j - n, 0) // 2)),
                       pl.BlockSpec((ff, nb), lambda j: (0, jnp.maximum(j - n - 1, 0) // 2))),
            compiler_params=pltpu.CompilerParams(vmem_limit_bytes=63 * 2 ** 20),
            cost_estimate=pl.CostEstimate(flops=6 * ff * tall * hid, bytes_accessed=12 * ff * hid, transcendentals=0),
            name="weight_grads",
        )(zt, dgt, dut, dya.reshape(tall, hid), xa.reshape(tall, hid))
        return dx, dwg.T, dwu.T, dwd

    tok_spec = P(('dp', 'tp'), None)
    col_spec = P(None, 'tp')
    act_spec = P('dp', 'tp')
    return jax.shard_map(local_backward, mesh=mesh,
                         in_specs=(tok_spec, col_spec, col_spec, P('tp', None), act_spec, act_spec, tok_spec),
                         out_specs=(tok_spec, act_spec, act_spec, tok_spec),
                         check_vma=False)
```

```python
import functools

import jax
import jax.numpy as jnp
from jax import lax
from jax.experimental import pallas as pl
from jax.experimental.pallas import tpu as pltpu
from jax.sharding import PartitionSpec as P

MESH = pl.DeviceIdType.MESH
BF16 = jnp.bfloat16
F32 = jnp.float32
NH = 8
NT = (((1,), (1,)), ((), ()))


def _lanes(n):
    return (n + 127) // 128 * 128


def _comm_kernel(x_ref, dy_ref, wd_ref, wg_ref, wu_ref, ug_ref, uu_ref,
                 sa_ref, ka_ref, sb_ref, kb_ref, zt_ref, dgt_ref, dut_ref, dya_ref, xa_ref,
                 dyv, gv, av, spv, utv, duv, wbuf, ugv, uuv, r0v, xov,
                 ys, yr, xs, xr, rs, rr, yl, xl, wl, ul, ol, dl, po):
    tok, hid = dy_ref.shape
    ff = wd_ref.shape[0]
    fp = _lanes(ff)
    nfull, rest = ff // 128, ff % 128
    hc = hid // NH
    tall = 8 * tok
    half = NH // 2

    t = lax.axis_index("tp")
    ty, tx, tc = t // 4, (t // 2) % 2, t % 2
    xn = t + 2 - 4 * tx
    yn = t + 4 - 8 * ty
    dg = xn + yn - t
    pn = t + 1 - 2 * tc

    def n1(k):
        return xn + (yn - xn) * (k % 2)

    def n2(k):
        return yn + (xn - yn) * (k % 2)

    def cols(k):
        return pl.ds(pl.multiple_of(k * hc, hc), hc)

    def blk(ref, owner, k):
        return ref.at[owner // 2, owner % 2, :, cols(k)]

    def rcopy(src, dst, ss, rs_, dev):
        return pltpu.make_async_remote_copy(src_ref=src, dst_ref=dst, send_sem=ss, recv_sem=rs_,
                                            device_id={"tp": dev}, device_id_type=MESH)

    def ag(buf, ss, sr, k, j, owner, dev):
        return rcopy(blk(buf, owner, k), blk(buf, owner, k), ss.at[k, j], sr.at[k, j], dev)

    def ag_own(buf, ss, sr, k):
        ag(buf, ss, sr, k, 0, t, n1(k)).start()
        ag(buf, ss, sr, k, 1, t, n2(k)).start()
        ag(buf, ss, sr, k, 3, t, pn).start()

    def x_own(k, j, dev):
        return rcopy(xov.at[:, cols(k)], blk(xa_ref, t, k), xs.at[k, j], xr.at[k, j], dev)

    def x_send(k):
        x_own(k, 0, n1(k)).start()
        x_own(k, 1, n2(k)).start()
        x_own(k, 3, pn).start()

    def ag_mid(buf, ss, sr, k):
        ag(buf, ss, sr, k, 0, n1(k), n1(k)).wait_recv()
        ag(buf, ss, sr, k, 2, n1(k), n2(k)).start()
        ag(buf, ss, sr, k, 4, n1(k), pn).start()

    def ag_last(buf, ss, sr, k):
        ag(buf, ss, sr, k, 1, n2(k), n2(k)).wait_recv()
        ag(buf, ss, sr, k, 5, n2(k), pn).start()
        ag(buf, ss, sr, k, 2, dg, n2(k)).wait_recv()
        ag(buf, ss, sr, k, 6, dg, pn).start()

    def ag_end(buf, ss, sr, k):
        pc = 1 - 2 * tc
        ag(buf, ss, sr, k, 3, t + pc, pn).wait_recv()
        ag(buf, ss, sr, k, 4, n1(k) + pc, pn).wait_recv()
        ag(buf, ss, sr, k, 5, n2(k) + pc, pn).wait_recv()
        ag(buf, ss, sr, k, 6, dg + pc, pn).wait_recv()

    def ag_sent(buf, ss, sr, k):
        ag(buf, ss, sr, k, 0, t, n1(k)).wait_send()
        ag(buf, ss, sr, k, 1, t, n2(k)).wait_send()
        ag(buf, ss, sr, k, 2, n1(k), n2(k)).wait_send()
        ag(buf, ss, sr, k, 3, t, pn).wait_send()
        ag(buf, ss, sr, k, 4, n1(k), pn).wait_send()
        ag(buf, ss, sr, k, 5, n2(k), pn).wait_send()
        ag(buf, ss, sr, k, 6, dg, pn).wait_send()

    def y_local(k):
        return pltpu.make_async_copy(dy_ref.at[:, cols(k)], blk(dyv, t, k), yl.at[k])

    def x_local(k):
        return pltpu.make_async_copy(x_ref.at[:, cols(k)], xov.at[:, cols(k)], xl.at[k])

    def x_put(k):
        return pltpu.make_async_copy(xov.at[:, cols(k)], blk(xa_ref, t, k), xl.at[k])

    def wd_load(k):
        return pltpu.make_async_copy(wd_ref.at[:, cols(k)], wbuf.at[0, k % 2, pl.ds(0, ff), :], wl.at[0, k % 2])

    def w_load(k, j):
        src = (wg_ref, wu_ref)[j]
        return pltpu.make_async_copy(src.at[:, cols(k)], wbuf.at[(k + 1) % 2, j, pl.ds(0, ff), :],
                                     wl.at[(k + 1) % 2, j])

    def dy_out(k):
        return pltpu.make_async_copy(dyv.at[:, :, :, cols(k)], dya_ref.at[:, :, :, cols(k)], dl.at[k])

    ug_in = pltpu.make_async_copy(ug_ref, ugv, ul.at[0])
    uu_in = pltpu.make_async_copy(uu_ref, uuv, ul.at[1])
    for k in range(NH):
        y_local(k).start()
    wd_load(0).start()
    wd_load(1).start()
    ug_in.start()
    uu_in.start()
    for k in range(NH):
        x_local(k).start()

    barrier = pltpu.get_barrier_semaphore()
    for dev in (xn, yn, pn):
        pl.semaphore_signal(barrier, inc=1, device_id={"tp": dev}, device_id_type=MESH)
    pl.semaphore_wait(barrier, 3)

    for k in range(2):
        y_local(k).wait()
        ag_own(dyv, ys, yr, k)

    for a in range(2):
        for b in range(2):
            wbuf[a, b, ff:, :] = jnp.zeros((fp - ff, hc), BF16)
    gv[...] = jnp.zeros_like(gv)
    ug_in.wait()
    uu_in.wait()

    def u_block(r0, n):
        rows = pl.ds(r0, n)
        ug = ugv[rows, :].astype(F32)
        ub = uuv[rows, :]
        uu = ub.astype(F32)
        s = jax.nn.sigmoid(ug)
        a = ug * s
        sp = s * (1.0 + ug * (1.0 - s))
        ugv[rows, :] = (a * uu).astype(BF16)
        if n < 128:
            pad = jnp.zeros((128 - n, tall), F32)
            a = jnp.concatenate([a, pad], axis=0)
            sp = jnp.concatenate([sp, pad], axis=0)
            uu = jnp.concatenate([uu, pad], axis=0)
        lanes = pl.ds(r0, 128)
        av[:, lanes] = a.T
        spv[:, lanes] = sp.T
        utv[:, lanes] = uu.T.astype(BF16)

    def phase1(i, carry):
        @pl.when(i < NH - 2)
        def _():
            y_local(i + 2).wait()
            ag_own(dyv, ys, yr, i + 2)

        @pl.when(i < NH)
        def _():
            ag_mid(dyv, ys, yr, i)

        for first, ks in ((NH - 1, range(0, 2)), (NH, range(2, 5)), (NH + 1, range(5, NH))):
            @pl.when(i == first)
            def _():
                for k in ks:
                    x_send(k)

        @pl.when(i < nfull)
        def _():
            u_block(pl.multiple_of(i * 128, 128), 128)

        @pl.when((i >= 1) & (i <= NH))
        def _():
            ag_last(dyv, ys, yr, i - 1)

        @pl.when(i >= 2)
        def _():
            k = i - 2
            ag_end(dyv, ys, yr, k)
            dy_out(k).start()
            wd_load(k).wait()
            dyc = dyv[:, :, :, cols(k)].reshape(tall, hc)
            for n in range(0, fp, 256):
                w = min(256, fp - n)
                gv[:, n:n + w] += lax.dot_general(dyc, wbuf[0, k % 2, n:n + w, :], NT, preferred_element_type=F32)

            @pl.when(k + 2 < NH)
            def _():
                wd_load(k + 2).start()

        return carry

    w_load(0, 0).start()
    w_load(0, 1).start()
    for k in range(NH):
        x_local(k).wait()
        x_put(k).start()
    lax.fori_loop(0, NH + 2, phase1, 0)
    w_load(1, 0).start()
    w_load(1, 1).start()
    if rest:
        u_block(nfull * 128, rest)
    zt_out = pltpu.make_async_copy(ugv, zt_ref, ol.at[0])
    zt_out.start()
    def gates(i, carry):
        rows = pl.ds(pl.multiple_of(i * 128, 128), 128)
        g = gv[rows, :]
        duv[rows, :fp] = (g * utv[rows, :].astype(F32) * spv[rows, :]).astype(BF16)
        duv[rows, fp:] = (g * av[rows, :]).astype(BF16)
        return carry

    lax.fori_loop(0, tall // 128, gates, 0)

    def sent(k, carry):
        ag_sent(dyv, ys, yr, k)
        dy_out(k).wait()
        return carry

    lax.fori_loop(0, NH, sent, 0)
    zt_out.wait()

    def rs0(k, c):
        return rcopy(dyv.at[:, c, :, cols(k)], r0v.at[k], rs.at[k], rr.at[k], pn)

    def sums_out(k, left):
        kk = k if left else k - half
        send, keep, far, near = (sa_ref, ka_ref, xn, yn) if left else (sb_ref, kb_ref, yn, xn)
        return [pltpu.make_async_copy(blk(dyv, owner, k), ref.at[b, :, cols(kk)], po.at[k, 2 * a + b])
                for a, ref, owners in ((0, send, (far, dg)), (1, keep, (t, near))) for b, owner in enumerate(owners)]

    def add(owner, k, other):
        b = blk(dyv, owner, k)
        b[...] = (b[...].astype(F32) + other.astype(F32)).astype(BF16)

    def t_block(r0, n):
        lanes = pl.ds(r0, 128)
        rows = pl.ds(r0, n)
        ugv[rows, :] = duv[:, lanes].T[:n]
        uuv[rows, :] = duv[:, pl.ds(fp + r0, 128)].T[:n]

    def phase2(i, carry):
        @pl.when(i < NH)
        def _():
            ag_mid(xa_ref, xs, xr, i)
            w_load(i, 0).wait()
            w_load(i, 1).wait()
            slot = (i + 1) % 2
            for n in range(0, hc, 256):
                p = lax.dot_general(duv[:, :fp], wbuf[slot, 0, :, n:n + 256], (((1,), (0,)), ((), ())),
                                    preferred_element_type=F32)
                p = p + lax.dot_general(duv[:, fp:], wbuf[slot, 1, :, n:n + 256], (((1,), (0,)), ((), ())),
                                        preferred_element_type=F32)
                dyv[:, :, :, pl.ds(pl.multiple_of(i * hc + n, 256), 256)] = p.astype(BF16).reshape(4, 2, tok, 256)

            @pl.when(i + 2 < NH)
            def _():
                w_load(i + 2, 0).start()
                w_load(i + 2, 1).start()

        for b in (2 * i, 2 * i + 1):
            @pl.when(b < nfull)
            def _():
                t_block(pl.multiple_of(b * 128, 128), 128)

        @pl.when(i < NH)
        def _():
            rs0(i, 1 - tc).start()

        @pl.when((i >= 1) & (i <= NH))
        def _():
            k = i - 1
            ag_last(xa_ref, xs, xr, k)
            rs0(k, tc).wait_recv()
            for q in range(4):
                add(2 * q + tc, k, r0v[k, q])

            @pl.when(k < half)
            def _():
                for o in sums_out(k, True):
                    o.start()

            @pl.when(k >= half)
            def _():
                for o in sums_out(k, False):
                    o.start()

        return carry

    lax.fori_loop(0, NH + 1, phase2, 0)
    if rest:
        t_block(nfull * 128, rest)
    outs = [pltpu.make_async_copy(ugv, dgt_ref, ol.at[0]), pltpu.make_async_copy(uuv, dut_ref, ol.at[1])]
    for o in outs:
        o.start()

    def drain(k, carry):
        ag_end(xa_ref, xs, xr, k)
        x_put(k).wait()
        x_own(k, 0, n1(k)).wait_send()
        x_own(k, 1, n2(k)).wait_send()
        ag(xa_ref, xs, xr, k, 2, n1(k), n2(k)).wait_send()
        x_own(k, 3, pn).wait_send()
        ag(xa_ref, xs, xr, k, 4, n1(k), pn).wait_send()
        ag(xa_ref, xs, xr, k, 5, n2(k), pn).wait_send()
        ag(xa_ref, xs, xr, k, 6, dg, pn).wait_send()
        rs0(k, 1 - tc).wait_send()

        @pl.when(k < half)
        def _():
            for o in sums_out(k, True):
                o.wait()

        @pl.when(k >= half)
        def _():
            for o in sums_out(k, False):
                o.wait()

        return carry

    lax.fori_loop(0, NH, drain, 0)
    for o in outs:
        o.wait()


def _row_chunks(ff):
    n = ff // 16
    size = -(-n // 4)
    return [16 * min(size, n - i) for i in range(0, n, size)]


def _weight_kernel(*refs, n):
    m = len(refs) // 3
    lhs, rhs, out = refs[:m], refs[m:2 * m], refs[2 * m:]
    ff, tall = lhs[0].shape
    nb = out[0].shape[1]
    sizes = _row_chunks(ff)
    j = pl.program_id(0)

    def product(a, b, o, accs):
        steps = []
        for pair in range(nb // 512):
            row = 0
            for c, size in enumerate(sizes):
                for kt in range(tall // 256):
                    steps.append((pair, c, row, size, kt))
                row += size

        def push(s):
            pair, _, _, _, kt = steps[s]
            for q in range(2):
                lo = pair * 512 + q * 256
                pltpu.matmul_push_rhs(b[kt * 256:kt * 256 + 256, lo:lo + 256], s % 2, q)

        def pop(pair, c, row, size):
            for q in range(2):
                lo = pair * 512 + q * 256
                o[row:row + size, lo:lo + 256] = pltpu.matmul_pop(accs[q][c])

        push(0)
        late = None
        for s, (pair, c, row, size, kt) in enumerate(steps):
            if s + 1 < len(steps):
                push(s + 1)
            block = a[row:row + size, kt * 256:kt * 256 + 256]
            for q in range(2):
                pltpu.matmul_acc_lhs(accs[q][c], block, load_staged_rhs=s % 2)
            if kt == 0 and late is not None:
                pop(*late)
            if kt == tall // 256 - 1:
                late = (pair, c, row, size)
        pop(*late)

    def body(*flat):
        half = len(flat) // 2
        accs = []
        for part in (flat[:half], flat[half:]):
            accs.append([part[2] if i == len(sizes) - 1 else part[i % 2] for i in range(len(sizes))])
        for i in range(m):
            @pl.when((j >= i * n) & (j < (i + 1) * n))
            def _():
                product(lhs[i], rhs[i], out[i], accs)

    pl.run_scoped(body, *[pltpu.ACC(q)((size, 256), F32) for q in range(2) for size in (sizes[0], sizes[0], sizes[-1])])


def _weight_grads(lhs, rhs, name):
    m = len(lhs)
    ff, tall = lhs[0].shape
    hid = rhs[0].shape[1]
    nb = 1024
    n = hid // nb

    def col(i):
        return lambda j: (0, jnp.clip(j - i * n, 0, n - 1))

    return pl.pallas_call(
        functools.partial(_weight_kernel, n=n),
        grid=(m * n,),
        out_shape=(jax.ShapeDtypeStruct((ff, hid), F32),) * m,
        in_specs=[pl.BlockSpec((ff, tall), lambda j: (0, 0))] * m + [pl.BlockSpec((tall, nb), col(i)) for i in range(m)],
        out_specs=tuple(pl.BlockSpec((ff, nb), col(i)) for i in range(m)),
        compiler_params=pltpu.CompilerParams(vmem_limit_bytes=63 * 2 ** 20),
        cost_estimate=pl.CostEstimate(flops=2 * m * ff * tall * hid, bytes_accessed=m * 4 * ff * hid, transcendentals=0),
        name=name,
    )(*lhs, *rhs)


def solution(mesh):
    def local_backward(x, wg, wu, wd, ug, uu, dy):
        tok, hid = dy.shape
        ff = wd.shape[0]
        fp = _lanes(ff)
        tall = 8 * tok
        hc = hid // NH
        any_ = pl.BlockSpec(memory_space=pl.ANY)
        sem = pltpu.SemaphoreType.DMA
        full = jax.ShapeDtypeStruct((4, 2, tok, hid), BF16)
        act = jax.ShapeDtypeStruct((ff, tall), BF16)
        half = jax.ShapeDtypeStruct((2, tok, hid // 2), BF16)
        sa, ka, sb, kb, zt, dgt, dut, dya, xa = pl.pallas_call(
            _comm_kernel,
            out_shape=(half, half, half, half, act, act, act, full, full),
            in_specs=[any_] * 7,
            out_specs=(any_,) * 9,
            scratch_shapes=[
                pltpu.VMEM((4, 2, tok, hid), BF16),
                pltpu.VMEM((tall, fp), F32),
                pltpu.VMEM((tall, fp), F32),
                pltpu.VMEM((tall, fp), F32),
                pltpu.VMEM((tall, fp), BF16),
                pltpu.VMEM((tall, 2 * fp), BF16),
                pltpu.VMEM((2, 2, fp, hc), BF16),
                pltpu.VMEM((ff, tall), BF16),
                pltpu.VMEM((ff, tall), BF16),
                pltpu.VMEM((NH, 4, tok, hc), BF16),
                pltpu.VMEM((tok, hid), BF16),
                sem((NH, 7)), sem((NH, 7)), sem((NH, 7)), sem((NH, 7)), sem((NH,)), sem((NH,)),
                sem((NH,)), sem((NH,)), sem((2, 2)), sem((2,)), sem((2,)), sem((NH,)), sem((NH, 4)),
            ],
            compiler_params=pltpu.CompilerParams(collective_id=0, has_side_effects=True, vmem_limit_bytes=67043328),
            name="gather_partial",
        )(x, dy, wd, wg.T, wu.T, ug.T, uu.T)
        dya = dya.reshape(tall, hid)
        xa = xa.reshape(tall, hid)

        def to_x(v):
            return lax.ppermute(v, 'tp', [(i, i ^ 2) for i in range(8)])

        def to_y(v):
            return lax.ppermute(v, 'tp', [(i, i ^ 4) for i in range(8)])

        def plus(*terms):
            return sum(v.astype(F32) for v in terms).astype(BF16)

        ra, rb = to_x(sa), to_y(sb)
        dwd, dwg = _weight_grads((zt, dgt), (dya, xa), "grads_down_gate")
        ra, rb, dwd, dwg = lax.optimization_barrier((ra, rb, dwd, dwg))
        ma, mb = plus(ka[1], ra[1]), plus(kb[1], rb[1])
        ma, mb, dut = lax.optimization_barrier((ma, mb, dut))
        fa, fb = to_y(ma), to_x(mb)
        dwu, = _weight_grads((dut,), (xa,), "grads_up")
        fa, fb, dwu = lax.optimization_barrier((fa, fb, dwu))
        dx = jnp.concatenate([plus(ka[0], ra[0], fa), plus(kb[0], rb[0], fb)], axis=1)
        return dx, dwg.T, dwu.T, dwd

    tok_spec = P(('dp', 'tp'), None)
    col_spec = P(None, 'tp')
    act_spec = P('dp', 'tp')
    return jax.shard_map(local_backward, mesh=mesh,
                         in_specs=(tok_spec, col_spec, col_spec, P('tp', None), act_spec, act_spec, tok_spec),
                         out_specs=(tok_spec, act_spec, act_spec, tok_spec),
                         check_vma=False)
```

```python
import functools

import jax
import jax.numpy as jnp
from jax import lax
from jax.experimental import pallas as pl
from jax.experimental.pallas import tpu as pltpu
from jax.sharding import PartitionSpec as P

MESH = pl.DeviceIdType.MESH
BF16 = jnp.bfloat16
F32 = jnp.float32
AHEAD = 3
NH = 8
NT = (((1,), (1,)), ((), ()))


def _lanes(n):
    return (n + 127) // 128 * 128


def _comm_kernel(x_ref, dy_ref, wd_ref, wg_ref, wu_ref, ug_ref, uu_ref,
                 sa_ref, ka_ref, sb_ref, kb_ref, zt_ref, dgt_ref, dut_ref, dya_ref, xa_ref,
                 dyv, gv, av, spv, utv, duv, wbuf, ugv, uuv, r0v, xov,
                 ys, yr, xs, xr, rs, rr, yl, xl, wl, ul, ol, dl, po):
    tok, hid = dy_ref.shape
    ff = wd_ref.shape[0]
    fp = _lanes(ff)
    nfull, rest = ff // 128, ff % 128
    hc = hid // NH
    tall = 8 * tok
    half = NH // 2

    t = lax.axis_index("tp")
    ty, tx, tc = t // 4, (t // 2) % 2, t % 2
    xn = t + 2 - 4 * tx
    yn = t + 4 - 8 * ty
    dg = xn + yn - t
    pn = t + 1 - 2 * tc

    def n1(k):
        return xn + (yn - xn) * (k % 2)

    def n2(k):
        return yn + (xn - yn) * (k % 2)

    def cols(k):
        return pl.ds(pl.multiple_of(k * hc, hc), hc)

    def blk(ref, owner, k):
        return ref.at[owner // 2, owner % 2, :, cols(k)]

    def rcopy(src, dst, ss, rs_, dev):
        return pltpu.make_async_remote_copy(src_ref=src, dst_ref=dst, send_sem=ss, recv_sem=rs_,
                                            device_id={"tp": dev}, device_id_type=MESH)

    def ag(buf, ss, sr, k, j, owner, dev):
        return rcopy(blk(buf, owner, k), blk(buf, owner, k), ss.at[k, j], sr.at[k, j], dev)

    def ag_own(buf, ss, sr, k):
        ag(buf, ss, sr, k, 0, t, n1(k)).start()
        ag(buf, ss, sr, k, 1, t, n2(k)).start()
        ag(buf, ss, sr, k, 3, t, pn).start()

    def x_own(k, j, dev):
        return rcopy(xov.at[:, cols(k)], blk(xa_ref, t, k), xs.at[k, j], xr.at[k, j], dev)

    def x_send(k):
        x_own(k, 0, n1(k)).start()
        x_own(k, 1, n2(k)).start()
        x_own(k, 3, pn).start()

    def ag_mid(buf, ss, sr, k):
        ag(buf, ss, sr, k, 0, n1(k), n1(k)).wait_recv()
        ag(buf, ss, sr, k, 2, n1(k), n2(k)).start()
        ag(buf, ss, sr, k, 4, n1(k), pn).start()

    def ag_last(buf, ss, sr, k):
        ag(buf, ss, sr, k, 1, n2(k), n2(k)).wait_recv()
        ag(buf, ss, sr, k, 5, n2(k), pn).start()
        ag(buf, ss, sr, k, 2, dg, n2(k)).wait_recv()
        ag(buf, ss, sr, k, 6, dg, pn).start()

    def ag_end(buf, ss, sr, k):
        pc = 1 - 2 * tc
        ag(buf, ss, sr, k, 3, t + pc, pn).wait_recv()
        ag(buf, ss, sr, k, 4, n1(k) + pc, pn).wait_recv()
        ag(buf, ss, sr, k, 5, n2(k) + pc, pn).wait_recv()
        ag(buf, ss, sr, k, 6, dg + pc, pn).wait_recv()

    def ag_sent(buf, ss, sr, k):
        ag(buf, ss, sr, k, 0, t, n1(k)).wait_send()
        ag(buf, ss, sr, k, 1, t, n2(k)).wait_send()
        ag(buf, ss, sr, k, 2, n1(k), n2(k)).wait_send()
        ag(buf, ss, sr, k, 3, t, pn).wait_send()
        ag(buf, ss, sr, k, 4, n1(k), pn).wait_send()
        ag(buf, ss, sr, k, 5, n2(k), pn).wait_send()
        ag(buf, ss, sr, k, 6, dg, pn).wait_send()

    def y_local(k):
        return pltpu.make_async_copy(dy_ref.at[:, cols(k)], blk(dyv, t, k), yl.at[k])

    def x_local(k):
        return pltpu.make_async_copy(x_ref.at[:, cols(k)], xov.at[:, cols(k)], xl.at[k])

    def x_put(k):
        return pltpu.make_async_copy(xov.at[:, cols(k)], blk(xa_ref, t, k), xl.at[k])

    def wd_load(k):
        return pltpu.make_async_copy(wd_ref.at[:, cols(k)], wbuf.at[0, k % 2, pl.ds(0, ff), :], wl.at[0, k % 2])

    def w_load(k, j):
        src = (wg_ref, wu_ref)[j]
        return pltpu.make_async_copy(src.at[:, cols(k)], wbuf.at[(k + 1) % 2, j, pl.ds(0, ff), :],
                                     wl.at[(k + 1) % 2, j])

    def dy_out(k):
        return pltpu.make_async_copy(dyv.at[:, :, :, cols(k)], dya_ref.at[:, :, :, cols(k)], dl.at[k])

    ug_in = pltpu.make_async_copy(ug_ref, ugv, ul.at[0])
    uu_in = pltpu.make_async_copy(uu_ref, uuv, ul.at[1])
    for k in range(NH):
        y_local(k).start()
    wd_load(0).start()
    wd_load(1).start()
    ug_in.start()
    uu_in.start()
    for k in range(NH):
        x_local(k).start()

    barrier = pltpu.get_barrier_semaphore()
    for dev in (xn, yn, pn):
        pl.semaphore_signal(barrier, inc=1, device_id={"tp": dev}, device_id_type=MESH)
    pl.semaphore_wait(barrier, 3)

    for k in range(AHEAD):
        y_local(k).wait()
        ag_own(dyv, ys, yr, k)

    for a in range(2):
        for b in range(2):
            wbuf[a, b, ff:, :] = jnp.zeros((fp - ff, hc), BF16)
    gv[...] = jnp.zeros_like(gv)
    ug_in.wait()
    uu_in.wait()

    def u_block(r0, n):
        rows = pl.ds(r0, n)
        ug = ugv[rows, :].astype(F32)
        ub = uuv[rows, :]
        uu = ub.astype(F32)
        s = jax.nn.sigmoid(ug)
        a = ug * s
        sp = s * (1.0 + ug * (1.0 - s))
        ugv[rows, :] = (a * uu).astype(BF16)
        if n < 128:
            pad = jnp.zeros((128 - n, tall), F32)
            a = jnp.concatenate([a, pad], axis=0)
            sp = jnp.concatenate([sp, pad], axis=0)
            uu = jnp.concatenate([uu, pad], axis=0)
        lanes = pl.ds(r0, 128)
        av[:, lanes] = a.T
        spv[:, lanes] = sp.T
        utv[:, lanes] = uu.T.astype(BF16)

    def phase1(i, carry):
        @pl.when(i < NH - AHEAD)
        def _():
            y_local(i + AHEAD).wait()
            ag_own(dyv, ys, yr, i + AHEAD)

        @pl.when(i < NH)
        def _():
            ag_mid(dyv, ys, yr, i)

        for first, ks in ((NH - 1, range(0, 2)), (NH, range(2, 4)), (NH + 1, range(4, 6)), (NH + 2, range(6, NH))):
            @pl.when(i == first)
            def _():
                for k in ks:
                    x_send(k)

        @pl.when(i < nfull)
        def _():
            u_block(pl.multiple_of(i * 128, 128), 128)

        @pl.when((i >= 2) & (i <= NH + 1))
        def _():
            ag_last(dyv, ys, yr, i - 2)

        @pl.when(i >= 3)
        def _():
            k = i - 3
            ag_end(dyv, ys, yr, k)
            dy_out(k).start()
            wd_load(k).wait()
            dyc = dyv[:, :, :, cols(k)].reshape(tall, hc)
            for n in range(0, fp, 256):
                w = min(256, fp - n)
                gv[:, n:n + w] += lax.dot_general(dyc, wbuf[0, k % 2, n:n + w, :], NT, preferred_element_type=F32)

            @pl.when(k + 2 < NH)
            def _():
                wd_load(k + 2).start()

        return carry

    w_load(0, 0).start()
    w_load(0, 1).start()
    for k in range(NH):
        x_local(k).wait()
        x_put(k).start()
    lax.fori_loop(0, NH + 3, phase1, 0)
    w_load(1, 0).start()
    w_load(1, 1).start()
    if rest:
        u_block(nfull * 128, rest)
    zt_out = pltpu.make_async_copy(ugv, zt_ref, ol.at[0])
    zt_out.start()
    def gates(i, carry):
        rows = pl.ds(pl.multiple_of(i * 128, 128), 128)
        g = gv[rows, :]
        duv[rows, :fp] = (g * utv[rows, :].astype(F32) * spv[rows, :]).astype(BF16)
        duv[rows, fp:] = (g * av[rows, :]).astype(BF16)
        return carry

    lax.fori_loop(0, tall // 128, gates, 0)

    def sent(k, carry):
        ag_sent(dyv, ys, yr, k)
        dy_out(k).wait()
        return carry

    lax.fori_loop(0, NH, sent, 0)
    zt_out.wait()

    def rs0(k, c):
        return rcopy(dyv.at[:, c, :, cols(k)], r0v.at[k], rs.at[k], rr.at[k], pn)

    def sums_out(k, left):
        kk = k if left else k - half
        send, keep, far, near = (sa_ref, ka_ref, xn, yn) if left else (sb_ref, kb_ref, yn, xn)
        return [pltpu.make_async_copy(blk(dyv, owner, k), ref.at[b, :, cols(kk)], po.at[k, 2 * a + b])
                for a, ref, owners in ((0, send, (far, dg)), (1, keep, (t, near))) for b, owner in enumerate(owners)]

    def add(owner, k, other):
        b = blk(dyv, owner, k)
        b[...] = (b[...].astype(F32) + other.astype(F32)).astype(BF16)

    def t_block(r0, n):
        lanes = pl.ds(r0, 128)
        rows = pl.ds(r0, n)
        ugv[rows, :] = duv[:, lanes].T[:n]
        uuv[rows, :] = duv[:, pl.ds(fp + r0, 128)].T[:n]

    per = -(-nfull // NH)

    def phase2(i, carry):
        for first, ks in ((NH - 2, range(0, 3)), (NH - 1, range(3, 6)), (NH, range(6, NH))):
            @pl.when(i == first)
            def _():
                for k in ks:
                    ag_last(xa_ref, xs, xr, k)

        @pl.when(i < NH)
        def _():
            ag_mid(xa_ref, xs, xr, i)
            w_load(i, 0).wait()
            w_load(i, 1).wait()
            slot = (i + 1) % 2
            for b in range(per):
                t_block(pl.multiple_of(jnp.minimum(per * i + b, nfull - 1) * 128, 128), 128)
            for n in range(0, hc, 256):
                p = lax.dot_general(duv[:, :fp], wbuf[slot, 0, :, n:n + 256], (((1,), (0,)), ((), ())),
                                    preferred_element_type=F32)
                p = p + lax.dot_general(duv[:, fp:], wbuf[slot, 1, :, n:n + 256], (((1,), (0,)), ((), ())),
                                        preferred_element_type=F32)
                dyv[:, :, :, pl.ds(pl.multiple_of(i * hc + n, 256), 256)] = p.astype(BF16).reshape(4, 2, tok, 256)

            @pl.when(i + 2 < NH)
            def _():
                w_load(i + 2, 0).start()
                w_load(i + 2, 1).start()

        @pl.when(i < NH)
        def _():
            rs0(i, 1 - tc).start()

        @pl.when((i >= 1) & (i <= NH))
        def _():
            k = i - 1
            rs0(k, tc).wait_recv()
            for q in range(4):
                add(2 * q + tc, k, r0v[k, q])

            @pl.when(k < half)
            def _():
                for o in sums_out(k, True):
                    o.start()

            @pl.when(k >= half)
            def _():
                for o in sums_out(k, False):
                    o.start()

        return carry

    lax.fori_loop(0, NH + 1, phase2, 0)
    if rest:
        t_block(nfull * 128, rest)
    outs = [pltpu.make_async_copy(ugv, dgt_ref, ol.at[0]), pltpu.make_async_copy(uuv, dut_ref, ol.at[1])]
    for o in outs:
        o.start()

    def drain(k, carry):
        ag_end(xa_ref, xs, xr, k)
        x_put(k).wait()
        x_own(k, 0, n1(k)).wait_send()
        x_own(k, 1, n2(k)).wait_send()
        ag(xa_ref, xs, xr, k, 2, n1(k), n2(k)).wait_send()
        x_own(k, 3, pn).wait_send()
        ag(xa_ref, xs, xr, k, 4, n1(k), pn).wait_send()
        ag(xa_ref, xs, xr, k, 5, n2(k), pn).wait_send()
        ag(xa_ref, xs, xr, k, 6, dg, pn).wait_send()
        rs0(k, 1 - tc).wait_send()

        @pl.when(k < half)
        def _():
            for o in sums_out(k, True):
                o.wait()

        @pl.when(k >= half)
        def _():
            for o in sums_out(k, False):
                o.wait()

        return carry

    lax.fori_loop(0, NH, drain, 0)
    for o in outs:
        o.wait()


def _plus(*terms):
    return sum(v.astype(F32) for v in terms).astype(BF16)


def _pass_kernel(ka_ref, ra_ref, kb_ref, rb_ref, ma_ref, mb_ref):
    ma_ref[...] = _plus(ka_ref[0], ra_ref[0])
    mb_ref[...] = _plus(kb_ref[0], rb_ref[0])


def _join_kernel(ka_ref, ra_ref, fa_ref, kb_ref, rb_ref, fb_ref, dx_ref):
    h = fa_ref.shape[1]
    dx_ref[:, :h] = _plus(ka_ref[0], ra_ref[0], fa_ref[...])
    dx_ref[:, h:] = _plus(kb_ref[0], rb_ref[0], fb_ref[...])


def _row_chunks(ff):
    n = ff // 16
    size = -(-n // 4)
    return [16 * min(size, n - i) for i in range(0, n, size)]


def _weight_kernel(*refs, n):
    m = len(refs) // 3
    lhs, rhs, out = refs[:m], refs[m:2 * m], refs[2 * m:]
    ff, tall = lhs[0].shape
    nb = out[0].shape[1]
    sizes = _row_chunks(ff)
    j = pl.program_id(0)

    def product(a, b, o, accs):
        steps = []
        for pair in range(nb // 512):
            row = 0
            for c, size in enumerate(sizes):
                for kt in range(tall // 256):
                    steps.append((pair, c, row, size, kt))
                row += size

        def push(s):
            pair, _, _, _, kt = steps[s]
            for q in range(2):
                lo = pair * 512 + q * 256
                pltpu.matmul_push_rhs(b[kt * 256:kt * 256 + 256, lo:lo + 256], s % 2, q)

        def pop(pair, c, row, size):
            for q in range(2):
                lo = pair * 512 + q * 256
                o[row:row + size, lo:lo + 256] = pltpu.matmul_pop(accs[q][c])

        push(0)
        late = None
        for s, (pair, c, row, size, kt) in enumerate(steps):
            if s + 1 < len(steps):
                push(s + 1)
            block = a[row:row + size, kt * 256:kt * 256 + 256]
            for q in range(2):
                pltpu.matmul_acc_lhs(accs[q][c], block, load_staged_rhs=s % 2)
            if kt == 0 and late is not None:
                pop(*late)
            if kt == tall // 256 - 1:
                late = (pair, c, row, size)
        pop(*late)

    def body(*flat):
        half = len(flat) // 2
        accs = []
        for part in (flat[:half], flat[half:]):
            accs.append([part[2] if i == len(sizes) - 1 else part[i % 2] for i in range(len(sizes))])
        for i in range(m):
            @pl.when((j >= i * n) & (j < (i + 1) * n))
            def _():
                product(lhs[i], rhs[i], out[i], accs)

    pl.run_scoped(body, *[pltpu.ACC(q)((size, 256), F32) for q in range(2) for size in (sizes[0], sizes[0], sizes[-1])])


def _weight_grads(lhs, rhs, name):
    m = len(lhs)
    ff, tall = lhs[0].shape
    hid = rhs[0].shape[1]
    nb = 1024
    n = hid // nb

    def col(i):
        return lambda j: (0, jnp.clip(j - i * n, 0, n - 1))

    return pl.pallas_call(
        functools.partial(_weight_kernel, n=n),
        grid=(m * n,),
        out_shape=(jax.ShapeDtypeStruct((ff, hid), F32),) * m,
        in_specs=[pl.BlockSpec((ff, tall), lambda j: (0, 0))] * m + [pl.BlockSpec((tall, nb), col(i)) for i in range(m)],
        out_specs=tuple(pl.BlockSpec((ff, nb), col(i)) for i in range(m)),
        compiler_params=pltpu.CompilerParams(vmem_limit_bytes=63 * 2 ** 20),
        cost_estimate=pl.CostEstimate(flops=2 * m * ff * tall * hid, bytes_accessed=m * 4 * ff * hid, transcendentals=0),
        name=name,
    )(*lhs, *rhs)


def solution(mesh):
    def local_backward(x, wg, wu, wd, ug, uu, dy):
        tok, hid = dy.shape
        ff = wd.shape[0]
        fp = _lanes(ff)
        tall = 8 * tok
        hc = hid // NH
        any_ = pl.BlockSpec(memory_space=pl.ANY)
        sem = pltpu.SemaphoreType.DMA
        full = jax.ShapeDtypeStruct((4, 2, tok, hid), BF16)
        act = jax.ShapeDtypeStruct((ff, tall), BF16)
        half = jax.ShapeDtypeStruct((2, tok, hid // 2), BF16)
        sa, ka, sb, kb, zt, dgt, dut, dya, xa = pl.pallas_call(
            _comm_kernel,
            out_shape=(half, half, half, half, act, act, act, full, full),
            in_specs=[any_] * 7,
            out_specs=(any_,) * 9,
            scratch_shapes=[
                pltpu.VMEM((4, 2, tok, hid), BF16),
                pltpu.VMEM((tall, fp), F32),
                pltpu.VMEM((tall, fp), F32),
                pltpu.VMEM((tall, fp), F32),
                pltpu.VMEM((tall, fp), BF16),
                pltpu.VMEM((tall, 2 * fp), BF16),
                pltpu.VMEM((2, 2, fp, hc), BF16),
                pltpu.VMEM((ff, tall), BF16),
                pltpu.VMEM((ff, tall), BF16),
                pltpu.VMEM((NH, 4, tok, hc), BF16),
                pltpu.VMEM((tok, hid), BF16),
                sem((NH, 7)), sem((NH, 7)), sem((NH, 7)), sem((NH, 7)), sem((NH,)), sem((NH,)),
                sem((NH,)), sem((NH,)), sem((2, 2)), sem((2,)), sem((2,)), sem((NH,)), sem((NH, 4)),
            ],
            compiler_params=pltpu.CompilerParams(collective_id=0, has_side_effects=True, vmem_limit_bytes=67043328),
            name="gather_partial",
        )(x, dy, wd, wg.T, wu.T, ug.T, uu.T)
        dya = dya.reshape(tall, hid)
        xa = xa.reshape(tall, hid)

        def to_x(v):
            return lax.ppermute(v, 'tp', [(i, i ^ 2) for i in range(8)])

        def to_y(v):
            return lax.ppermute(v, 'tp', [(i, i ^ 4) for i in range(8)])

        ra, rb = to_x(sa), to_y(sb)
        dwd, dwg = _weight_grads((zt, dgt), (dya, xa), "grads_down_gate")
        ra, rb, dwd, dwg = lax.optimization_barrier((ra, rb, dwd, dwg))
        rows = tok // 2
        flat = pl.BlockSpec((rows, hid // 2), lambda j: (j, 0))
        pair = jax.ShapeDtypeStruct((tok, hid // 2), BF16)
        second = pl.BlockSpec((1, rows, hid // 2), lambda j: (1, j, 0))
        ma, mb = pl.pallas_call(_pass_kernel, out_shape=(pair, pair), in_specs=[second] * 4, out_specs=(flat, flat), grid=(2,),
                                name="pass_on")(ka, ra, kb, rb)
        ma, mb, dut = lax.optimization_barrier((ma, mb, dut))
        fa, fb = to_y(ma), to_x(mb)
        dwu, = _weight_grads((dut,), (xa,), "grads_up")
        fa, fb, dwu = lax.optimization_barrier((fa, fb, dwu))
        first = pl.BlockSpec((1, rows, hid // 2), lambda j: (0, j, 0))
        dx = pl.pallas_call(_join_kernel, out_shape=jax.ShapeDtypeStruct((tok, hid), BF16),
                            in_specs=[first, first, flat, first, first, flat],
                            out_specs=pl.BlockSpec((rows, hid), lambda j: (j, 0)), grid=(2,), name="join")(ka, ra, fa, kb, rb, fb)
        return dx, dwg.T, dwu.T, dwd

    tok_spec = P(('dp', 'tp'), None)
    col_spec = P(None, 'tp')
    act_spec = P('dp', 'tp')
    return jax.shard_map(local_backward, mesh=mesh,
                         in_specs=(tok_spec, col_spec, col_spec, P('tp', None), act_spec, act_spec, tok_spec),
                         out_specs=(tok_spec, act_spec, act_spec, tok_spec),
                         check_vma=False)
```

```python
import functools

import jax
import jax.numpy as jnp
from jax import lax
from jax.experimental import pallas as pl
from jax.experimental.pallas import tpu as pltpu
from jax.sharding import PartitionSpec as P

MESH = pl.DeviceIdType.MESH
BF16 = jnp.bfloat16
F32 = jnp.float32
NH = 8
NY = 16
AHEAD, LAG, TAKE = 4, 4, 6
NT = (((1,), (1,)), ((), ()))


def _lanes(n):
    return (n + 127) // 128 * 128


def _comm_kernel(x_ref, dy_ref, wd_ref, wg_ref, wu_ref, ug_ref, uu_ref,
                 so_ref, sx_ref, sy_ref, sd_ref, zt_ref, dgt_ref, dut_ref, dya_ref, xa_ref,
                 dyv, gv, av, spv, utv, duv, wbuf, ugv, uuv, r0v, r1v, xov,
                 ys, yr, xs, xr, rs, rr, r1s, r1r, yl, xl, wl, ul, ol, dl, po):
    tok, hid = dy_ref.shape
    ff = wd_ref.shape[0]
    fp = _lanes(ff)
    nfull, rest = ff // 128, ff % 128
    hc = hid // NH
    tall = 8 * tok
    half = NH // 2

    t = lax.axis_index("tp")
    ty, tx, tc = t // 4, (t // 2) % 2, t % 2
    xn = t + 2 - 4 * tx
    yn = t + 4 - 8 * ty
    dg = xn + yn - t
    pn = t + 1 - 2 * tc

    def n1(k):
        return xn + (yn - xn) * (k % 2)

    def n2(k):
        return yn + (xn - yn) * (k % 2)

    hy = hid // NY
    per_h = NY // NH

    def cols(k, w=hc):
        return pl.ds(pl.multiple_of(k * w, w), w)

    def blk(ref, owner, k, w=hc):
        return ref.at[owner // 2, owner % 2, :, cols(k, w)]

    def rcopy(src, dst, ss, rs_, dev):
        return pltpu.make_async_remote_copy(src_ref=src, dst_ref=dst, send_sem=ss, recv_sem=rs_,
                                            device_id={"tp": dev}, device_id_type=MESH)

    def ag(buf, ss, sr, k, j, owner, dev):
        w = hid // ss.shape[0]
        return rcopy(blk(buf, owner, k, w), blk(buf, owner, k, w), ss.at[k, j], sr.at[k, j], dev)

    def ag_own(buf, ss, sr, k):
        ag(buf, ss, sr, k, 0, t, n1(k)).start()
        ag(buf, ss, sr, k, 1, t, n2(k)).start()
        ag(buf, ss, sr, k, 3, t, pn).start()

    def x_own(k, j, dev):
        return rcopy(xov.at[:, cols(k)], blk(xa_ref, t, k), xs.at[k, j], xr.at[k, j], dev)

    def x_send(k):
        x_own(k, 0, n1(k)).start()
        x_own(k, 1, n2(k)).start()
        x_own(k, 3, pn).start()

    def ag_mid(buf, ss, sr, k):
        ag(buf, ss, sr, k, 0, n1(k), n1(k)).wait_recv()
        ag(buf, ss, sr, k, 2, n1(k), n2(k)).start()
        ag(buf, ss, sr, k, 4, n1(k), pn).start()

    def ag_last(buf, ss, sr, k):
        ag(buf, ss, sr, k, 1, n2(k), n2(k)).wait_recv()
        ag(buf, ss, sr, k, 5, n2(k), pn).start()
        ag(buf, ss, sr, k, 2, dg, n2(k)).wait_recv()
        ag(buf, ss, sr, k, 6, dg, pn).start()

    def ag_end(buf, ss, sr, k):
        pc = 1 - 2 * tc
        ag(buf, ss, sr, k, 3, t + pc, pn).wait_recv()
        ag(buf, ss, sr, k, 4, n1(k) + pc, pn).wait_recv()
        ag(buf, ss, sr, k, 5, n2(k) + pc, pn).wait_recv()
        ag(buf, ss, sr, k, 6, dg + pc, pn).wait_recv()

    def ag_sent(buf, ss, sr, k):
        ag(buf, ss, sr, k, 0, t, n1(k)).wait_send()
        ag(buf, ss, sr, k, 1, t, n2(k)).wait_send()
        ag(buf, ss, sr, k, 2, n1(k), n2(k)).wait_send()
        ag(buf, ss, sr, k, 3, t, pn).wait_send()
        ag(buf, ss, sr, k, 4, n1(k), pn).wait_send()
        ag(buf, ss, sr, k, 5, n2(k), pn).wait_send()
        ag(buf, ss, sr, k, 6, dg, pn).wait_send()

    def y_local(k):
        return pltpu.make_async_copy(dy_ref.at[:, cols(k, hy)], blk(dyv, t, k, hy), yl.at[k])

    def x_local(k):
        return pltpu.make_async_copy(x_ref.at[:, cols(k)], xov.at[:, cols(k)], xl.at[k])

    def x_put(k):
        return pltpu.make_async_copy(xov.at[:, cols(k)], blk(xa_ref, t, k), xl.at[k])

    def wd_load(k):
        return pltpu.make_async_copy(wd_ref.at[:, cols(k)], wbuf.at[0, k % 2, pl.ds(0, ff), :], wl.at[0, k % 2])

    def w_load(k, j):
        src = (wg_ref, wu_ref)[j]
        return pltpu.make_async_copy(src.at[:, cols(k)], wbuf.at[(k + 1) % 2, j, pl.ds(0, ff), :],
                                     wl.at[(k + 1) % 2, j])

    def dy_out(k):
        return pltpu.make_async_copy(dyv.at[:, :, :, cols(k)], dya_ref.at[:, :, :, cols(k)], dl.at[k])

    ug_in = pltpu.make_async_copy(ug_ref, ugv, ul.at[0])
    uu_in = pltpu.make_async_copy(uu_ref, uuv, ul.at[1])
    for k in range(NY):
        y_local(k).start()
    wd_load(0).start()
    wd_load(1).start()
    ug_in.start()
    uu_in.start()
    for k in range(NH):
        x_local(k).start()

    barrier = pltpu.get_barrier_semaphore()
    for dev in (xn, yn, pn):
        pl.semaphore_signal(barrier, inc=1, device_id={"tp": dev}, device_id_type=MESH)
    pl.semaphore_wait(barrier, 3)

    for k in range(AHEAD):
        y_local(k).wait()
        ag_own(dyv, ys, yr, k)

    for a in range(2):
        for b in range(2):
            wbuf[a, b, ff:, :] = jnp.zeros((fp - ff, hc), BF16)
    gv[...] = jnp.zeros_like(gv)
    ug_in.wait()
    uu_in.wait()

    def u_block(r0, n):
        rows = pl.ds(r0, n)
        ug = ugv[rows, :].astype(F32)
        ub = uuv[rows, :]
        uu = ub.astype(F32)
        s = jax.nn.sigmoid(ug)
        a = ug * s
        sp = s * (1.0 + ug * (1.0 - s))
        ugv[rows, :] = (a * uu).astype(BF16)
        if n < 128:
            pad = jnp.zeros((128 - n, tall), F32)
            a = jnp.concatenate([a, pad], axis=0)
            sp = jnp.concatenate([sp, pad], axis=0)
            uu = jnp.concatenate([uu, pad], axis=0)
        lanes = pl.ds(r0, 128)
        av[:, lanes] = a.T
        spv[:, lanes] = sp.T
        utv[:, lanes] = uu.T.astype(BF16)

    def phase1(i, carry):
        @pl.when(i < NY - AHEAD)
        def _():
            y_local(i + AHEAD).wait()
            ag_own(dyv, ys, yr, i + AHEAD)

        @pl.when(i < NY)
        def _():
            ag_mid(dyv, ys, yr, i)

        @pl.when(i >= NY + TAKE - NH)
        def _():
            x_send(i - (NY + TAKE - NH))

        @pl.when(i < nfull)
        def _():
            u_block(pl.multiple_of(i * 128, 128), 128)

        if rest:
            @pl.when(i == nfull)
            def _():
                u_block(nfull * 128, rest)

        @pl.when((i >= LAG) & (i < NY + LAG))
        def _():
            ag_last(dyv, ys, yr, i - LAG)

        @pl.when(i >= TAKE)
        def _():
            ag_end(dyv, ys, yr, i - TAKE)

        @pl.when((i >= TAKE) & ((i - TAKE) % per_h == per_h - 1))
        def _():
            k = (i - TAKE) // per_h
            dy_out(k).start()
            wd_load(k).wait()
            dyc = dyv[:, :, :, cols(k)].reshape(tall, hc)
            for n in range(0, fp, 256):
                w = min(256, fp - n)
                gv[:, n:n + w] += lax.dot_general(dyc, wbuf[0, k % 2, n:n + w, :], NT, preferred_element_type=F32)

            @pl.when(k + 2 < NH)
            def _():
                wd_load(k + 2).start()

        return carry

    w_load(0, 0).start()
    w_load(0, 1).start()
    for k in range(NH):
        x_local(k).wait()
        x_put(k).start()
    lax.fori_loop(0, NY + TAKE, phase1, 0)
    w_load(1, 0).start()
    w_load(1, 1).start()
    zt_out = pltpu.make_async_copy(ugv, zt_ref, ol.at[0])
    zt_out.start()
    def gates(i, carry):
        rows = pl.ds(pl.multiple_of(i * 128, 128), 128)
        g = gv[rows, :]
        duv[rows, :fp] = (g * utv[rows, :].astype(F32) * spv[rows, :]).astype(BF16)
        duv[rows, fp:] = (g * av[rows, :]).astype(BF16)
        return carry

    lax.fori_loop(0, tall // 128, gates, 0)

    def sent(k, carry):
        ag_sent(dyv, ys, yr, k)
        return carry

    lax.fori_loop(0, NY, sent, 0)
    for k in range(NH):
        dy_out(k).wait()
    zt_out.wait()

    def rs0(k, c):
        return rcopy(dyv.at[:, c, :, cols(k)], r0v.at[k], rs.at[k], rr.at[k], pn)

    def rs1(k):
        return rcopy(blk(dyv, dg, k), r1v.at[k], r1s.at[k], r1r.at[k], n1(k))

    def sums_out(k, diagonal):
        outs = [(so_ref, t, k), (sx_ref, xn, k), (sy_ref, yn, k)] + ([(sd_ref, dg, k - half)] if diagonal else [])
        return [pltpu.make_async_copy(blk(dyv, owner, k), ref.at[:, cols(c)], po.at[k, i])
                for i, (ref, owner, c) in enumerate(outs)]

    def add(owner, k, other):
        b = blk(dyv, owner, k)
        b[...] = (b[...].astype(F32) + other.astype(F32)).astype(BF16)

    def t_block(r0, n):
        lanes = pl.ds(r0, 128)
        rows = pl.ds(r0, n)
        ugv[rows, :] = duv[:, lanes].T[:n]
        uuv[rows, :] = duv[:, pl.ds(fp + r0, 128)].T[:n]

    per = -(-nfull // NH)

    def phase2(i, carry):
        for first, ks in ((NH - 2, range(0, 3)), (NH - 1, range(3, 6)), (NH, range(6, NH))):
            @pl.when(i == first)
            def _():
                for k in ks:
                    ag_last(xa_ref, xs, xr, k)

        @pl.when(i < NH)
        def _():
            ag_mid(xa_ref, xs, xr, i)
            w_load(i, 0).wait()
            w_load(i, 1).wait()
            slot = (i + 1) % 2
            for b in range(per):
                t_block(pl.multiple_of(jnp.minimum(per * i + b, nfull - 1) * 128, 128), 128)
            for n in range(0, hc, 256):
                p = lax.dot_general(duv[:, :fp], wbuf[slot, 0, :, n:n + 256], (((1,), (0,)), ((), ())),
                                    preferred_element_type=F32)
                p = p + lax.dot_general(duv[:, fp:], wbuf[slot, 1, :, n:n + 256], (((1,), (0,)), ((), ())),
                                        preferred_element_type=F32)
                dyv[:, :, :, pl.ds(pl.multiple_of(i * hc + n, 256), 256)] = p.astype(BF16).reshape(4, 2, tok, 256)

            @pl.when(i + 2 < NH)
            def _():
                w_load(i + 2, 0).start()
                w_load(i + 2, 1).start()

        @pl.when(i < NH)
        def _():
            rs0(i, 1 - tc).start()

        @pl.when((i >= 1) & (i <= NH))
        def _():
            k = i - 1
            rs0(k, tc).wait_recv()
            for q in range(4):
                add(2 * q + tc, k, r0v[k, q])

            @pl.when(k < half)
            def _():
                rs1(k).start()

            @pl.when(k >= half)
            def _():
                for o in sums_out(k, True):
                    o.start()

        @pl.when((i >= half) & (i < NH))
        def _():
            k = i - half
            rs1(k).wait_recv()
            add(n2(k), k, r1v[k])
            for o in sums_out(k, False):
                o.start()

        return carry

    lax.fori_loop(0, NH + 1, phase2, 0)
    if rest:
        t_block(nfull * 128, rest)
    outs = [pltpu.make_async_copy(ugv, dgt_ref, ol.at[0]), pltpu.make_async_copy(uuv, dut_ref, ol.at[1])]
    for o in outs:
        o.start()

    def drain(k, carry):
        ag_end(xa_ref, xs, xr, k)
        x_put(k).wait()
        x_own(k, 0, n1(k)).wait_send()
        x_own(k, 1, n2(k)).wait_send()
        ag(xa_ref, xs, xr, k, 2, n1(k), n2(k)).wait_send()
        x_own(k, 3, pn).wait_send()
        ag(xa_ref, xs, xr, k, 4, n1(k), pn).wait_send()
        ag(xa_ref, xs, xr, k, 5, n2(k), pn).wait_send()
        ag(xa_ref, xs, xr, k, 6, dg, pn).wait_send()
        rs0(k, 1 - tc).wait_send()

        @pl.when(k < half)
        def _():
            rs1(k).wait_send()
            for o in sums_out(k, False):
                o.wait()

        @pl.when(k >= half)
        def _():
            for o in sums_out(k, True):
                o.wait()

        return carry

    lax.fori_loop(0, NH, drain, 0)
    for o in outs:
        o.wait()


def _plus(*terms):
    return sum(v.astype(F32) for v in terms).astype(BF16)


def _join_kernel(so_ref, fx_ref, fy_ref, fd_ref, dx_ref):
    h = fd_ref.shape[1]
    dx_ref[:, :h] = _plus(so_ref[:, :h], fx_ref[:, :h], fy_ref[:, :h])
    dx_ref[:, h:] = _plus(so_ref[:, h:], fx_ref[:, h:], fy_ref[:, h:], fd_ref[...])


def _row_chunks(ff):
    n = ff // 16
    size = -(-n // 4)
    return [16 * min(size, n - i) for i in range(0, n, size)]


def _weight_kernel(zt_ref, dgt_ref, dut_ref, dy_ref, x_ref, dd_ref, dg_ref, du_ref,
                   zv, dgv, duv, yv, xv, o0, o1, o2, ls, ysem, xsem, os):
    ff, tall = zt_ref.shape
    hid = dy_ref.shape[1]
    nb = yv.shape[-1]
    n = hid // nb
    sizes = _row_chunks(ff)
    depth = tall // 256

    def load(src, dst, sem, j, p):
        lo = pl.ds(pl.multiple_of(j * nb + p * 512, 512), 512)
        return pltpu.make_async_copy(src.at[:, lo], dst.at[j % 2, :, p * 512:p * 512 + 512], sem.at[j % 2, p])

    def loads(j):
        return [load(src, dst, sem, j, p) for src, dst, sem in ((dy_ref, yv, ysem), (x_ref, xv, xsem))
                for p in range(nb // 512)]

    def put(i, j, rows, width, p):
        stage, out = ((o0, dd_ref), (o1, dg_ref), (o2, du_ref))[i]
        lo = pl.ds(pl.multiple_of(j * nb + p * 512, 512), width)
        slot = j % stage.shape[0]
        return pltpu.make_async_copy(stage.at[slot, rows, p * 512:p * 512 + width], out.at[rows, lo], os.at[i, slot])

    def put_all(i, j):
        return put(i, j, pl.ds(0, ff), nb, 0)

    def product(i, j, accs, waits):
        a = (zv, dgv, duv)[i]
        b = (yv, xv, xv)[i].at[j % 2]
        stage = (o0, o1, o2)[i]
        slot = j % stage.shape[0]
        steps = []
        for pair in range(nb // 512):
            row = 0
            for c, size in enumerate(sizes):
                for kt in range(depth):
                    steps.append((pair, c, row, size, kt))
                row += size

        def push(s):
            pair, _, _, _, kt = steps[s]
            for q in range(2):
                lo = pair * 512 + q * 256
                pltpu.matmul_push_rhs(b[kt * 256:kt * 256 + 256, lo:lo + 256], s % 2, q)

        def pop(pair, c, row, size):
            for q in range(2):
                lo = pair * 512 + q * 256
                stage[slot, row:row + size, lo:lo + 256] = pltpu.matmul_pop(accs[q][c])
            put(i, j, pl.ds(row, size), 512, pair).start()

        late = None
        for s, (pair, c, row, size, kt) in enumerate(steps):
            if s == 0 or (c == 0 and kt == 0 and waits):
                for w in waits[pair] if waits else ():
                    w.wait()
                push(s)
            if s + 1 < len(steps) and not (waits and steps[s + 1][1] == 0 and steps[s + 1][4] == 0):
                push(s + 1)
            block = a[row:row + size, kt * 256:kt * 256 + 256]
            for q in range(2):
                pltpu.matmul_acc_lhs(accs[q][c], block, load_staged_rhs=s % 2)
            if kt == 0 and late is not None:
                pop(*late)
            if kt == depth - 1:
                late = (pair, c, row, size)
        pop(*late)

    zl, gl, ul = (pltpu.make_async_copy(src, dst, ls.at[i])
                  for i, (src, dst) in enumerate(((zt_ref, zv), (dgt_ref, dgv), (dut_ref, duv))))
    first = loads(0)
    zl.start()
    for c in first[:2]:
        c.start()
    gl.start()
    for c in first[2:]:
        c.start()
    ul.start()
    for c in loads(1):
        c.start()

    def body(*flat):
        h = len(flat) // 2
        accs = [[part[2] if i == len(sizes) - 1 else part[i % 2] for i in range(len(sizes))]
                for part in (flat[:h], flat[h:])]
        product(0, 0, accs, [[zl, first[0]], [first[1]]])
        product(1, 0, accs, [[gl, first[2]], [first[3]]])
        product(2, 0, accs, [[ul], []])

        def rest(j, carry):
            for c in loads(j):
                c.wait()

            @pl.when(j + 1 < n)
            def _():
                for c in loads(j + 1):
                    c.start()

            put_all(0, j - 1).wait()
            put_all(1, j - 1).wait()

            @pl.when(j >= 2)
            def _():
                put_all(2, j - 2).wait()

            for i in range(3):
                product(i, j, accs, None)
            return carry

        lax.fori_loop(1, n, rest, 0)

    pl.run_scoped(body, *[pltpu.ACC(q)((size, 256), F32) for q in range(2) for size in (sizes[0], sizes[0], sizes[-1])])
    put_all(0, n - 1).wait()
    put_all(1, n - 1).wait()
    put_all(2, n - 2).wait()
    put_all(2, n - 1).wait()


def _weight_grads(zt, dgt, dut, dy, x):
    ff, tall = zt.shape
    hid = x.shape[1]
    nb = 1024
    sem = pltpu.SemaphoreType.DMA
    any_ = pl.BlockSpec(memory_space=pl.ANY)
    return pl.pallas_call(
        _weight_kernel,
        out_shape=(jax.ShapeDtypeStruct((ff, hid), F32),) * 3,
        in_specs=[any_] * 5,
        out_specs=(any_,) * 3,
        scratch_shapes=[pltpu.VMEM((ff, tall), BF16)] * 3 + [pltpu.VMEM((2, tall, nb), BF16)] * 2
        + [pltpu.VMEM((k, ff, nb), F32) for k in (1, 1, 2)] + [sem((3,)), sem((2, 2)), sem((2, 2)), sem((3, 2))],
        compiler_params=pltpu.CompilerParams(vmem_limit_bytes=63 * 2 ** 20),
        cost_estimate=pl.CostEstimate(flops=6 * ff * tall * hid, bytes_accessed=12 * ff * hid, transcendentals=0),
        name="weight_grads",
    )(zt, dgt, dut, dy, x)


def solution(mesh):
    def local_backward(x, wg, wu, wd, ug, uu, dy):
        tok, hid = dy.shape
        ff = wd.shape[0]
        fp = _lanes(ff)
        tall = 8 * tok
        hc = hid // NH
        any_ = pl.BlockSpec(memory_space=pl.ANY)
        sem = pltpu.SemaphoreType.DMA
        full = jax.ShapeDtypeStruct((4, 2, tok, hid), BF16)
        act = jax.ShapeDtypeStruct((ff, tall), BF16)
        own = jax.ShapeDtypeStruct((tok, hid), BF16)
        half = jax.ShapeDtypeStruct((tok, hid // 2), BF16)
        so, sx, sy, sd, zt, dgt, dut, dya, xa = pl.pallas_call(
            _comm_kernel,
            out_shape=(own, own, own, half, act, act, act, full, full),
            in_specs=[any_] * 7,
            out_specs=(any_,) * 9,
            scratch_shapes=[
                pltpu.VMEM((4, 2, tok, hid), BF16),
                pltpu.VMEM((tall, fp), F32),
                pltpu.VMEM((tall, fp), F32),
                pltpu.VMEM((tall, fp), F32),
                pltpu.VMEM((tall, fp), BF16),
                pltpu.VMEM((tall, 2 * fp), BF16),
                pltpu.VMEM((2, 2, fp, hc), BF16),
                pltpu.VMEM((ff, tall), BF16),
                pltpu.VMEM((ff, tall), BF16),
                pltpu.VMEM((NH, 4, tok, hc), BF16),
                pltpu.VMEM((NH // 2, tok, hc), BF16),
                pltpu.VMEM((tok, hid), BF16),
                sem((NY, 7)), sem((NY, 7)), sem((NH, 7)), sem((NH, 7)), sem((NH,)), sem((NH,)),
                sem((NH // 2,)), sem((NH // 2,)), sem((NY,)), sem((NH,)), sem((2, 2)), sem((2,)), sem((2,)), sem((NH,)), sem((NH, 4)),
            ],
            compiler_params=pltpu.CompilerParams(collective_id=0, has_side_effects=True, vmem_limit_bytes=67043328),
            name="gather_partial",
        )(x, dy, wd, wg.T, wu.T, ug.T, uu.T)
        dya = dya.reshape(tall, hid)
        xa = xa.reshape(tall, hid)

        def to(v, flip):
            return lax.ppermute(v, 'tp', [(i, i ^ flip) for i in range(8)])

        fx, fy, fd = to(sx, 2), to(sy, 4), to(sd, 6)
        dwd, dwg, dwu = _weight_grads(zt, dgt, dut, dya, xa)
        fx, fy, fd, dwd, dwg, dwu = lax.optimization_barrier((fx, fy, fd, dwd, dwg, dwu))
        rows = tok // 2
        wide = pl.BlockSpec((rows, hid), lambda j: (j, 0))
        dx = pl.pallas_call(_join_kernel, grid=(2,), out_shape=own, out_specs=wide,
                            in_specs=[wide, wide, wide, pl.BlockSpec((rows, hid // 2), lambda j: (j, 0))],
                            name="join")(so, fx, fy, fd)
        return dx, dwg.T, dwu.T, dwd

    tok_spec = P(('dp', 'tp'), None)
    col_spec = P(None, 'tp')
    act_spec = P('dp', 'tp')
    return jax.shard_map(local_backward, mesh=mesh,
                         in_specs=(tok_spec, col_spec, col_spec, P('tp', None), act_spec, act_spec, tok_spec),
                         out_specs=(tok_spec, act_spec, act_spec, tok_spec),
                         check_vma=False)
```

```python
import functools

import jax
import jax.numpy as jnp
from jax import lax
from jax.experimental import pallas as pl
from jax.experimental.pallas import tpu as pltpu
from jax.sharding import PartitionSpec as P

MESH = pl.DeviceIdType.MESH
BF16 = jnp.bfloat16
F32 = jnp.float32
NH = 8
DOWN = 4
NY = 16
AHEAD, LAG, TAKE = 4, 4, 6
NT = (((1,), (1,)), ((), ()))


def _lanes(n):
    return (n + 127) // 128 * 128


def _comm_kernel(x_ref, dy_ref, wd_ref, wg_ref, wu_ref, ug_ref, uu_ref,
                 so_ref, sx_ref, sy_ref, sd_ref, zt_ref, dgt_ref, dut_ref, dya_ref, xa_ref, dd_ref,
                 dyv, gv, av, spv, utv, duv, wbuf, ugv, uuv, r0v, r1v, xov, ddv,
                 ys, yr, xs, xr, rs, rr, r1r, yl, xl, wl, ul, ol, dl, po, pd):
    tok, hid = dy_ref.shape
    ff = wd_ref.shape[0]
    fp = _lanes(ff)
    nfull, rest = ff // 128, ff % 128
    hc = hid // NH
    tall = 8 * tok
    half = NH // 2

    t = lax.axis_index("tp")
    ty, tx, tc = t // 4, (t // 2) % 2, t % 2
    xn = t + 2 - 4 * tx
    yn = t + 4 - 8 * ty
    dg = xn + yn - t
    pn = t + 1 - 2 * tc

    def n1(k):
        return xn + (yn - xn) * (k % 2)

    def n2(k):
        return yn + (xn - yn) * (k % 2)

    hy = hid // NY
    per_h = NY // NH

    def cols(k, w=hc):
        return pl.ds(pl.multiple_of(k * w, w), w)

    def blk(ref, owner, k, w=hc):
        return ref.at[owner // 2, owner % 2, :, cols(k, w)]

    def rcopy(src, dst, ss, rs_, dev):
        return pltpu.make_async_remote_copy(src_ref=src, dst_ref=dst, send_sem=ss, recv_sem=rs_,
                                            device_id={"tp": dev}, device_id_type=MESH)

    def ag(buf, ss, sr, k, j, owner, dev):
        w = hid // sr.shape[0]
        return rcopy(blk(buf, owner, k, w), blk(buf, owner, k, w), ss.at[j], sr.at[k, (0, 1, 1, 2, 2, 2, 2)[j]], dev)

    def arrived(ref, sem):
        rcopy(ref, ref, sem, sem, t).wait_recv()

    def left(ref, sem):
        rcopy(ref, ref, sem, sem, t).wait_send()

    def ag_own(buf, ss, sr, k):
        ag(buf, ss, sr, k, 0, t, n1(k)).start()
        ag(buf, ss, sr, k, 1, t, n2(k)).start()
        ag(buf, ss, sr, k, 3, t, pn).start()

    def x_own(k, j, dev):
        return rcopy(xov.at[:, cols(k)], blk(xa_ref, t, k), xs.at[j], xr.at[k, (0, 1, 1, 2)[j]], dev)

    def x_send(k):
        x_own(k, 0, n1(k)).start()
        x_own(k, 1, n2(k)).start()
        x_own(k, 3, pn).start()

    def ag_mid(buf, ss, sr, k):
        ag(buf, ss, sr, k, 0, n1(k), n1(k)).wait_recv()
        ag(buf, ss, sr, k, 2, n1(k), n2(k)).start()
        ag(buf, ss, sr, k, 4, n1(k), pn).start()

    def ag_last(buf, ss, sr, k):
        w = hid // sr.shape[0]
        arrived(buf.at[pl.ds(0, 2), 0, :, cols(k, w)], sr.at[k, 1])
        ag(buf, ss, sr, k, 5, n2(k), pn).start()
        ag(buf, ss, sr, k, 6, dg, pn).start()

    def ag_end(buf, ss, sr, k):
        w = hid // sr.shape[0]
        arrived(buf.at[:, 0, :, cols(k, w)], sr.at[k, 2])

    def y_local(g):
        w = AHEAD * hy
        return pltpu.make_async_copy(dy_ref.at[:, cols(g, w)], blk(dyv, t, g, w), yl.at[g])

    x_local = pltpu.make_async_copy(x_ref, xov, xl.at[0])
    x_put = pltpu.make_async_copy(xov, xa_ref.at[t // 2, t % 2], xl.at[1])

    def down_out(k):
        return pltpu.make_async_copy(ddv.at[k % 2], dd_ref.at[:, cols(k)], pd.at[k % 2])

    def wd_load(k):
        return pltpu.make_async_copy(wd_ref.at[:, cols(k)], wbuf.at[0, pl.ds(pl.multiple_of(k % 2 * fp, fp), ff), :], wl.at[0, k % 2])

    def w_load(k, j):
        src = (wg_ref, wu_ref)[j]
        return pltpu.make_async_copy(src.at[:, cols(k)], wbuf.at[(k + 1) % 2, pl.ds(j * fp, ff), :],
                                     wl.at[(k + 1) % 2, j])

    def dy_out(k):
        return pltpu.make_async_copy(dyv.at[:, :, :, cols(k)], dya_ref.at[:, :, :, cols(k)], dl.at[0])

    ug_in = pltpu.make_async_copy(ug_ref, ugv.at[pl.ds(0, ff), :], ul.at[0])
    uu_in = pltpu.make_async_copy(uu_ref, uuv.at[pl.ds(0, ff), :], ul.at[1])
    for g in range(NY // AHEAD):
        y_local(g).start()
    wd_load(0).start()
    wd_load(1).start()
    ug_in.start()
    uu_in.start()
    x_local.start()

    barrier = pltpu.get_barrier_semaphore()
    for dev in (xn, yn, pn):
        pl.semaphore_signal(barrier, inc=1, device_id={"tp": dev}, device_id_type=MESH)
    pl.semaphore_wait(barrier, 3)

    y_local(0).wait()
    for k in range(AHEAD):
        ag_own(dyv, ys, yr, k)

    for a in range(2):
        for b in range(2):
            wbuf[a, b * fp + ff:b * fp + fp, :] = jnp.zeros((fp - ff, hc), BF16)
    gv[...] = jnp.zeros_like(gv)
    ug_in.wait()
    uu_in.wait()

    def u_block(r0, n):
        rows = pl.ds(r0, n)
        ug = ugv[rows, :].astype(F32)
        ub = uuv[rows, :]
        uu = ub.astype(F32)
        s = jax.nn.sigmoid(ug)
        a = ug * s
        sp = s * (1.0 + ug * (1.0 - s))
        ugv[rows, :] = (a * uu).astype(BF16)
        if n < 128:
            pad = jnp.zeros((128 - n, tall), F32)
            a = jnp.concatenate([a, pad], axis=0)
            sp = jnp.concatenate([sp, pad], axis=0)
            uu = jnp.concatenate([uu, pad], axis=0)
        lanes = pl.ds(r0, 128)
        av[:, lanes] = a.T
        spv[:, lanes] = sp.T
        utv[:, lanes] = uu.T.astype(BF16)

    down0 = -(-(fp // 128) // per_h) * per_h

    def phase1(i, carry):
        @pl.when((i < NY - AHEAD) & (i % AHEAD == 0))
        def _():
            y_local(i // AHEAD + 1).wait()

        @pl.when(i < NY - AHEAD)
        def _():
            ag_own(dyv, ys, yr, i + AHEAD)

        @pl.when(i < NY)
        def _():
            ag_mid(dyv, ys, yr, i)

        @pl.when(i >= NY + TAKE - NH)
        def _():
            x_send(i - (NY + TAKE - NH))

        @pl.when(i < nfull)
        def _():
            u_block(pl.multiple_of(i * 128, 128), 128)

        if rest:
            @pl.when(i == nfull)
            def _():
                u_block(nfull * 128, rest)

        @pl.when((i >= LAG) & (i < NY + LAG))
        def _():
            ag_last(dyv, ys, yr, i - LAG)

        @pl.when(i >= TAKE)
        def _():
            ag_end(dyv, ys, yr, i - TAKE)

        @pl.when((i >= TAKE) & ((i - TAKE) % per_h == per_h - 1))
        def _():
            k = (i - TAKE) // per_h
            dy_out(k).start()
            wd_load(k).wait()
            dyc = dyv[:, :, :, cols(k)].reshape(tall, hc)
            for n in range(0, fp, 256):
                w = min(256, fp - n)
                gv[:, n:n + w] += lax.dot_general(dyc, wbuf[0, pl.ds(pl.multiple_of(k % 2 * fp + n, 128), w), :], NT, preferred_element_type=F32)

            @pl.when(k + 2 < NH)
            def _():
                wd_load(k + 2).start()

        @pl.when((i >= down0) & ((i - down0) % per_h == 0) & (i < down0 + DOWN * per_h))
        def _():
            k = (i - down0) // per_h

            @pl.when(k >= 2)
            def _():
                down_out(k - 2).wait()

            dyc = dyv[:, :, :, cols(k)].reshape(tall, hc)
            ddv[k % 2] = jnp.dot(ugv[:ff, :], dyc, preferred_element_type=F32)
            down_out(k).start()

        return carry

    w_load(0, 0).start()
    w_load(0, 1).start()
    x_local.wait()
    x_put.start()
    lax.fori_loop(0, NY + TAKE, phase1, 0)
    w_load(1, 0).start()
    w_load(1, 1).start()
    zt_out = pltpu.make_async_copy(ugv.at[pl.ds(0, ff), :], zt_ref, ol.at[0])
    zt_out.start()
    def gates(i, carry):
        rows = pl.ds(pl.multiple_of(i * 128, 128), 128)
        g = gv[rows, :]
        duv[rows, :fp] = (g * utv[rows, :].astype(F32) * spv[rows, :]).astype(BF16)
        duv[rows, fp:] = (g * av[rows, :]).astype(BF16)
        return carry

    lax.fori_loop(0, tall // 128, gates, 0)

    for n in range(7):
        left(dyv.at[0, 0], ys.at[n])
    pltpu.make_async_copy(dyv, dya_ref, dl.at[0]).wait()
    zt_out.wait()
    for k in range(DOWN - 2, DOWN):
        down_out(k).wait()

    def rs0(k, c):
        return rcopy(dyv.at[:, c, :, cols(k)], r0v.at[k], rs.at[0], rr.at[k], pn)

    def rs1(k):
        return rcopy(blk(dyv, dg, k), r1v.at[k], rs.at[1], r1r.at[k], n1(k))

    def sums_out(k, diagonal):
        outs = [(so_ref, t, k), (sx_ref, xn, k), (sy_ref, yn, k)] + ([(sd_ref, dg, k - half)] if diagonal else [])
        return [pltpu.make_async_copy(blk(dyv, owner, k), ref.at[:, cols(c)], po.at[i])
                for i, (ref, owner, c) in enumerate(outs)]

    def add(owner, k, other):
        b = blk(dyv, owner, k)
        b[...] = (b[...].astype(F32) + other.astype(F32)).astype(BF16)

    def t_block(r0):
        rows = pl.ds(r0, 128)
        ugv[rows, :] = duv[:, rows].T
        uuv[rows, :] = duv[:, pl.ds(fp + r0, 128)].T

    blocks = fp // 128
    per = -(-blocks // NH)

    def phase2(i, carry):
        for first, ks in ((NH - 2, range(0, 3)), (NH - 1, range(3, 6)), (NH, range(6, NH))):
            @pl.when(i == first)
            def _():
                for k in ks:
                    ag_last(xa_ref, xs, xr, k)

        @pl.when(i < NH)
        def _():
            ag_mid(xa_ref, xs, xr, i)
            w_load(i, 0).wait()
            w_load(i, 1).wait()
            slot = (i + 1) % 2
            for b in range(per):
                t_block(pl.multiple_of(jnp.minimum(per * i + b, blocks - 1) * 128, 128))
            p = jnp.dot(duv[...], wbuf[slot], preferred_element_type=F32)
            dyv[:, :, :, cols(i)] = p.astype(BF16).reshape(4, 2, tok, hc)

            @pl.when(i + 2 < NH)
            def _():
                w_load(i + 2, 0).start()
                w_load(i + 2, 1).start()

        @pl.when(i < NH)
        def _():
            rs0(i, 1 - tc).start()

        @pl.when((i >= 1) & (i <= NH))
        def _():
            k = i - 1
            rs0(k, tc).wait_recv()
            for q in range(4):
                add(2 * q + tc, k, r0v[k, q])

            @pl.when(k < half)
            def _():
                rs1(k).start()

            @pl.when(k >= half)
            def _():
                for o in sums_out(k, True):
                    o.start()

        @pl.when((i >= half) & (i < NH))
        def _():
            k = i - half
            rs1(k).wait_recv()
            add(n2(k), k, r1v[k])
            for o in sums_out(k, False):
                o.start()

        return carry

    lax.fori_loop(0, NH + 1, phase2, 0)
    outs = [pltpu.make_async_copy(v.at[pl.ds(0, ff), :], ref, ol.at[i])
            for i, (v, ref) in enumerate(((ugv, dgt_ref), (uuv, dut_ref)))]
    for o in outs:
        o.start()

    def drain(k, carry):
        ag_end(xa_ref, xs, xr, k)
        return carry

    lax.fori_loop(0, NH, drain, 0)
    for n in range(7):
        left(xa_ref.at[0, 0], xs.at[n])
    left(dyv.at[:, 0], rs.at[0])
    left(dyv.at[0, 0, :, pl.ds(0, hid // 2)], rs.at[1])
    x_put.wait()
    for n, ref in enumerate((so_ref, sx_ref, sy_ref, sd_ref)):
        pltpu.make_async_copy(ref, ref, po.at[n]).wait()
    for o in outs:
        o.wait()


def _row_chunks(ff):
    n = ff // 16
    size = -(-n // 4)
    return [16 * min(size, n - i) for i in range(0, n, size)]


def _weight_kernel(zt_ref, dgt_ref, dut_ref, dy_ref, x_ref, part_ref, dd_ref, dg_ref, du_ref,
                   zv, dgv, duv, yv, xv, o0, o1, o2, cv, ls, ysem, xsem, os, ci, co):
    ff, tall = zt_ref.shape
    hid = dy_ref.shape[1]
    nb = yv.shape[-1]
    n = hid // nb
    sizes = _row_chunks(ff)
    depth = tall // 256

    def load(src, dst, sem, j, p):
        lo = pl.ds(j * nb + p * 512, 512)
        return pltpu.make_async_copy(src.at[:, lo], dst.at[j % 2, :, p * 512:p * 512 + 512], sem.at[j % 2, p])

    def put(i, j, rows, width, p):
        stage, out = ((o0, dd_ref), (o1, dg_ref), (o2, du_ref))[i]
        lo = pl.ds(j * nb + p * 512, width)
        slot = j % stage.shape[0]
        return pltpu.make_async_copy(stage.at[slot, rows, p * 512:p * 512 + width], out.at[rows, lo], os.at[i, slot])

    def put_all(i, j):
        return put(i, j, pl.ds(0, ff), nb, 0)

    def product(i, j, accs, waits):
        a = (zv, dgv, duv)[i]
        b = (yv, xv, xv)[i].at[j % 2]
        stage = (o0, o1, o2)[i]
        slot = j % stage.shape[0]
        steps = []
        for pair in range(nb // 512):
            row = 0
            for c, size in enumerate(sizes):
                for kt in range(depth):
                    steps.append((pair, c, row, size, kt))
                row += size

        def push(s):
            pair, _, _, _, kt = steps[s]
            for q in range(2):
                lo = pair * 512 + q * 256
                pltpu.matmul_push_rhs(b[kt * 256:kt * 256 + 256, lo:lo + 256], s % 2, q)

        def pop(pair, c, row, size):
            for q in range(2):
                lo = pair * 512 + q * 256
                stage[slot, row:row + size, lo:lo + 256] = pltpu.matmul_pop(accs[q][c])
            put(i, j, pl.ds(row, size), 512, pair).start()

        late = None
        for s, (pair, c, row, size, kt) in enumerate(steps):
            if s == 0 or (c == 0 and kt == 0 and waits):
                for w in waits[pair] if waits else ():
                    w.wait()
                push(s)
            if s + 1 < len(steps) and not (waits and steps[s + 1][1] == 0 and steps[s + 1][4] == 0):
                push(s + 1)
            block = a[row:row + size, kt * 256:kt * 256 + 256]
            for q in range(2):
                pltpu.matmul_acc_lhs(accs[q][c], block, load_staged_rhs=s % 2)
            if kt == 0 and late is not None:
                pop(*late)
            if kt == depth - 1:
                late = (pair, c, row, size)
        pop(*late)

    done = part_ref.shape[1]
    wide = cv.shape[2]
    pieces = done // wide

    def take(p):
        return pltpu.make_async_copy(part_ref.at[:, p * wide:p * wide + wide], cv.at[p % 2], ci.at[p % 2])

    def give(p):
        return pltpu.make_async_copy(cv.at[p % 2], dd_ref.at[:, p * wide:p * wide + wide], co.at[p % 2])

    def pass_on(p):
        if 1 <= p <= pieces:
            take(p - 1).wait()
            give(p - 1).start()
        if p < pieces:
            if p >= 2:
                give(p - 2).wait()
            take(p).start()

    zl, gl, ul = (pltpu.make_async_copy(src, dst, ls.at[i])
                  for i, (src, dst) in enumerate(((zt_ref, zv), (dgt_ref, dgv), (dut_ref, duv))))
    y_block = {j: [load(dy_ref, yv, ysem, j, h) for h in range(nb // 512)] for j in range(done // nb, n)}
    x_block = {j: [load(x_ref, xv, xsem, j, h) for h in range(nb // 512)] for j in range(2)}
    sent = {0: [], 1: [], 2: []}
    zl.start()
    for c in y_block[done // nb]:
        c.start()
    gl.start()
    for c in x_block[0]:
        c.start()
    ul.start()
    for j in range(done // nb + 1, n):
        for c in y_block[j]:
            c.start()
    for c in x_block[1]:
        c.start()

    def body(*flat):
        h = len(flat) // 2
        accs = [[part[2] if i == len(sizes) - 1 else part[i % 2] for i in range(len(sizes))]
                for part in (flat[:h], flat[h:])]
        todo = [(i, j) for j in range(n) for i in range(3) if i or j >= done // nb]
        down = [e for e in todo if not e[0]]
        order = []
        for j in range(n):
            order += down[j:j + 1] + [(1, j), (2, j)]
        for p, (i, j) in enumerate(order):
            if i == 1 and j and j + 1 < n:
                x_block[j + 1] = [load(x_ref, xv, xsem, j + 1, h) for h in range(nb // 512)]
            waits = []
            if p == 0:
                waits = [[zl, y_block[j][0]], [y_block[j][1]]]
            elif i == 0:
                waits = [y_block[j], []]
            elif (i, j) == (1, 0):
                waits = [[gl, x_block[0][0]], [x_block[0][1]]]
            elif (i, j) == (2, 0):
                waits = [[ul], []]
            elif i == 1:
                waits = [x_block[j], []]
            if i == 1 and j and j + 1 < n:
                for c in x_block[j + 1]:
                    c.start()
            before = sent[i]
            if len(before) >= (o0, o1, o2)[i].shape[0]:
                put_all(i, before[-(o0, o1, o2)[i].shape[0]]).wait()
            pass_on(p)
            product(i, j, accs, waits)
            before.append(j)

    pl.run_scoped(body, *[pltpu.ACC(q)((size, 256), F32) for q in range(2) for size in (sizes[0], sizes[0], sizes[-1])])
    for i, stage in enumerate((o0, o1, o2)):
        for j in sent[i][-stage.shape[0]:]:
            put_all(i, j).wait()
    for p in range(max(pieces - 2, 0), pieces):
        give(p).wait()


def _weight_grads(zt, dgt, dut, dy, x, part):
    ff, tall = zt.shape
    hid = x.shape[1]
    nb = 1024
    sem = pltpu.SemaphoreType.DMA
    any_ = pl.BlockSpec(memory_space=pl.ANY)
    return pl.pallas_call(
        _weight_kernel,
        out_shape=(jax.ShapeDtypeStruct((ff, hid), F32),) * 3,
        in_specs=[any_] * 6,
        out_specs=(any_,) * 3,
        scratch_shapes=[pltpu.VMEM((ff, tall), BF16)] * 3 + [pltpu.VMEM((2, tall, nb), BF16)] * 2
        + [pltpu.VMEM((k, ff, nb), F32) for k in (1, 2, 2)] + [pltpu.VMEM((2, ff, 256), F32)]
        + [sem((3,)), sem((2, 2)), sem((2, 2)), sem((3, 2)), sem((2,)), sem((2,))],
        compiler_params=pltpu.CompilerParams(vmem_limit_bytes=63 * 2 ** 20),
        cost_estimate=pl.CostEstimate(flops=6 * ff * tall * hid, bytes_accessed=12 * ff * hid, transcendentals=0),
        name="weight_grads",
    )(zt, dgt, dut, dy, x, part)


def solution(mesh):
    def local_backward(x, wg, wu, wd, ug, uu, dy):
        tok, hid = dy.shape
        ff = wd.shape[0]
        fp = _lanes(ff)
        tall = 8 * tok
        hc = hid // NH
        any_ = pl.BlockSpec(memory_space=pl.ANY)
        sem = pltpu.SemaphoreType.DMA
        full = jax.ShapeDtypeStruct((4, 2, tok, hid), BF16)
        act = jax.ShapeDtypeStruct((ff, tall), BF16)
        own = jax.ShapeDtypeStruct((tok, hid), BF16)
        half = jax.ShapeDtypeStruct((tok, hid // 2), BF16)
        so, sx, sy, sd, zt, dgt, dut, dya, xa, ddp = pl.pallas_call(
            _comm_kernel,
            out_shape=(own, own, own, half, act, act, act, full, full,
                       jax.ShapeDtypeStruct((ff, DOWN * hc), F32)),
            in_specs=[any_] * 7,
            out_specs=(any_,) * 10,
            scratch_shapes=[
                pltpu.VMEM((4, 2, tok, hid), BF16),
                pltpu.VMEM((tall, fp), F32),
                pltpu.VMEM((tall, fp), F32),
                pltpu.VMEM((tall, fp), F32),
                pltpu.VMEM((tall, fp), BF16),
                pltpu.VMEM((tall, 2 * fp), BF16),
                pltpu.VMEM((2, 2 * fp, hc), BF16),
                pltpu.VMEM((fp, tall), BF16),
                pltpu.VMEM((fp, tall), BF16),
                pltpu.VMEM((NH, 4, tok, hc), BF16),
                pltpu.VMEM((NH // 2, tok, hc), BF16),
                pltpu.VMEM((tok, hid), BF16),
                pltpu.VMEM((2, ff, hc), F32),
                sem((7,)), sem((NY, 3)), sem((7,)), sem((NH, 3)), sem((2,)), sem((NH,)), sem((NH // 2,)),
                sem((NY // AHEAD,)), sem((2,)), sem((2, 2)), sem((2,)), sem((2,)), sem((1,)), sem((4,)), sem((2,)),
            ],
            compiler_params=pltpu.CompilerParams(collective_id=0, has_side_effects=True, vmem_limit_bytes=67043328),
            name="gather_partial",
        )(x, dy, wd, wg.T, wu.T, ug.T, uu.T)
        dya = dya.reshape(tall, hid)
        xa = xa.reshape(tall, hid)

        def to(v, flip):
            return lax.ppermute(v, 'tp', [(i, i ^ flip) for i in range(8)])

        fx, fy, fd = to(sx, 2), to(sy, 4), to(sd, 6)
        dwd, dwg, dwu = _weight_grads(zt, dgt, dut, dya, xa, ddp)
        fx, fy, fd, dwd, dwg, dwu = lax.optimization_barrier((fx, fy, fd, dwd, dwg, dwu))
        right = jnp.pad(fd, ((0, 0), (hid // 2, 0)))
        dx = sum(v.astype(F32) for v in (so, fx, fy, right)).astype(BF16)
        return dx, dwg.T, dwu.T, dwd

    tok_spec = P(('dp', 'tp'), None)
    col_spec = P(None, 'tp')
    act_spec = P('dp', 'tp')
    return jax.shard_map(local_backward, mesh=mesh,
                         in_specs=(tok_spec, col_spec, col_spec, P('tp', None), act_spec, act_spec, tok_spec),
                         out_specs=(tok_spec, act_spec, act_spec, tok_spec),
                         check_vma=False)
```

```python
import functools

import jax
import jax.numpy as jnp
from jax import lax
from jax.experimental import pallas as pl
from jax.experimental.pallas import tpu as pltpu
from jax.sharding import PartitionSpec as P

MESH = pl.DeviceIdType.MESH
BF16 = jnp.bfloat16
F32 = jnp.float32
NH = 8
DOWN = 2
NY = 16
AHEAD, LAG, TAKE = 4, 4, 6
NT = (((1,), (1,)), ((), ()))


def _lanes(n):
    return (n + 127) // 128 * 128


def _comm_kernel(x_ref, dy_ref, wd_ref, wg_ref, wu_ref, ug_ref, uu_ref,
                 so_ref, sx_ref, sy_ref, sd_ref, zt_ref, dgt_ref, dut_ref, dya_ref, xa_ref, dd_ref,
                 dyv, gv, av, spv, utv, duv, wbuf, ugv, uuv, r0v, r1v, xov, ddv,
                 ys, yr, xs, xr, rs, rr, r1r, yl, xl, wl, ul, ol, dl, po, pd):
    tok, hid = dy_ref.shape
    ff = wd_ref.shape[0]
    fp = _lanes(ff)
    nfull, rest = ff // 128, ff % 128
    hc = hid // NH
    tall = 8 * tok
    half = NH // 2

    t = lax.axis_index("tp")
    ty, tx, tc = t // 4, (t // 2) % 2, t % 2
    xn = t + 2 - 4 * tx
    yn = t + 4 - 8 * ty
    dg = xn + yn - t
    pn = t + 1 - 2 * tc

    def n1(k):
        return xn + (yn - xn) * (k % 2)

    def n2(k):
        return yn + (xn - yn) * (k % 2)

    hy = hid // NY
    per_h = NY // NH

    def cols(k, w=hc):
        return pl.ds(pl.multiple_of(k * w, w), w)

    def blk(ref, owner, k, w=hc):
        return ref.at[owner // 2, owner % 2, :, cols(k, w)]

    def rcopy(src, dst, ss, rs_, dev):
        return pltpu.make_async_remote_copy(src_ref=src, dst_ref=dst, send_sem=ss, recv_sem=rs_,
                                            device_id={"tp": dev}, device_id_type=MESH)

    def ag(buf, ss, sr, k, j, owner, dev):
        w = hid // sr.shape[0]
        return rcopy(blk(buf, owner, k, w), blk(buf, owner, k, w), ss.at[j], sr.at[k, (0, 1, 1, 2, 2, 2, 2)[j]], dev)

    def arrived(ref, sem):
        rcopy(ref, ref, sem, sem, t).wait_recv()

    def left(ref, sem):
        rcopy(ref, ref, sem, sem, t).wait_send()

    def ag_own(buf, ss, sr, k):
        ag(buf, ss, sr, k, 0, t, n1(k)).start()
        ag(buf, ss, sr, k, 1, t, n2(k)).start()
        ag(buf, ss, sr, k, 3, t, pn).start()

    def x_own(k, j, dev):
        return rcopy(xov.at[:, cols(k)], blk(xa_ref, t, k), xs.at[j], xr.at[k, (0, 1, 1, 2)[j]], dev)

    def x_send(k):
        x_own(k, 0, n1(k)).start()
        x_own(k, 1, n2(k)).start()
        x_own(k, 3, pn).start()

    def ag_mid(buf, ss, sr, k):
        ag(buf, ss, sr, k, 0, n1(k), n1(k)).wait_recv()
        ag(buf, ss, sr, k, 2, n1(k), n2(k)).start()
        ag(buf, ss, sr, k, 4, n1(k), pn).start()

    def ag_last(buf, ss, sr, k):
        w = hid // sr.shape[0]
        arrived(buf.at[pl.ds(0, 2), 0, :, cols(k, w)], sr.at[k, 1])
        ag(buf, ss, sr, k, 5, n2(k), pn).start()
        ag(buf, ss, sr, k, 6, dg, pn).start()

    def ag_end(buf, ss, sr, k):
        w = hid // sr.shape[0]
        arrived(buf.at[:, 0, :, cols(k, w)], sr.at[k, 2])

    def y_local(g):
        w = AHEAD * hy
        return pltpu.make_async_copy(dy_ref.at[:, cols(g, w)], blk(dyv, t, g, w), yl.at[g])

    x_local = pltpu.make_async_copy(x_ref, xov, xl.at[0])
    x_put = pltpu.make_async_copy(xov, xa_ref.at[t // 2, t % 2], xl.at[1])

    def down_out(k):
        return pltpu.make_async_copy(ddv.at[k % 2], dd_ref.at[:, cols(k)], pd.at[k % 2])

    def wd_load(k):
        return pltpu.make_async_copy(wd_ref.at[:, cols(k)], wbuf.at[0, pl.ds(pl.multiple_of(k % 2 * fp, fp), ff), :], wl.at[0, k % 2])

    def w_load(k, j):
        src = (wg_ref, wu_ref)[j]
        return pltpu.make_async_copy(src.at[:, cols(k)], wbuf.at[(k + 1) % 2, pl.ds(j * fp, ff), :],
                                     wl.at[(k + 1) % 2, j])

    def dy_out(k):
        return pltpu.make_async_copy(dyv.at[:, :, :, cols(k)], dya_ref.at[:, :, :, cols(k)], dl.at[0])

    ug_in = pltpu.make_async_copy(ug_ref, ugv.at[pl.ds(0, ff), :], ul.at[0])
    uu_in = pltpu.make_async_copy(uu_ref, uuv.at[pl.ds(0, ff), :], ul.at[1])
    for g in range(NY // AHEAD):
        y_local(g).start()
    wd_load(0).start()
    wd_load(1).start()
    ug_in.start()
    uu_in.start()
    x_local.start()

    barrier = pltpu.get_barrier_semaphore()
    for dev in (xn, yn, pn):
        pl.semaphore_signal(barrier, inc=1, device_id={"tp": dev}, device_id_type=MESH)
    pl.semaphore_wait(barrier, 3)

    y_local(0).wait()
    for k in range(AHEAD):
        ag_own(dyv, ys, yr, k)

    for a in range(2):
        for b in range(2):
            wbuf[a, b * fp + ff:b * fp + fp, :] = jnp.zeros((fp - ff, hc), BF16)
    gv[...] = jnp.zeros_like(gv)
    ug_in.wait()
    uu_in.wait()

    def u_block(r0, n):
        rows = pl.ds(r0, n)
        ug = ugv[rows, :].astype(F32)
        ub = uuv[rows, :]
        uu = ub.astype(F32)
        s = jax.nn.sigmoid(ug)
        a = ug * s
        sp = s * (1.0 + ug * (1.0 - s))
        ugv[rows, :] = (a * uu).astype(BF16)
        if n < 128:
            pad = jnp.zeros((128 - n, tall), F32)
            a = jnp.concatenate([a, pad], axis=0)
            sp = jnp.concatenate([sp, pad], axis=0)
            uu = jnp.concatenate([uu, pad], axis=0)
        lanes = pl.ds(r0, 128)
        av[:, lanes] = a.T
        spv[:, lanes] = sp.T
        utv[:, lanes] = uu.T.astype(BF16)

    down0 = -(-(fp // 128) // per_h) * per_h

    def phase1(i, carry):
        @pl.when((i < NY - AHEAD) & (i % AHEAD == 0))
        def _():
            y_local(i // AHEAD + 1).wait()

        @pl.when(i < NY - AHEAD)
        def _():
            ag_own(dyv, ys, yr, i + AHEAD)

        @pl.when(i < NY)
        def _():
            ag_mid(dyv, ys, yr, i)

        @pl.when(i >= NY + TAKE - NH)
        def _():
            x_send(i - (NY + TAKE - NH))

        @pl.when(i < nfull)
        def _():
            u_block(pl.multiple_of(i * 128, 128), 128)

        if rest:
            @pl.when(i == nfull)
            def _():
                u_block(nfull * 128, rest)

        @pl.when((i >= LAG) & (i < NY + LAG))
        def _():
            ag_last(dyv, ys, yr, i - LAG)

        @pl.when(i >= TAKE)
        def _():
            ag_end(dyv, ys, yr, i - TAKE)

        @pl.when((i >= TAKE) & ((i - TAKE) % per_h == per_h - 1))
        def _():
            k = (i - TAKE) // per_h
            dy_out(k).start()
            wd_load(k).wait()
            dyc = dyv[:, :, :, cols(k)].reshape(tall, hc)
            for n in range(0, fp, 256):
                w = min(256, fp - n)
                gv[:, n:n + w] += lax.dot_general(dyc, wbuf[0, pl.ds(pl.multiple_of(k % 2 * fp + n, 128), w), :], NT, preferred_element_type=F32)

            @pl.when(k + 2 < NH)
            def _():
                wd_load(k + 2).start()

        @pl.when((i >= down0) & ((i - down0) % per_h == 0) & (i < down0 + DOWN * per_h))
        def _():
            k = (i - down0) // per_h

            @pl.when(k >= 2)
            def _():
                down_out(k - 2).wait()

            dyc = dyv[:, :, :, cols(k)].reshape(tall, hc)
            ddv[k % 2] = jnp.dot(ugv[:ff, :], dyc, preferred_element_type=F32)
            down_out(k).start()

        return carry

    w_load(0, 0).start()
    w_load(0, 1).start()
    x_local.wait()
    x_put.start()
    lax.fori_loop(0, NY + TAKE, phase1, 0)
    w_load(1, 0).start()
    w_load(1, 1).start()
    zt_out = pltpu.make_async_copy(ugv.at[pl.ds(0, ff), :], zt_ref, ol.at[0])
    zt_out.start()
    def gates(i, carry):
        rows = pl.ds(pl.multiple_of(i * 128, 128), 128)
        g = gv[rows, :]
        duv[rows, :fp] = (g * utv[rows, :].astype(F32) * spv[rows, :]).astype(BF16)
        duv[rows, fp:] = (g * av[rows, :]).astype(BF16)
        return carry

    lax.fori_loop(0, tall // 128, gates, 0)

    for n in range(7):
        left(dyv.at[0, 0], ys.at[n])
    pltpu.make_async_copy(dyv, dya_ref, dl.at[0]).wait()
    zt_out.wait()
    for k in range(DOWN - 2, DOWN):
        down_out(k).wait()

    def rs0(k, c):
        return rcopy(dyv.at[:, c, :, cols(k)], r0v.at[k], rs.at[0], rr.at[k], pn)

    def rs1(k):
        return rcopy(blk(dyv, dg, k), r1v.at[k], rs.at[1], r1r.at[k], n1(k))

    def sums_out(k, diagonal):
        outs = [(so_ref, t, k), (sx_ref, xn, k), (sy_ref, yn, k)] + ([(sd_ref, dg, k - half)] if diagonal else [])
        return [pltpu.make_async_copy(blk(dyv, owner, k), ref.at[:, cols(c)], po.at[i])
                for i, (ref, owner, c) in enumerate(outs)]

    def add(owner, k, other):
        b = blk(dyv, owner, k)
        b[...] = (b[...].astype(F32) + other.astype(F32)).astype(BF16)

    def t_block(r0):
        rows = pl.ds(r0, 128)
        ugv[rows, :] = duv[:, rows].T
        uuv[rows, :] = duv[:, pl.ds(fp + r0, 128)].T

    blocks = fp // 128
    per = -(-blocks // NH)

    def phase2(i, carry):
        for first, ks in ((NH - 3, range(0, 2)), (NH - 2, range(2, 4)), (NH - 1, range(4, 6)), (NH, range(6, NH))):
            @pl.when(i == first)
            def _():
                for k in ks:
                    ag_last(xa_ref, xs, xr, k)

        @pl.when(i < NH)
        def _():
            ag_mid(xa_ref, xs, xr, i)
            w_load(i, 0).wait()
            w_load(i, 1).wait()
            slot = (i + 1) % 2
            for b in range(per):
                t_block(pl.multiple_of(jnp.minimum(per * i + b, blocks - 1) * 128, 128))
            p = jnp.dot(duv[...], wbuf[slot], preferred_element_type=F32)
            dyv[:, :, :, cols(i)] = p.astype(BF16).reshape(4, 2, tok, hc)

            @pl.when(i + 2 < NH)
            def _():
                w_load(i + 2, 0).start()
                w_load(i + 2, 1).start()

        @pl.when(i < NH)
        def _():
            rs0(i, 1 - tc).start()

        @pl.when((i >= 1) & (i <= NH))
        def _():
            k = i - 1
            rs0(k, tc).wait_recv()
            for q in range(4):
                add(2 * q + tc, k, r0v[k, q])

            @pl.when(k < half)
            def _():
                rs1(k).start()

            @pl.when(k >= half)
            def _():
                for o in sums_out(k, True):
                    o.start()

        @pl.when((i >= half) & (i < NH))
        def _():
            k = i - half
            rs1(k).wait_recv()
            add(n2(k), k, r1v[k])
            for o in sums_out(k, False):
                o.start()

        return carry

    lax.fori_loop(0, NH + 1, phase2, 0)
    outs = [pltpu.make_async_copy(v.at[pl.ds(0, ff), :], ref, ol.at[i])
            for i, (v, ref) in enumerate(((ugv, dgt_ref), (uuv, dut_ref)))]
    for o in outs:
        o.start()

    def drain(k, carry):
        ag_end(xa_ref, xs, xr, k)
        return carry

    lax.fori_loop(0, NH, drain, 0)
    for n in range(7):
        left(xa_ref.at[0, 0], xs.at[n])
    left(dyv.at[:, 0], rs.at[0])
    left(dyv.at[0, 0, :, pl.ds(0, hid // 2)], rs.at[1])
    x_put.wait()
    for n, ref in enumerate((so_ref, sx_ref, sy_ref, sd_ref)):
        pltpu.make_async_copy(ref, ref, po.at[n]).wait()
    for o in outs:
        o.wait()


def _row_chunks(ff):
    n = ff // 16
    size = -(-n // 4)
    return [16 * min(size, n - i) for i in range(0, n, size)]


def _weight_kernel(zt_ref, dgt_ref, dut_ref, dy_ref, x_ref, part_ref, dd_ref, dg_ref, du_ref,
                   zv, dgv, duv, yv, xv, o0, o1, o2, cv, ls, ysem, xsem, os, ci, co):
    ff, tall = zt_ref.shape
    hid = dy_ref.shape[1]
    nb = yv.shape[-1]
    n = hid // nb
    sizes = _row_chunks(ff)
    depth = tall // 256

    def load(src, dst, sem, j, p):
        lo = pl.ds(pl.multiple_of(j * nb + p * 512, 512), 512)
        return pltpu.make_async_copy(src.at[:, lo], dst.at[j % 2, :, p * 512:p * 512 + 512], sem.at[j % 2, p])

    def y_loads(j):
        return [load(dy_ref, yv, ysem, j, p) for p in range(nb // 512)]

    def x_loads(j):
        return [load(x_ref, xv, xsem, j, p) for p in range(nb // 512)]

    def put(i, j, rows, width, p):
        stage, out = ((o0, dd_ref), (o1, dg_ref), (o2, du_ref))[i]
        lo = pl.ds(pl.multiple_of(j * nb + p * 512, 512), width)
        slot = j % stage.shape[0]
        return pltpu.make_async_copy(stage.at[slot, rows, p * 512:p * 512 + width], out.at[rows, lo], os.at[i, slot])

    def put_all(i, j):
        return put(i, j, pl.ds(0, ff), nb, 0)

    def product(i, j, accs, waits):
        a = (zv, dgv, duv)[i]
        b = (yv, xv, xv)[i].at[j % 2]
        stage = (o0, o1, o2)[i]
        slot = j % stage.shape[0]
        steps = []
        for pair in range(nb // 512):
            row = 0
            for c, size in enumerate(sizes):
                for kt in range(depth):
                    steps.append((pair, c, row, size, kt))
                row += size

        def push(s):
            pair, _, _, _, kt = steps[s]
            for q in range(2):
                lo = pair * 512 + q * 256
                pltpu.matmul_push_rhs(b[kt * 256:kt * 256 + 256, lo:lo + 256], s % 2, q)

        def pop(pair, c, row, size):
            for q in range(2):
                lo = pair * 512 + q * 256
                stage[slot, row:row + size, lo:lo + 256] = pltpu.matmul_pop(accs[q][c])
            put(i, j, pl.ds(row, size), 512, pair).start()

        late = None
        for s, (pair, c, row, size, kt) in enumerate(steps):
            if s == 0 or (c == 0 and kt == 0 and waits):
                for w in waits[pair] if waits else ():
                    w.wait()
                push(s)
            if s + 1 < len(steps) and not (waits and steps[s + 1][1] == 0 and steps[s + 1][4] == 0):
                push(s + 1)
            block = a[row:row + size, kt * 256:kt * 256 + 256]
            for q in range(2):
                pltpu.matmul_acc_lhs(accs[q][c], block, load_staged_rhs=s % 2)
            if kt == 0 and late is not None:
                pop(*late)
            if kt == depth - 1:
                late = (pair, c, row, size)
        pop(*late)

    def take(p):
        return pltpu.make_async_copy(part_ref.at[:, p * 512:p * 512 + 512], cv.at[p], ci.at[p])

    def give(p):
        return pltpu.make_async_copy(cv.at[p], dd_ref.at[:, p * 512:p * 512 + 512], co.at[p])

    zl, gl, ul = (pltpu.make_async_copy(src, dst, ls.at[i])
                  for i, (src, dst) in enumerate(((zt_ref, zv), (dgt_ref, dgv), (dut_ref, duv))))
    parts = range(nb // 512)
    first = x_loads(0)
    gl.start()
    for c in first:
        c.start()
    ul.start()
    zl.start()
    for c in y_loads(1) + x_loads(1):
        c.start()
    for p in parts:
        take(p).start()

    def body(*flat):
        h = len(flat) // 2
        accs = [[part[2] if i == len(sizes) - 1 else part[i % 2] for i in range(len(sizes))]
                for part in (flat[:h], flat[h:])]
        product(1, 0, accs, [[gl, first[0]], first[1:]])
        product(2, 0, accs, [[ul], []])
        zl.wait()
        for p in parts:
            take(p).wait()
            give(p).start()

        def rest(j, carry):
            for c in y_loads(j) + x_loads(j):
                c.wait()

            @pl.when(j + 1 < n)
            def _():
                for c in y_loads(j + 1) + x_loads(j + 1):
                    c.start()

            @pl.when(j >= 2)
            def _():
                put_all(0, j - 1).wait()
                put_all(2, j - 2).wait()

            put_all(1, j - 1).wait()
            for i in range(3):
                product(i, j, accs, None)
            return carry

        lax.fori_loop(1, n, rest, 0)

    pl.run_scoped(body, *[pltpu.ACC(q)((size, 256), F32) for q in range(2) for size in (sizes[0], sizes[0], sizes[-1])])
    put_all(0, n - 1).wait()
    put_all(1, n - 1).wait()
    put_all(2, n - 2).wait()
    put_all(2, n - 1).wait()
    for p in parts:
        give(p).wait()


def _weight_grads(zt, dgt, dut, dy, x, part):
    ff, tall = zt.shape
    hid = x.shape[1]
    nb = 1024
    sem = pltpu.SemaphoreType.DMA
    any_ = pl.BlockSpec(memory_space=pltpu.HBM)
    return pl.pallas_call(
        _weight_kernel,
        out_shape=(jax.ShapeDtypeStruct((ff, hid), F32),) * 3,
        in_specs=[any_] * 6,
        out_specs=(any_,) * 3,
        scratch_shapes=[pltpu.VMEM((ff, tall), BF16)] * 3 + [pltpu.VMEM((2, tall, nb), BF16)] * 2
        + [pltpu.VMEM((k, ff, nb), F32) for k in (1, 1, 2)] + [pltpu.VMEM((nb // 512, ff, 512), F32)]
        + [sem((3,)), sem((2, 2)), sem((2, 2)), sem((3, 2)), sem((2,)), sem((2,))],
        compiler_params=pltpu.CompilerParams(vmem_limit_bytes=54 * 2 ** 20),
        cost_estimate=pl.CostEstimate(flops=6 * ff * tall * hid, bytes_accessed=12 * ff * hid, transcendentals=0),
        name="weight_grads",
    )(zt, dgt, dut, dy, x, part)


def solution(mesh):
    def local_backward(x, wg, wu, wd, ug, uu, dy):
        tok, hid = dy.shape
        ff = wd.shape[0]
        fp = _lanes(ff)
        tall = 8 * tok
        hc = hid // NH
        any_ = pl.BlockSpec(memory_space=pl.ANY)
        sem = pltpu.SemaphoreType.DMA
        full = jax.ShapeDtypeStruct((4, 2, tok, hid), BF16)
        act = jax.ShapeDtypeStruct((ff, tall), BF16)
        own = jax.ShapeDtypeStruct((tok, hid), BF16)
        half = jax.ShapeDtypeStruct((tok, hid // 2), BF16)
        so, sx, sy, sd, zt, dgt, dut, dya, xa, ddp = pl.pallas_call(
            _comm_kernel,
            out_shape=(own, own, own, half, act, act, act, full, full,
                       jax.ShapeDtypeStruct((ff, DOWN * hc), F32)),
            in_specs=[any_] * 7,
            out_specs=(any_,) * 10,
            scratch_shapes=[
                pltpu.VMEM((4, 2, tok, hid), BF16),
                pltpu.VMEM((tall, fp), F32),
                pltpu.VMEM((tall, fp), F32),
                pltpu.VMEM((tall, fp), F32),
                pltpu.VMEM((tall, fp), BF16),
                pltpu.VMEM((tall, 2 * fp), BF16),
                pltpu.VMEM((2, 2 * fp, hc), BF16),
                pltpu.VMEM((fp, tall), BF16),
                pltpu.VMEM((fp, tall), BF16),
                pltpu.VMEM((NH, 4, tok, hc), BF16),
                pltpu.VMEM((NH // 2, tok, hc), BF16),
                pltpu.VMEM((tok, hid), BF16),
                pltpu.VMEM((2, ff, hc), F32),
                sem((7,)), sem((NY, 3)), sem((7,)), sem((NH, 3)), sem((2,)), sem((NH,)), sem((NH // 2,)),
                sem((NY // AHEAD,)), sem((2,)), sem((2, 2)), sem((2,)), sem((2,)), sem((1,)), sem((4,)), sem((2,)),
            ],
            compiler_params=pltpu.CompilerParams(collective_id=0, has_side_effects=True, vmem_limit_bytes=67043328),
            name="gather_partial",
        )(x, dy, wd, wg.T, wu.T, ug.T, uu.T)
        dya = dya.reshape(tall, hid)
        xa = xa.reshape(tall, hid)

        def to(v, flip):
            return lax.ppermute(v, 'tp', [(i, i ^ flip) for i in range(8)])

        fx, fy, fd = to(sx, 2), to(sy, 4), to(sd, 6)
        zt, dgt, dut, ddp = (pltpu.with_memory_space_constraint(v, pltpu.HBM) for v in (zt, dgt, dut, ddp))
        dwd, dwg, dwu = _weight_grads(zt, dgt, dut, dya, xa, ddp)
        fx, fy, fd, dwd, dwg, dwu = lax.optimization_barrier((fx, fy, fd, dwd, dwg, dwu))
        right = jnp.pad(fd, ((0, 0), (hid // 2, 0)))
        dx = sum(v.astype(F32) for v in (so, fx, fy, right)).astype(BF16)
        return dx, dwg.T, dwu.T, dwd

    tok_spec = P(('dp', 'tp'), None)
    col_spec = P(None, 'tp')
    act_spec = P('dp', 'tp')
    return jax.shard_map(local_backward, mesh=mesh,
                         in_specs=(tok_spec, col_spec, col_spec, P('tp', None), act_spec, act_spec, tok_spec),
                         out_specs=(tok_spec, act_spec, act_spec, tok_spec),
                         check_vma=False)
```

```python
import functools

import jax
import jax.numpy as jnp
from jax import lax
from jax.experimental import pallas as pl
from jax.experimental.pallas import tpu as pltpu
from jax.sharding import PartitionSpec as P

MESH = pl.DeviceIdType.MESH
BF16 = jnp.bfloat16
F32 = jnp.float32
NH = 8
DOWN = 2
NY = 16
AHEAD, LAG, TAKE = 4, 4, 6
NT = (((1,), (1,)), ((), ()))


def _lanes(n):
    return (n + 127) // 128 * 128


def _comm_kernel(x_ref, dy_ref, wd_ref, wg_ref, wu_ref, ug_ref, uu_ref,
                 so_ref, sx_ref, sy_ref, sd_ref, zt_ref, dgt_ref, dut_ref, dya_ref, xa_ref, dd_ref,
                 dyv, gv, av, spv, utv, duv, wbuf, ugv, uuv, r0v, r1v, xov, ddv,
                 ys, yr, xs, xr, rs, rr, r1r, yl, xl, wl, ul, ol, dl, po, pd):
    tok, hid = dy_ref.shape
    ff = wd_ref.shape[0]
    fp = _lanes(ff)
    nfull, rest = ff // 128, ff % 128
    hc = hid // NH
    tall = 8 * tok
    half = NH // 2

    t = lax.axis_index("tp")
    ty, tx, tc = t // 4, (t // 2) % 2, t % 2
    xn = t + 2 - 4 * tx
    yn = t + 4 - 8 * ty
    dg = xn + yn - t
    pn = t + 1 - 2 * tc

    def n1(k):
        return xn + (yn - xn) * (k % 2)

    def n2(k):
        return yn + (xn - yn) * (k % 2)

    hy = hid // NY
    per_h = NY // NH

    def cols(k, w=hc):
        return pl.ds(pl.multiple_of(k * w, w), w)

    def blk(ref, owner, k, w=hc):
        return ref.at[owner // 2, owner % 2, :, cols(k, w)]

    def rcopy(src, dst, ss, rs_, dev):
        return pltpu.make_async_remote_copy(src_ref=src, dst_ref=dst, send_sem=ss, recv_sem=rs_,
                                            device_id={"tp": dev}, device_id_type=MESH)

    def ag(buf, ss, sr, k, j, owner, dev):
        w = hid // sr.shape[0]
        return rcopy(blk(buf, owner, k, w), blk(buf, owner, k, w), ss.at[j], sr.at[k, (0, 1, 1, 2, 2, 2, 2)[j]], dev)

    def arrived(ref, sem):
        rcopy(ref, ref, sem, sem, t).wait_recv()

    def left(ref, sem):
        rcopy(ref, ref, sem, sem, t).wait_send()

    def ag_own(buf, ss, sr, k):
        ag(buf, ss, sr, k, 0, t, n1(k)).start()
        ag(buf, ss, sr, k, 1, t, n2(k)).start()
        ag(buf, ss, sr, k, 3, t, pn).start()

    def x_own(k, j, dev):
        return rcopy(xov.at[:, cols(k)], blk(xa_ref, t, k), xs.at[j], xr.at[k, (0, 1, 1, 2)[j]], dev)

    def x_send(k):
        x_own(k, 0, n1(k)).start()
        x_own(k, 1, n2(k)).start()
        x_own(k, 3, pn).start()

    def ag_mid(buf, ss, sr, k):
        ag(buf, ss, sr, k, 0, n1(k), n1(k)).wait_recv()
        ag(buf, ss, sr, k, 2, n1(k), n2(k)).start()
        ag(buf, ss, sr, k, 4, n1(k), pn).start()

    def ag_last(buf, ss, sr, k):
        w = hid // sr.shape[0]
        arrived(buf.at[pl.ds(0, 2), 0, :, cols(k, w)], sr.at[k, 1])
        ag(buf, ss, sr, k, 5, n2(k), pn).start()
        ag(buf, ss, sr, k, 6, dg, pn).start()

    def ag_end(buf, ss, sr, k):
        w = hid // sr.shape[0]
        arrived(buf.at[:, 0, :, cols(k, w)], sr.at[k, 2])

    def y_local(g):
        w = AHEAD * hy
        return pltpu.make_async_copy(dy_ref.at[:, cols(g, w)], blk(dyv, t, g, w), yl.at[g])

    x_local = pltpu.make_async_copy(x_ref, xov, xl.at[0])
    x_put = pltpu.make_async_copy(xov, xa_ref.at[t // 2, t % 2], xl.at[1])

    def down_out(k):
        return pltpu.make_async_copy(ddv.at[k % 2], dd_ref.at[:, cols(k)], pd.at[k % 2])

    def wd_load(k):
        return pltpu.make_async_copy(wd_ref.at[:, cols(k)], wbuf.at[0, pl.ds(pl.multiple_of(k % 2 * fp, fp), ff), :], wl.at[0, k % 2])

    def w_load(k, j):
        src = (wg_ref, wu_ref)[j]
        return pltpu.make_async_copy(src.at[:, cols(k)], wbuf.at[(k + 1) % 2, pl.ds(j * fp, ff), :],
                                     wl.at[(k + 1) % 2, j])

    def dy_out(k):
        return pltpu.make_async_copy(dyv.at[:, :, :, cols(k)], dya_ref.at[:, :, :, cols(k)], dl.at[0])

    ug_in = pltpu.make_async_copy(ug_ref, ugv.at[pl.ds(0, ff), :], ul.at[0])
    uu_in = pltpu.make_async_copy(uu_ref, uuv.at[pl.ds(0, ff), :], ul.at[1])
    for g in range(NY // AHEAD):
        y_local(g).start()
    wd_load(0).start()
    wd_load(1).start()
    ug_in.start()
    uu_in.start()
    x_local.start()

    barrier = pltpu.get_barrier_semaphore()
    for dev in (xn, yn, pn):
        pl.semaphore_signal(barrier, inc=1, device_id={"tp": dev}, device_id_type=MESH)
    pl.semaphore_wait(barrier, 3)

    y_local(0).wait()
    for k in range(AHEAD):
        ag_own(dyv, ys, yr, k)

    for a in range(2):
        for b in range(2):
            wbuf[a, b * fp + ff:b * fp + fp, :] = jnp.zeros((fp - ff, hc), BF16)
    gv[...] = jnp.zeros_like(gv)
    ug_in.wait()
    uu_in.wait()

    def u_block(r0, n):
        rows = pl.ds(r0, n)
        ug = ugv[rows, :].astype(F32)
        ub = uuv[rows, :]
        uu = ub.astype(F32)
        s = jax.nn.sigmoid(ug)
        a = ug * s
        sp = s * (1.0 + ug * (1.0 - s))
        ugv[rows, :] = (a * uu).astype(BF16)
        if n < 128:
            pad = jnp.zeros((128 - n, tall), F32)
            a = jnp.concatenate([a, pad], axis=0)
            sp = jnp.concatenate([sp, pad], axis=0)
            uu = jnp.concatenate([uu, pad], axis=0)
        lanes = pl.ds(r0, 128)
        av[:, lanes] = a.T
        spv[:, lanes] = sp.T
        utv[:, lanes] = uu.T.astype(BF16)

    down0 = -(-(fp // 128) // per_h) * per_h

    def phase1(i, carry):
        @pl.when((i < NY - AHEAD) & (i % AHEAD == 0))
        def _():
            y_local(i // AHEAD + 1).wait()

        @pl.when(i < NY - AHEAD)
        def _():
            ag_own(dyv, ys, yr, i + AHEAD)

        @pl.when(i < NY)
        def _():
            ag_mid(dyv, ys, yr, i)

        @pl.when(i >= NY + TAKE - NH)
        def _():
            x_send(i - (NY + TAKE - NH))

        @pl.when(i < nfull)
        def _():
            u_block(pl.multiple_of(i * 128, 128), 128)

        if rest:
            @pl.when(i == nfull)
            def _():
                u_block(nfull * 128, rest)

        @pl.when((i >= LAG) & (i < NY + LAG))
        def _():
            ag_last(dyv, ys, yr, i - LAG)

        @pl.when(i >= TAKE)
        def _():
            ag_end(dyv, ys, yr, i - TAKE)

        @pl.when((i >= TAKE) & ((i - TAKE) % per_h == per_h - 1))
        def _():
            k = (i - TAKE) // per_h
            dy_out(k).start()
            wd_load(k).wait()
            dyc = dyv[:, :, :, cols(k)].reshape(tall, hc)
            for n in range(0, fp, 256):
                w = min(256, fp - n)
                gv[:, n:n + w] += lax.dot_general(dyc, wbuf[0, pl.ds(pl.multiple_of(k % 2 * fp + n, 128), w), :], NT, preferred_element_type=F32)

            @pl.when(k + 2 < NH)
            def _():
                wd_load(k + 2).start()

        @pl.when((i >= down0) & ((i - down0) % per_h == 0) & (i < down0 + DOWN * per_h))
        def _():
            k = (i - down0) // per_h

            @pl.when(k >= 2)
            def _():
                down_out(k - 2).wait()

            dyc = dyv[:, :, :, cols(k)].reshape(tall, hc)
            ddv[k % 2] = jnp.dot(ugv[:ff, :], dyc, preferred_element_type=F32)
            down_out(k).start()

        return carry

    w_load(0, 0).start()
    w_load(0, 1).start()
    x_local.wait()
    x_put.start()
    lax.fori_loop(0, NY + TAKE, phase1, 0)
    w_load(1, 0).start()
    w_load(1, 1).start()
    zt_out = pltpu.make_async_copy(ugv.at[pl.ds(0, ff), :], zt_ref, ol.at[0])
    zt_out.start()
    def gates(i, carry):
        rows = pl.ds(pl.multiple_of(i * 128, 128), 128)
        g = gv[rows, :]
        duv[rows, :fp] = (g * utv[rows, :].astype(F32) * spv[rows, :]).astype(BF16)
        duv[rows, fp:] = (g * av[rows, :]).astype(BF16)
        return carry

    lax.fori_loop(0, tall // 128, gates, 0)

    for n in range(7):
        left(dyv.at[0, 0], ys.at[n])
    pltpu.make_async_copy(dyv, dya_ref, dl.at[0]).wait()
    zt_out.wait()
    for k in range(DOWN - 2, DOWN):
        down_out(k).wait()

    def rs0(k, c):
        return rcopy(dyv.at[:, c, :, cols(k)], r0v.at[k], rs.at[0], rr.at[k], pn)

    def rs1(k):
        return rcopy(blk(dyv, dg, k), r1v.at[k], rs.at[1], r1r.at[k], n1(k))

    def sums_out(k, diagonal):
        outs = [(so_ref, t, k), (sx_ref, xn, k), (sy_ref, yn, k)] + ([(sd_ref, dg, k - half)] if diagonal else [])
        return [pltpu.make_async_copy(blk(dyv, owner, k), ref.at[:, cols(c)], po.at[i])
                for i, (ref, owner, c) in enumerate(outs)]

    def add(owner, k, other):
        b = blk(dyv, owner, k)
        b[...] = (b[...].astype(F32) + other.astype(F32)).astype(BF16)

    def t_block(r0):
        rows = pl.ds(r0, 128)
        ugv[rows, :] = duv[:, rows].T
        uuv[rows, :] = duv[:, pl.ds(fp + r0, 128)].T

    blocks = fp // 128
    per = -(-blocks // NH)

    def phase2(i, carry):
        for first, ks in ((NH - 1, range(0, 3)), (NH, range(3, NH))):
            @pl.when(i == first)
            def _():
                for k in ks:
                    ag_last(xa_ref, xs, xr, k)

        @pl.when(i < NH - 1)
        def _():
            ag_mid(xa_ref, xs, xr, i + 1)

        @pl.when(i < NH)
        def _():
            w_load(i, 0).wait()
            w_load(i, 1).wait()
            slot = (i + 1) % 2
            for b in range(per):
                t_block(pl.multiple_of(jnp.minimum(per * i + b, blocks - 1) * 128, 128))
            p = jnp.dot(duv[...], wbuf[slot], preferred_element_type=F32)
            dyv[:, :, :, cols(i)] = p.astype(BF16).reshape(4, 2, tok, hc)

            @pl.when(i + 2 < NH)
            def _():
                w_load(i + 2, 0).start()
                w_load(i + 2, 1).start()

        @pl.when(i < NH)
        def _():
            rs0(i, 1 - tc).start()

        @pl.when((i >= 1) & (i <= NH))
        def _():
            k = i - 1
            rs0(k, tc).wait_recv()
            for q in range(4):
                add(2 * q + tc, k, r0v[k, q])

            @pl.when(k < half)
            def _():
                rs1(k).start()

            @pl.when(k >= half)
            def _():
                for o in sums_out(k, True):
                    o.start()

        @pl.when(i >= NH + 1 - half)
        def _():
            k = i - (NH + 1 - half)
            rs1(k).wait_recv()
            add(n2(k), k, r1v[k])
            for o in sums_out(k, False):
                o.start()

        return carry

    ag_mid(xa_ref, xs, xr, 0)
    lax.fori_loop(0, NH + 1, phase2, 0)
    outs = [pltpu.make_async_copy(v.at[pl.ds(0, ff), :], ref, ol.at[i])
            for i, (v, ref) in enumerate(((ugv, dgt_ref), (uuv, dut_ref)))]
    for o in outs:
        o.start()

    def drain(k, carry):
        ag_end(xa_ref, xs, xr, k)
        return carry

    lax.fori_loop(0, NH, drain, 0)
    for n in range(7):
        left(xa_ref.at[0, 0], xs.at[n])
    left(dyv.at[:, 0], rs.at[0])
    left(dyv.at[0, 0, :, pl.ds(0, hid // 2)], rs.at[1])
    x_put.wait()
    for n, ref in enumerate((so_ref, sx_ref, sy_ref, sd_ref)):
        pltpu.make_async_copy(ref, ref, po.at[n]).wait()
    for o in outs:
        o.wait()


def _row_chunks(ff):
    n = ff // 16
    size = -(-n // 4)
    return [16 * min(size, n - i) for i in range(0, n, size)]


def _weight_kernel(zt_ref, dgt_ref, dut_ref, dy_ref, x_ref, part_ref, dd_ref, dg_ref, du_ref,
                   zv, dgv, duv, yv, xv, o0, o1, o2, cv, ls, ysem, xsem, os, ci, co):
    ff, tall = zt_ref.shape
    hid = dy_ref.shape[1]
    nb = yv.shape[-1]
    n = hid // nb
    sizes = _row_chunks(ff)
    depth = tall // 256

    def load(src, dst, sem, j, p):
        lo = pl.ds(pl.multiple_of(j * nb + p * 512, 512), 512)
        return pltpu.make_async_copy(src.at[:, lo], dst.at[j % 2, :, p * 512:p * 512 + 512], sem.at[j % 2, p])

    def y_loads(j):
        return [load(dy_ref, yv, ysem, j, p) for p in range(nb // 512)]

    def x_loads(j):
        return [load(x_ref, xv, xsem, j, p) for p in range(nb // 512)]

    def put(i, j, rows, width, p):
        stage, out = ((o0, dd_ref), (o1, dg_ref), (o2, du_ref))[i]
        lo = pl.ds(pl.multiple_of(j * nb + p * 512, 512), width)
        slot = j % stage.shape[0]
        return pltpu.make_async_copy(stage.at[slot, rows, p * 512:p * 512 + width], out.at[rows, lo], os.at[i, slot])

    def put_all(i, j):
        return put(i, j, pl.ds(0, ff), nb, 0)

    def product(i, j, accs, waits):
        a = (zv, dgv, duv)[i]
        b = (yv, xv, xv)[i].at[j % 2]
        stage = (o0, o1, o2)[i]
        slot = j % stage.shape[0]
        steps = []
        for pair in range(nb // 512):
            row = 0
            for c, size in enumerate(sizes):
                for kt in range(depth):
                    steps.append((pair, c, row, size, kt))
                row += size

        def push(s):
            pair, _, _, _, kt = steps[s]
            for q in range(2):
                lo = pair * 512 + q * 256
                pltpu.matmul_push_rhs(b[kt * 256:kt * 256 + 256, lo:lo + 256], s % 2, q)

        def pop(pair, c, row, size):
            for q in range(2):
                lo = pair * 512 + q * 256
                stage[slot, row:row + size, lo:lo + 256] = pltpu.matmul_pop(accs[q][c])
            put(i, j, pl.ds(row, size), 512, pair).start()

        late = None
        for s, (pair, c, row, size, kt) in enumerate(steps):
            if s == 0 or (c == 0 and kt == 0 and waits):
                for w in waits[pair] if waits else ():
                    w.wait()
                push(s)
            if s + 1 < len(steps) and not (waits and steps[s + 1][1] == 0 and steps[s + 1][4] == 0):
                push(s + 1)
            block = a[row:row + size, kt * 256:kt * 256 + 256]
            for q in range(2):
                pltpu.matmul_acc_lhs(accs[q][c], block, load_staged_rhs=s % 2)
            if kt == 0 and late is not None:
                pop(*late)
            if kt == depth - 1:
                late = (pair, c, row, size)
        pop(*late)

    def take(p):
        return pltpu.make_async_copy(part_ref.at[:, p * 512:p * 512 + 512], cv.at[p], ci.at[p])

    def give(p):
        return pltpu.make_async_copy(cv.at[p], dd_ref.at[:, p * 512:p * 512 + 512], co.at[p])

    zl, gl, ul = (pltpu.make_async_copy(src, dst, ls.at[i])
                  for i, (src, dst) in enumerate(((zt_ref, zv), (dgt_ref, dgv), (dut_ref, duv))))
    parts = range(nb // 512)
    first = x_loads(0)
    gl.start()
    for c in first:
        c.start()
    ul.start()
    zl.start()
    for c in y_loads(1) + x_loads(1):
        c.start()

    def body(*flat):
        h = len(flat) // 2
        accs = [[part[2] if i == len(sizes) - 1 else part[i % 2] for i in range(len(sizes))]
                for part in (flat[:h], flat[h:])]
        product(1, 0, accs, [[gl, first[0]], first[1:]])
        product(2, 0, accs, [[ul], []])
        zl.wait()

        def rest(j, carry):
            for c in y_loads(j) + x_loads(j):
                c.wait()

            @pl.when(j + 1 < n)
            def _():
                for c in y_loads(j + 1) + x_loads(j + 1):
                    c.start()

            @pl.when(j == 1)
            def _():
                for p in parts:
                    take(p).start()

            @pl.when(j == 2)
            def _():
                for p in parts:
                    take(p).wait()
                    give(p).start()

            @pl.when(j >= 2)
            def _():
                put_all(0, j - 1).wait()
                put_all(2, j - 2).wait()

            put_all(1, j - 1).wait()
            for i in range(3):
                product(i, j, accs, None)
            return carry

        lax.fori_loop(1, n, rest, 0)

    pl.run_scoped(body, *[pltpu.ACC(q)((size, 256), F32) for q in range(2) for size in (sizes[0], sizes[0], sizes[-1])])
    put_all(0, n - 1).wait()
    put_all(1, n - 1).wait()
    put_all(2, n - 2).wait()
    put_all(2, n - 1).wait()
    for p in parts:
        give(p).wait()


def _weight_grads(zt, dgt, dut, dy, x, part):
    ff, tall = zt.shape
    hid = x.shape[1]
    nb = 1024
    sem = pltpu.SemaphoreType.DMA
    any_ = pl.BlockSpec(memory_space=pltpu.HBM)
    return pl.pallas_call(
        _weight_kernel,
        out_shape=(jax.ShapeDtypeStruct((ff, hid), F32),) * 3,
        in_specs=[any_] * 6,
        out_specs=(any_,) * 3,
        scratch_shapes=[pltpu.VMEM((ff, tall), BF16)] * 3 + [pltpu.VMEM((2, tall, nb), BF16)] * 2
        + [pltpu.VMEM((k, ff, nb), F32) for k in (1, 1, 2)] + [pltpu.VMEM((nb // 512, ff, 512), F32)]
        + [sem((3,)), sem((2, 2)), sem((2, 2)), sem((3, 2)), sem((2,)), sem((2,))],
        compiler_params=pltpu.CompilerParams(vmem_limit_bytes=54 * 2 ** 20),
        cost_estimate=pl.CostEstimate(flops=6 * ff * tall * hid, bytes_accessed=12 * ff * hid, transcendentals=0),
        name="weight_grads",
    )(zt, dgt, dut, dy, x, part)


def solution(mesh):
    def local_backward(x, wg, wu, wd, ug, uu, dy):
        tok, hid = dy.shape
        ff = wd.shape[0]
        fp = _lanes(ff)
        tall = 8 * tok
        hc = hid // NH
        any_ = pl.BlockSpec(memory_space=pl.ANY)
        sem = pltpu.SemaphoreType.DMA
        full = jax.ShapeDtypeStruct((4, 2, tok, hid), BF16)
        act = jax.ShapeDtypeStruct((ff, tall), BF16)
        own = jax.ShapeDtypeStruct((tok, hid), BF16)
        half = jax.ShapeDtypeStruct((tok, hid // 2), BF16)
        so, sx, sy, sd, zt, dgt, dut, dya, xa, ddp = pl.pallas_call(
            _comm_kernel,
            out_shape=(own, own, own, half, act, act, act, full, full,
                       jax.ShapeDtypeStruct((ff, DOWN * hc), F32)),
            in_specs=[any_] * 7,
            out_specs=(any_,) * 10,
            scratch_shapes=[
                pltpu.VMEM((4, 2, tok, hid), BF16),
                pltpu.VMEM((tall, fp), F32),
                pltpu.VMEM((tall, fp), F32),
                pltpu.VMEM((tall, fp), F32),
                pltpu.VMEM((tall, fp), BF16),
                pltpu.VMEM((tall, 2 * fp), BF16),
                pltpu.VMEM((2, 2 * fp, hc), BF16),
                pltpu.VMEM((fp, tall), BF16),
                pltpu.VMEM((fp, tall), BF16),
                pltpu.VMEM((NH, 4, tok, hc), BF16),
                pltpu.VMEM((NH // 2, tok, hc), BF16),
                pltpu.VMEM((tok, hid), BF16),
                pltpu.VMEM((2, ff, hc), F32),
                sem((7,)), sem((NY, 3)), sem((7,)), sem((NH, 3)), sem((2,)), sem((NH,)), sem((NH // 2,)),
                sem((NY // AHEAD,)), sem((2,)), sem((2, 2)), sem((2,)), sem((2,)), sem((1,)), sem((4,)), sem((2,)),
            ],
            compiler_params=pltpu.CompilerParams(collective_id=0, has_side_effects=True, vmem_limit_bytes=67043328),
            name="gather_partial",
        )(x, dy, wd, wg.T, wu.T, ug.T, uu.T)
        dya = dya.reshape(tall, hid)
        xa = xa.reshape(tall, hid)

        def to(v, flip):
            return lax.ppermute(v, 'tp', [(i, i ^ flip) for i in range(8)])

        fx, fy, fd = to(sx, 2), to(sy, 4), to(sd, 6)
        zt, dgt, dut, ddp = (pltpu.with_memory_space_constraint(v, pltpu.HBM) for v in (zt, dgt, dut, ddp))
        dwd, dwg, dwu = _weight_grads(zt, dgt, dut, dya, xa, ddp)
        fx, fy, fd, dwd, dwg, dwu = lax.optimization_barrier((fx, fy, fd, dwd, dwg, dwu))
        right = jnp.pad(fd, ((0, 0), (hid // 2, 0)))
        dx = sum(v.astype(F32) for v in (so, fx, fy, right)).astype(BF16)
        return dx, dwg.T, dwu.T, dwd

    tok_spec = P(('dp', 'tp'), None)
    col_spec = P(None, 'tp')
    act_spec = P('dp', 'tp')
    return jax.shard_map(local_backward, mesh=mesh,
                         in_specs=(tok_spec, col_spec, col_spec, P('tp', None), act_spec, act_spec, tok_spec),
                         out_specs=(tok_spec, act_spec, act_spec, tok_spec),
                         check_vma=False)
```

```python
import functools

import jax
import jax.numpy as jnp
from jax import lax
from jax.experimental import pallas as pl
from jax.experimental.pallas import tpu as pltpu
from jax.sharding import PartitionSpec as P

MESH = pl.DeviceIdType.MESH
BF16 = jnp.bfloat16
F32 = jnp.float32
NH = 8
HOPS = 2
DOWN = 2
NY = 16
AHEAD, LAG, TAKE = 4, 4, 6
NT = (((1,), (1,)), ((), ()))


def _lanes(n):
    return (n + 127) // 128 * 128


def _comm_kernel(x_ref, dy_ref, wd_ref, wg_ref, wu_ref, ug_ref, uu_ref,
                 so_ref, sx_ref, sy_ref, sd_ref, zt_ref, dgt_ref, dut_ref, dya_ref, xa_ref, dd_ref,
                 dyv, gv, av, spv, utv, duv, wbuf, ugv, uuv, r0v, r1v, xov, ddv,
                 ys, yr, xs, xr, rs, rr, r1r, yl, xl, wl, ul, ol, dl, po, pd):
    tok, hid = dy_ref.shape
    ff = wd_ref.shape[0]
    fp = _lanes(ff)
    nfull, rest = ff // 128, ff % 128
    hc = hid // NH
    tall = 8 * tok

    t = lax.axis_index("tp")
    ty, tx, tc = t // 4, (t // 2) % 2, t % 2
    xn = t + 2 - 4 * tx
    yn = t + 4 - 8 * ty
    dg = xn + yn - t
    pn = t + 1 - 2 * tc

    def n1(k):
        return xn + (yn - xn) * (k % 2)

    def n2(k):
        return yn + (xn - yn) * (k % 2)

    hy = hid // NY
    per_h = NY // NH

    def cols(k, w=hc):
        return pl.ds(pl.multiple_of(k * w, w), w)

    def blk(ref, owner, k, w=hc):
        return ref.at[owner // 2, owner % 2, :, cols(k, w)]

    def rcopy(src, dst, ss, rs_, dev):
        return pltpu.make_async_remote_copy(src_ref=src, dst_ref=dst, send_sem=ss, recv_sem=rs_,
                                            device_id={"tp": dev}, device_id_type=MESH)

    def ag(buf, ss, sr, k, j, owner, dev):
        w = hid // sr.shape[0]
        return rcopy(blk(buf, owner, k, w), blk(buf, owner, k, w), ss.at[j], sr.at[k, (0, 1, 1, 2, 2, 2, 2)[j]], dev)

    def arrived(ref, sem):
        rcopy(ref, ref, sem, sem, t).wait_recv()

    def left(ref, sem):
        rcopy(ref, ref, sem, sem, t).wait_send()

    def ag_own(buf, ss, sr, k):
        ag(buf, ss, sr, k, 0, t, n1(k)).start()
        ag(buf, ss, sr, k, 1, t, n2(k)).start()
        ag(buf, ss, sr, k, 3, t, pn).start()

    def x_own(k, j, dev):
        return rcopy(xov.at[:, cols(k)], blk(xa_ref, t, k), xs.at[j], xr.at[k, (0, 1, 1, 2)[j]], dev)

    def x_send(k):
        x_own(k, 0, n1(k)).start()
        x_own(k, 1, n2(k)).start()
        x_own(k, 3, pn).start()

    def ag_mid(buf, ss, sr, k):
        ag(buf, ss, sr, k, 0, n1(k), n1(k)).wait_recv()
        ag(buf, ss, sr, k, 2, n1(k), n2(k)).start()
        ag(buf, ss, sr, k, 4, n1(k), pn).start()

    def ag_last(buf, ss, sr, k):
        w = hid // sr.shape[0]
        arrived(buf.at[pl.ds(0, 2), 0, :, cols(k, w)], sr.at[k, 1])
        ag(buf, ss, sr, k, 5, n2(k), pn).start()
        ag(buf, ss, sr, k, 6, dg, pn).start()

    def ag_end(buf, ss, sr, k):
        w = hid // sr.shape[0]
        arrived(buf.at[:, 0, :, cols(k, w)], sr.at[k, 2])

    def y_local(g):
        w = AHEAD * hy
        return pltpu.make_async_copy(dy_ref.at[:, cols(g, w)], blk(dyv, t, g, w), yl.at[g])

    x_local = pltpu.make_async_copy(x_ref, xov, xl.at[0])
    x_put = pltpu.make_async_copy(xov, xa_ref.at[t // 2, t % 2], xl.at[1])

    def down_out(k):
        return pltpu.make_async_copy(ddv.at[k % 2], dd_ref.at[:, cols(k)], pd.at[k % 2])

    def wd_load(k):
        return pltpu.make_async_copy(wd_ref.at[:, cols(k)], wbuf.at[0, pl.ds(pl.multiple_of(k % 2 * fp, fp), ff), :], wl.at[0, k % 2])

    def w_load(k, j):
        src = (wg_ref, wu_ref)[j]
        return pltpu.make_async_copy(src.at[:, cols(k)], wbuf.at[(k + 1) % 2, pl.ds(j * fp, ff), :],
                                     wl.at[(k + 1) % 2, j])

    def dy_out(k):
        return pltpu.make_async_copy(dyv.at[:, :, :, cols(k)], dya_ref.at[:, :, :, cols(k)], dl.at[0])

    ug_in = pltpu.make_async_copy(ug_ref, ugv.at[pl.ds(0, ff), :], ul.at[0])
    uu_in = pltpu.make_async_copy(uu_ref, uuv.at[pl.ds(0, ff), :], ul.at[1])
    for g in range(NY // AHEAD):
        y_local(g).start()
    wd_load(0).start()
    wd_load(1).start()
    ug_in.start()
    uu_in.start()
    x_local.start()

    barrier = pltpu.get_barrier_semaphore()
    for dev in (xn, yn, pn):
        pl.semaphore_signal(barrier, inc=1, device_id={"tp": dev}, device_id_type=MESH)
    pl.semaphore_wait(barrier, 3)

    y_local(0).wait()
    for k in range(AHEAD):
        ag_own(dyv, ys, yr, k)

    for a in range(2):
        for b in range(2):
            wbuf[a, b * fp + ff:b * fp + fp, :] = jnp.zeros((fp - ff, hc), BF16)
    gv[...] = jnp.zeros_like(gv)
    ug_in.wait()
    uu_in.wait()

    def u_block(r0, n):
        rows = pl.ds(r0, n)
        ug = ugv[rows, :].astype(F32)
        ub = uuv[rows, :]
        uu = ub.astype(F32)
        s = jax.nn.sigmoid(ug)
        a = ug * s
        sp = s * (1.0 + ug * (1.0 - s))
        ugv[rows, :] = (a * uu).astype(BF16)
        if n < 128:
            pad = jnp.zeros((128 - n, tall), F32)
            a = jnp.concatenate([a, pad], axis=0)
            sp = jnp.concatenate([sp, pad], axis=0)
            uu = jnp.concatenate([uu, pad], axis=0)
        lanes = pl.ds(r0, 128)
        av[:, lanes] = a.T
        spv[:, lanes] = sp.T
        utv[:, lanes] = uu.T.astype(BF16)

    down0 = -(-(fp // 128) // per_h) * per_h

    def phase1(i, carry):
        @pl.when((i < NY - AHEAD) & (i % AHEAD == 0))
        def _():
            y_local(i // AHEAD + 1).wait()

        @pl.when(i < NY - AHEAD)
        def _():
            ag_own(dyv, ys, yr, i + AHEAD)

        @pl.when(i < NY)
        def _():
            ag_mid(dyv, ys, yr, i)

        @pl.when(i >= NY + TAKE - NH)
        def _():
            x_send(i - (NY + TAKE - NH))

        @pl.when(i < nfull)
        def _():
            u_block(pl.multiple_of(i * 128, 128), 128)

        if rest:
            @pl.when(i == nfull)
            def _():
                u_block(nfull * 128, rest)

        @pl.when((i >= LAG) & (i < NY + LAG))
        def _():
            ag_last(dyv, ys, yr, i - LAG)

        @pl.when(i >= TAKE)
        def _():
            ag_end(dyv, ys, yr, i - TAKE)

        @pl.when((i >= TAKE) & ((i - TAKE) % per_h == per_h - 1))
        def _():
            k = (i - TAKE) // per_h
            dy_out(k).start()
            wd_load(k).wait()
            dyc = dyv[:, :, :, cols(k)].reshape(tall, hc)
            for n in range(0, fp, 256):
                w = min(256, fp - n)
                gv[:, n:n + w] += lax.dot_general(dyc, wbuf[0, pl.ds(pl.multiple_of(k % 2 * fp + n, 128), w), :], NT, preferred_element_type=F32)

            @pl.when(k + 2 < NH)
            def _():
                wd_load(k + 2).start()

        @pl.when((i >= down0) & ((i - down0) % per_h == 0) & (i < down0 + DOWN * per_h))
        def _():
            k = (i - down0) // per_h

            @pl.when(k >= 2)
            def _():
                down_out(k - 2).wait()

            dyc = dyv[:, :, :, cols(k)].reshape(tall, hc)
            ddv[k % 2] = jnp.dot(ugv[:ff, :], dyc, preferred_element_type=F32)
            down_out(k).start()

        return carry

    w_load(0, 0).start()
    w_load(0, 1).start()
    x_local.wait()
    x_put.start()
    lax.fori_loop(0, NY + TAKE, phase1, 0)
    w_load(1, 0).start()
    w_load(1, 1).start()
    zt_out = pltpu.make_async_copy(ugv.at[pl.ds(0, ff), :], zt_ref, ol.at[0])
    zt_out.start()
    def gates(i, carry):
        rows = pl.ds(pl.multiple_of(i * 128, 128), 128)
        g = gv[rows, :]
        duv[rows, :fp] = (g * utv[rows, :].astype(F32) * spv[rows, :]).astype(BF16)
        duv[rows, fp:] = (g * av[rows, :]).astype(BF16)
        return carry

    lax.fori_loop(0, tall // 128, gates, 0)

    for n in range(7):
        left(dyv.at[0, 0], ys.at[n])
    pltpu.make_async_copy(dyv, dya_ref, dl.at[0]).wait()
    zt_out.wait()
    for k in range(DOWN - 2, DOWN):
        down_out(k).wait()

    def rs0(k, c):
        return rcopy(dyv.at[:, c, :, cols(k)], r0v.at[k], rs.at[0], rr.at[k], pn)

    def rs1(k):
        return rcopy(blk(dyv, dg, k), r1v.at[k], rs.at[1], r1r.at[k], n1(k))

    def sums_out(k, diagonal):
        outs = [(so_ref, t, k), (sx_ref, xn, k), (sy_ref, yn, k)] + ([(sd_ref, dg, k - HOPS)] if diagonal else [])
        return [pltpu.make_async_copy(blk(dyv, owner, k), ref.at[:, cols(c)], po.at[i])
                for i, (ref, owner, c) in enumerate(outs)]

    def add(owner, k, other):
        b = blk(dyv, owner, k)
        b[...] = (b[...].astype(F32) + other.astype(F32)).astype(BF16)

    def t_block(b):
        src = pl.multiple_of(jnp.minimum(b, blocks - 1) * 128, 128)
        rows = pl.ds(pl.multiple_of(jnp.minimum(b, blocks) * 128, 128), 128)
        ugv[rows, :] = duv[:, pl.ds(src, 128)].T
        uuv[rows, :] = duv[:, pl.ds(fp + src, 128)].T

    blocks = fp // 128
    per = -(-blocks // NH)

    outs = [pltpu.make_async_copy(v.at[pl.ds(0, ff), :], ref, ol.at[i])
            for i, (v, ref) in enumerate(((ugv, dgt_ref), (uuv, dut_ref)))]

    def phase2(i, carry):
        for first, ks in ((NH - 1, range(0, 3)),):
            @pl.when(i == first)
            def _():
                for k in ks:
                    ag_last(xa_ref, xs, xr, k)

        @pl.when(i < NH - 1)
        def _():
            ag_mid(xa_ref, xs, xr, i + 1)

        @pl.when(i < NH)
        def _():
            w_load(i, 0).wait()
            w_load(i, 1).wait()
            slot = (i + 1) % 2
            for b in range(per):
                t_block(per * i + b)
            p = jnp.dot(duv[...], wbuf[slot], preferred_element_type=F32)
            dyv[:, :, :, cols(i)] = p.astype(BF16).reshape(4, 2, tok, hc)

            @pl.when(i + 2 < NH)
            def _():
                w_load(i + 2, 0).start()
                w_load(i + 2, 1).start()

        @pl.when(i == -(-blocks // per))
        def _():
            for o in outs:
                o.start()

        @pl.when(i < NH)
        def _():
            rs0(i, 1 - tc).start()

        @pl.when((i >= 1) & (i <= NH))
        def _():
            k = i - 1
            rs0(k, tc).wait_recv()
            for q in range(4):
                add(2 * q + tc, k, r0v[k, q])

            @pl.when(k < HOPS)
            def _():
                rs1(k).start()

            @pl.when(k >= HOPS)
            def _():
                for o in sums_out(k, True):
                    o.start()

        @pl.when((i >= 5) & (i < 5 + HOPS))
        def _():
            k = i - 5
            rs1(k).wait_recv()
            add(n2(k), k, r1v[k])
            for o in sums_out(k, False):
                o.start()

        return carry

    ag_mid(xa_ref, xs, xr, 0)
    lax.fori_loop(0, NH + 1, phase2, 0)
    for k in range(3, NH):
        ag_last(xa_ref, xs, xr, k)

    def drain(k, carry):
        ag_end(xa_ref, xs, xr, k)
        return carry

    lax.fori_loop(0, NH, drain, 0)
    for n in range(7):
        left(xa_ref.at[0, 0], xs.at[n])
    left(dyv.at[:, 0], rs.at[0])
    left(dyv.at[0, 0, :, pl.ds(0, HOPS * hc)], rs.at[1])
    x_put.wait()
    for n, ref in enumerate((so_ref, sx_ref, sy_ref, sd_ref)):
        pltpu.make_async_copy(ref, ref, po.at[n]).wait()
    for o in outs:
        o.wait()


def _row_chunks(ff):
    n = ff // 16
    size = -(-n // 4)
    return [16 * min(size, n - i) for i in range(0, n, size)]


def _weight_kernel(zt_ref, dgt_ref, dut_ref, dy_ref, x_ref, part_ref, dd_ref, dg_ref, du_ref,
                   zv, dgv, duv, yv, xv, o0, o1, o2, cv, ls, ysem, xsem, os, ci, co):
    ff, tall = zt_ref.shape
    hid = dy_ref.shape[1]
    nb = yv.shape[-1]
    n = hid // nb
    sizes = _row_chunks(ff)
    depth = tall // 256

    def load(src, dst, sem, j, p):
        lo = pl.ds(pl.multiple_of(j * nb + p * 512, 512), 512)
        return pltpu.make_async_copy(src.at[:, lo], dst.at[j % 2, :, p * 512:p * 512 + 512], sem.at[j % 2, p])

    def y_loads(j):
        return [load(dy_ref, yv, ysem, j, p) for p in range(nb // 512)]

    def x_loads(j):
        return [load(x_ref, xv, xsem, j, p) for p in range(nb // 512)]

    def put(i, j, rows, width, p):
        stage, out = ((o0, dd_ref), (o1, dg_ref), (o2, du_ref))[i]
        lo = pl.ds(pl.multiple_of(j * nb + p * 512, 512), width)
        slot = j % stage.shape[0]
        return pltpu.make_async_copy(stage.at[slot, rows, p * 512:p * 512 + width], out.at[rows, lo], os.at[i, slot])

    def put_all(i, j):
        return put(i, j, pl.ds(0, ff), nb, 0)

    def product(i, j, accs, waits):
        a = (zv, dgv, duv)[i]
        b = (yv, xv, xv)[i].at[j % 2]
        stage = (o0, o1, o2)[i]
        slot = j % stage.shape[0]
        steps = []
        for pair in range(nb // 512):
            row = 0
            for c, size in enumerate(sizes):
                for kt in range(depth):
                    steps.append((pair, c, row, size, kt))
                row += size

        def push(s):
            pair, _, _, _, kt = steps[s]
            for q in range(2):
                lo = pair * 512 + q * 256
                pltpu.matmul_push_rhs(b[kt * 256:kt * 256 + 256, lo:lo + 256], s % 2, q)

        def pop(pair, c, row, size):
            for q in range(2):
                lo = pair * 512 + q * 256
                stage[slot, row:row + size, lo:lo + 256] = pltpu.matmul_pop(accs[q][c])
            put(i, j, pl.ds(row, size), 512, pair).start()

        late = None
        for s, (pair, c, row, size, kt) in enumerate(steps):
            if s == 0 or (c == 0 and kt == 0 and waits):
                for w in waits[pair] if waits else ():
                    w.wait()
                push(s)
            if s + 1 < len(steps) and not (waits and steps[s + 1][1] == 0 and steps[s + 1][4] == 0):
                push(s + 1)
            block = a[row:row + size, kt * 256:kt * 256 + 256]
            for q in range(2):
                pltpu.matmul_acc_lhs(accs[q][c], block, load_staged_rhs=s % 2)
            if kt == 0 and late is not None:
                pop(*late)
            if kt == depth - 1:
                late = (pair, c, row, size)
        pop(*late)

    def take(p):
        return pltpu.make_async_copy(part_ref.at[:, p * 512:p * 512 + 512], cv.at[p], ci.at[p])

    def give(p):
        return pltpu.make_async_copy(cv.at[p], dd_ref.at[:, p * 512:p * 512 + 512], co.at[p])

    zl, gl, ul = (pltpu.make_async_copy(src, dst, ls.at[i])
                  for i, (src, dst) in enumerate(((zt_ref, zv), (dgt_ref, dgv), (dut_ref, duv))))
    parts = range(nb // 512)
    first = x_loads(0)
    gl.start()
    for c in first:
        c.start()
    ul.start()
    zl.start()
    for c in y_loads(1) + x_loads(1):
        c.start()

    def body(*flat):
        h = len(flat) // 2
        accs = [[part[2] if i == len(sizes) - 1 else part[i % 2] for i in range(len(sizes))]
                for part in (flat[:h], flat[h:])]
        product(1, 0, accs, [[gl, first[0]], first[1:]])
        product(2, 0, accs, [[ul], []])
        zl.wait()

        def rest(j, carry):
            for c in y_loads(j) + x_loads(j):
                c.wait()

            @pl.when(j + 1 < n)
            def _():
                for c in y_loads(j + 1) + x_loads(j + 1):
                    c.start()

            @pl.when(j == 1)
            def _():
                for p in parts:
                    take(p).start()

            @pl.when(j == 2)
            def _():
                for p in parts:
                    take(p).wait()
                    give(p).start()

            @pl.when(j >= 2)
            def _():
                put_all(0, j - 1).wait()
                put_all(2, j - 2).wait()

            put_all(1, j - 1).wait()
            for i in range(3):
                product(i, j, accs, None)
            return carry

        lax.fori_loop(1, n, rest, 0)

    pl.run_scoped(body, *[pltpu.ACC(q)((size, 256), F32) for q in range(2) for size in (sizes[0], sizes[0], sizes[-1])])
    put_all(0, n - 1).wait()
    put_all(1, n - 1).wait()
    put_all(2, n - 2).wait()
    put_all(2, n - 1).wait()
    for p in parts:
        give(p).wait()


def _weight_grads(zt, dgt, dut, dy, x, part):
    ff, tall = zt.shape
    hid = x.shape[1]
    nb = 1024
    sem = pltpu.SemaphoreType.DMA
    any_ = pl.BlockSpec(memory_space=pltpu.HBM)
    return pl.pallas_call(
        _weight_kernel,
        out_shape=(jax.ShapeDtypeStruct((ff, hid), F32),) * 3,
        in_specs=[any_] * 6,
        out_specs=(any_,) * 3,
        scratch_shapes=[pltpu.VMEM((ff, tall), BF16)] * 3 + [pltpu.VMEM((2, tall, nb), BF16)] * 2
        + [pltpu.VMEM((k, ff, nb), F32) for k in (1, 1, 2)] + [pltpu.VMEM((nb // 512, ff, 512), F32)]
        + [sem((3,)), sem((2, 2)), sem((2, 2)), sem((3, 2)), sem((2,)), sem((2,))],
        compiler_params=pltpu.CompilerParams(vmem_limit_bytes=54 * 2 ** 20),
        cost_estimate=pl.CostEstimate(flops=6 * ff * tall * hid, bytes_accessed=12 * ff * hid, transcendentals=0),
        name="weight_grads",
    )(zt, dgt, dut, dy, x, part)


def solution(mesh):
    def local_backward(x, wg, wu, wd, ug, uu, dy):
        tok, hid = dy.shape
        ff = wd.shape[0]
        fp = _lanes(ff)
        tall = 8 * tok
        hc = hid // NH
        any_ = pl.BlockSpec(memory_space=pl.ANY)
        sem = pltpu.SemaphoreType.DMA
        full = jax.ShapeDtypeStruct((4, 2, tok, hid), BF16)
        act = jax.ShapeDtypeStruct((ff, tall), BF16)
        own = jax.ShapeDtypeStruct((tok, hid), BF16)
        rest = jax.ShapeDtypeStruct((tok, hid - HOPS * hc), BF16)
        so, sx, sy, sd, zt, dgt, dut, dya, xa, ddp = pl.pallas_call(
            _comm_kernel,
            out_shape=(own, own, own, rest, act, act, act, full, full,
                       jax.ShapeDtypeStruct((ff, DOWN * hc), F32)),
            in_specs=[any_] * 7,
            out_specs=(any_,) * 10,
            scratch_shapes=[
                pltpu.VMEM((4, 2, tok, hid), BF16),
                pltpu.VMEM((tall, fp), F32),
                pltpu.VMEM((tall, fp), F32),
                pltpu.VMEM((tall, fp), F32),
                pltpu.VMEM((tall, fp), BF16),
                pltpu.VMEM((tall, 2 * fp), BF16),
                pltpu.VMEM((2, 2 * fp, hc), BF16),
                pltpu.VMEM((fp + 128, tall), BF16),
                pltpu.VMEM((fp + 128, tall), BF16),
                pltpu.VMEM((NH, 4, tok, hc), BF16),
                pltpu.VMEM((HOPS, tok, hc), BF16),
                pltpu.VMEM((tok, hid), BF16),
                pltpu.VMEM((2, ff, hc), F32),
                sem((7,)), sem((NY, 3)), sem((7,)), sem((NH, 3)), sem((2,)), sem((NH,)), sem((HOPS,)),
                sem((NY // AHEAD,)), sem((2,)), sem((2, 2)), sem((2,)), sem((2,)), sem((1,)), sem((4,)), sem((2,)),
            ],
            compiler_params=pltpu.CompilerParams(collective_id=0, has_side_effects=True, vmem_limit_bytes=67043328),
            name="gather_partial",
        )(x, dy, wd, wg.T, wu.T, ug.T, uu.T)
        dya = dya.reshape(tall, hid)
        xa = xa.reshape(tall, hid)

        def to(v, flip):
            return lax.ppermute(v, 'tp', [(i, i ^ flip) for i in range(8)])

        fx, fy, fd = to(sx, 2), to(sy, 4), to(sd, 6)
        zt, dgt, dut, ddp = (pltpu.with_memory_space_constraint(v, pltpu.HBM) for v in (zt, dgt, dut, ddp))
        dwd, dwg, dwu = _weight_grads(zt, dgt, dut, dya, xa, ddp)
        fx, fy, fd, dwd, dwg, dwu = lax.optimization_barrier((fx, fy, fd, dwd, dwg, dwu))
        right = jnp.pad(fd, ((0, 0), (HOPS * hc, 0)))
        dx = sum(v.astype(F32) for v in (so, fx, fy, right)).astype(BF16)
        return dx, dwg.T, dwu.T, dwd

    tok_spec = P(('dp', 'tp'), None)
    col_spec = P(None, 'tp')
    act_spec = P('dp', 'tp')
    return jax.shard_map(local_backward, mesh=mesh,
                         in_specs=(tok_spec, col_spec, col_spec, P('tp', None), act_spec, act_spec, tok_spec),
                         out_specs=(tok_spec, act_spec, act_spec, tok_spec),
                         check_vma=False)
```

```python
import functools

import jax
import jax.numpy as jnp
from jax import lax
from jax.experimental import pallas as pl
from jax.experimental.pallas import tpu as pltpu
from jax.sharding import PartitionSpec as P

MESH = pl.DeviceIdType.MESH
BF16 = jnp.bfloat16
F32 = jnp.float32
NH = 8
HOPS = 4
DOWN = 2
NY = 16
AHEAD, LAG, TAKE = 4, 4, 6
NT = (((1,), (1,)), ((), ()))


def _lanes(n):
    return (n + 127) // 128 * 128


def _comm_kernel(x_ref, dy_ref, wd_ref, wg_ref, wu_ref, ug_ref, uu_ref,
                 so_ref, sx_ref, sy_ref, sd_ref, zt_ref, dgt_ref, dut_ref, dya_ref, xa_ref, dd_ref,
                 dyv, gv, av, spv, utv, duv, wbuf, ugv, uuv, r0v, r1v, xov, ddv,
                 ys, yr, xs, xr, rs, rr, r1r, yl, xl, wl, ul, ol, dl, po, pd):
    tok, hid = dy_ref.shape
    ff = wd_ref.shape[0]
    fp = _lanes(ff)
    nfull, rest = ff // 128, ff % 128
    hc = hid // NH
    tall = 8 * tok

    t = lax.axis_index("tp")
    ty, tx, tc = t // 4, (t // 2) % 2, t % 2
    xn = t + 2 - 4 * tx
    yn = t + 4 - 8 * ty
    dg = xn + yn - t
    pn = t + 1 - 2 * tc

    def n1(k):
        return xn + (yn - xn) * (k % 2)

    def n2(k):
        return yn + (xn - yn) * (k % 2)

    hy = hid // NY
    per_h = NY // NH

    def cols(k, w=hc):
        return pl.ds(pl.multiple_of(k * w, w), w)

    def blk(ref, owner, k, w=hc):
        return ref.at[owner // 2, owner % 2, :, cols(k, w)]

    def rcopy(src, dst, ss, rs_, dev):
        return pltpu.make_async_remote_copy(src_ref=src, dst_ref=dst, send_sem=ss, recv_sem=rs_,
                                            device_id={"tp": dev}, device_id_type=MESH)

    def ag(buf, ss, sr, k, j, owner, dev):
        w = hid // sr.shape[0]
        return rcopy(blk(buf, owner, k, w), blk(buf, owner, k, w), ss.at[j], sr.at[k, (0, 1, 1, 2, 2, 2, 2)[j]], dev)

    def arrived(ref, sem):
        rcopy(ref, ref, sem, sem, t).wait_recv()

    def left(ref, sem):
        rcopy(ref, ref, sem, sem, t).wait_send()

    def ag_own(buf, ss, sr, k):
        ag(buf, ss, sr, k, 0, t, n1(k)).start()
        ag(buf, ss, sr, k, 1, t, n2(k)).start()
        ag(buf, ss, sr, k, 3, t, pn).start()

    def x_own(k, j, dev):
        return rcopy(xov.at[:, cols(k)], blk(xa_ref, t, k), xs.at[j], xr.at[k, (0, 1, 1, 2)[j]], dev)

    def x_send(k):
        x_own(k, 0, n1(k)).start()
        x_own(k, 1, n2(k)).start()
        x_own(k, 3, pn).start()

    def ag_mid(buf, ss, sr, k):
        ag(buf, ss, sr, k, 0, n1(k), n1(k)).wait_recv()
        ag(buf, ss, sr, k, 2, n1(k), n2(k)).start()
        ag(buf, ss, sr, k, 4, n1(k), pn).start()

    def ag_last(buf, ss, sr, k):
        w = hid // sr.shape[0]
        arrived(buf.at[pl.ds(0, 2), 0, :, cols(k, w)], sr.at[k, 1])
        ag(buf, ss, sr, k, 5, n2(k), pn).start()
        ag(buf, ss, sr, k, 6, dg, pn).start()

    def ag_end(buf, ss, sr, k):
        w = hid // sr.shape[0]
        arrived(buf.at[:, 0, :, cols(k, w)], sr.at[k, 2])

    def y_local(g):
        w = AHEAD * hy
        return pltpu.make_async_copy(dy_ref.at[:, cols(g, w)], blk(dyv, t, g, w), yl.at[g])

    x_local = pltpu.make_async_copy(x_ref, xov, xl.at[0])
    x_put = pltpu.make_async_copy(xov, xa_ref.at[t // 2, t % 2], xl.at[1])

    def down_out(k):
        return pltpu.make_async_copy(ddv.at[k % 2], dd_ref.at[:, cols(k)], pd.at[k % 2])

    def wd_load(k):
        return pltpu.make_async_copy(wd_ref.at[:, cols(k)], wbuf.at[0, pl.ds(pl.multiple_of(k % 2 * fp, fp), ff), :], wl.at[0, k % 2])

    def w_load(k, j):
        src = (wg_ref, wu_ref)[j]
        return pltpu.make_async_copy(src.at[:, cols(k)], wbuf.at[(k + 1) % 2, pl.ds(j * fp, ff), :],
                                     wl.at[(k + 1) % 2, j])

    def dy_out(k):
        return pltpu.make_async_copy(dyv.at[:, :, :, cols(k)], dya_ref.at[:, :, :, cols(k)], dl.at[0])

    ug_in = pltpu.make_async_copy(ug_ref, ugv.at[pl.ds(0, ff), :], ul.at[0])
    uu_in = pltpu.make_async_copy(uu_ref, uuv.at[pl.ds(0, ff), :], ul.at[1])
    for g in range(NY // AHEAD):
        y_local(g).start()
    wd_load(0).start()
    wd_load(1).start()
    ug_in.start()
    uu_in.start()
    x_local.start()

    barrier = pltpu.get_barrier_semaphore()
    for dev in (xn, yn, pn):
        pl.semaphore_signal(barrier, inc=1, device_id={"tp": dev}, device_id_type=MESH)
    pl.semaphore_wait(barrier, 3)

    y_local(0).wait()
    for k in range(AHEAD):
        ag_own(dyv, ys, yr, k)

    for a in range(2):
        for b in range(2):
            wbuf[a, b * fp + ff:b * fp + fp, :] = jnp.zeros((fp - ff, hc), BF16)
    gv[...] = jnp.zeros_like(gv)
    ug_in.wait()
    uu_in.wait()

    def u_block(r0, n):
        rows = pl.ds(r0, n)
        ug = ugv[rows, :].astype(F32)
        ub = uuv[rows, :]
        uu = ub.astype(F32)
        s = jax.nn.sigmoid(ug)
        a = ug * s
        sp = s * (1.0 + ug * (1.0 - s))
        ugv[rows, :] = (a * uu).astype(BF16)
        if n < 128:
            pad = jnp.zeros((128 - n, tall), F32)
            a = jnp.concatenate([a, pad], axis=0)
            sp = jnp.concatenate([sp, pad], axis=0)
            uu = jnp.concatenate([uu, pad], axis=0)
        lanes = pl.ds(r0, 128)
        av[:, lanes] = a.T
        spv[:, lanes] = sp.T
        utv[:, lanes] = uu.T.astype(BF16)

    down0 = -(-(fp // 128) // per_h) * per_h

    def phase1(i, carry):
        @pl.when((i < NY - AHEAD) & (i % AHEAD == 0))
        def _():
            y_local(i // AHEAD + 1).wait()

        @pl.when(i < NY - AHEAD)
        def _():
            ag_own(dyv, ys, yr, i + AHEAD)

        @pl.when(i < NY)
        def _():
            ag_mid(dyv, ys, yr, i)

        @pl.when(i >= NY + TAKE - NH)
        def _():
            x_send(i - (NY + TAKE - NH))

        @pl.when(i < nfull)
        def _():
            u_block(pl.multiple_of(i * 128, 128), 128)

        if rest:
            @pl.when(i == nfull)
            def _():
                u_block(nfull * 128, rest)

        @pl.when((i >= LAG) & (i < NY + LAG))
        def _():
            ag_last(dyv, ys, yr, i - LAG)

        @pl.when(i >= TAKE)
        def _():
            ag_end(dyv, ys, yr, i - TAKE)

        @pl.when((i >= TAKE) & ((i - TAKE) % per_h == per_h - 1))
        def _():
            k = (i - TAKE) // per_h
            dy_out(k).start()
            wd_load(k).wait()
            dyc = dyv[:, :, :, cols(k)].reshape(tall, hc)
            for n in range(0, fp, 256):
                w = min(256, fp - n)
                gv[:, n:n + w] += lax.dot_general(dyc, wbuf[0, pl.ds(pl.multiple_of(k % 2 * fp + n, 128), w), :], NT, preferred_element_type=F32)

            @pl.when(k + 2 < NH)
            def _():
                wd_load(k + 2).start()

        @pl.when((i >= down0) & ((i - down0) % per_h == 0) & (i < down0 + DOWN * per_h))
        def _():
            k = (i - down0) // per_h

            @pl.when(k >= 2)
            def _():
                down_out(k - 2).wait()

            dyc = dyv[:, :, :, cols(k)].reshape(tall, hc)
            ddv[k % 2] = jnp.dot(ugv[:ff, :], dyc, preferred_element_type=F32)
            down_out(k).start()

        return carry

    w_load(0, 0).start()
    w_load(0, 1).start()
    x_local.wait()
    x_put.start()
    lax.fori_loop(0, NY + TAKE, phase1, 0)
    w_load(1, 0).start()
    w_load(1, 1).start()
    zt_out = pltpu.make_async_copy(ugv.at[pl.ds(0, ff), :], zt_ref, ol.at[0])
    zt_out.start()
    def gates(i, carry):
        rows = pl.ds(pl.multiple_of(i * 128, 128), 128)
        g = gv[rows, :]
        duv[rows, :fp] = (g * utv[rows, :].astype(F32) * spv[rows, :]).astype(BF16)
        duv[rows, fp:] = (g * av[rows, :]).astype(BF16)
        return carry

    lax.fori_loop(0, tall // 128, gates, 0)

    for n in range(7):
        left(dyv.at[0, 0], ys.at[n])
    pltpu.make_async_copy(dyv, dya_ref, dl.at[0]).wait()
    zt_out.wait()
    for k in range(DOWN - 2, DOWN):
        down_out(k).wait()

    def rs0(k, c):
        return rcopy(dyv.at[:, c, :, cols(k)], r0v.at[k], rs.at[0], rr.at[k], pn)

    def rs1(k):
        return rcopy(blk(dyv, dg, k), r1v.at[k], rs.at[1], r1r.at[k], n1(k))

    def sums_out(k, diagonal):
        outs = [(so_ref, t, k), (sx_ref, xn, k), (sy_ref, yn, k)] + ([(sd_ref, dg, k - HOPS)] if diagonal else [])
        return [pltpu.make_async_copy(blk(dyv, owner, k), ref.at[:, cols(c)], po.at[i])
                for i, (ref, owner, c) in enumerate(outs)]

    def add(owner, k, other):
        b = blk(dyv, owner, k)
        b[...] = (b[...].astype(F32) + other.astype(F32)).astype(BF16)

    def t_block(b):
        src = pl.multiple_of(jnp.minimum(b, blocks - 1) * 128, 128)
        rows = pl.ds(pl.multiple_of(jnp.minimum(b, blocks) * 128, 128), 128)
        ugv[rows, :] = duv[:, pl.ds(src, 128)].T
        uuv[rows, :] = duv[:, pl.ds(fp + src, 128)].T

    blocks = fp // 128
    per = -(-blocks // NH)

    outs = [pltpu.make_async_copy(v.at[pl.ds(0, ff), :], ref, ol.at[i])
            for i, (v, ref) in enumerate(((ugv, dgt_ref), (uuv, dut_ref)))]

    def phase2(i, carry):
        for first, ks in ((NH - 1, range(0, 3)),):
            @pl.when(i == first)
            def _():
                for k in ks:
                    ag_last(xa_ref, xs, xr, k)

        @pl.when(i < NH - 1)
        def _():
            ag_mid(xa_ref, xs, xr, i + 1)

        @pl.when(i < NH)
        def _():
            w_load(i, 0).wait()
            w_load(i, 1).wait()
            slot = (i + 1) % 2
            for b in range(per):
                t_block(per * i + b)
            p = jnp.dot(duv[...], wbuf[slot], preferred_element_type=F32)
            dyv[:, :, :, cols(i)] = p.astype(BF16).reshape(4, 2, tok, hc)

            @pl.when(i + 2 < NH)
            def _():
                w_load(i + 2, 0).start()
                w_load(i + 2, 1).start()

        @pl.when(i == -(-blocks // per))
        def _():
            for o in outs:
                o.start()

        @pl.when(i < NH)
        def _():
            rs0(i, 1 - tc).start()

        @pl.when((i >= 1) & (i <= NH))
        def _():
            k = i - 1
            rs0(k, tc).wait_recv()
            for q in range(4):
                add(2 * q + tc, k, r0v[k, q])

            @pl.when(k < HOPS)
            def _():
                rs1(k).start()

            @pl.when(k >= HOPS)
            def _():
                for o in sums_out(k, True):
                    o.start()

        @pl.when((i >= 5) & (i < 5 + HOPS))
        def _():
            k = i - 5
            rs1(k).wait_recv()
            add(n2(k), k, r1v[k])
            for o in sums_out(k, False):
                o.start()

        return carry

    ag_mid(xa_ref, xs, xr, 0)
    lax.fori_loop(0, NH + 1, phase2, 0)
    for k in range(3, NH):
        ag_last(xa_ref, xs, xr, k)

    def drain(k, carry):
        ag_end(xa_ref, xs, xr, k)
        return carry

    lax.fori_loop(0, NH, drain, 0)
    for n in range(7):
        left(xa_ref.at[0, 0], xs.at[n])
    left(dyv.at[:, 0], rs.at[0])
    left(dyv.at[0, 0, :, pl.ds(0, HOPS * hc)], rs.at[1])
    x_put.wait()
    for n, ref in enumerate((so_ref, sx_ref, sy_ref, sd_ref)):
        pltpu.make_async_copy(ref, ref, po.at[n]).wait()
    for o in outs:
        o.wait()


def _row_chunks(ff):
    n = ff // 16
    size = -(-n // 4)
    return [16 * min(size, n - i) for i in range(0, n, size)]


def _weight_kernel(zt_ref, dgt_ref, dut_ref, dy_ref, x_ref, part_ref, dd_ref, dg_ref, du_ref,
                   zv, dgv, duv, yv, xv, o0, o1, o2, cv, ls, ysem, xsem, os, ci, co):
    ff, tall = zt_ref.shape
    hid = dy_ref.shape[1]
    nb = yv.shape[-1]
    n = hid // nb
    sizes = _row_chunks(ff)
    depth = tall // 256

    def load(src, dst, sem, j, p):
        lo = pl.ds(pl.multiple_of(j * nb + p * 512, 512), 512)
        return pltpu.make_async_copy(src.at[:, lo], dst.at[j % 2, :, p * 512:p * 512 + 512], sem.at[j % 2, p])

    def y_loads(j):
        return [load(dy_ref, yv, ysem, j, p) for p in range(nb // 512)]

    def x_loads(j):
        return [load(x_ref, xv, xsem, j, p) for p in range(nb // 512)]

    def put(i, j, rows, width, p):
        stage, out = ((o0, dd_ref), (o1, dg_ref), (o2, du_ref))[i]
        lo = pl.ds(pl.multiple_of(j * nb + p * 512, 512), width)
        slot = j % stage.shape[0]
        return pltpu.make_async_copy(stage.at[slot, rows, p * 512:p * 512 + width], out.at[rows, lo], os.at[i, slot])

    def put_all(i, j):
        return put(i, j, pl.ds(0, ff), nb, 0)

    def product(i, j, accs, waits):
        a = (zv, dgv, duv)[i]
        b = (yv, xv, xv)[i].at[j % 2]
        stage = (o0, o1, o2)[i]
        slot = j % stage.shape[0]
        steps = []
        for pair in range(nb // 512):
            row = 0
            for c, size in enumerate(sizes):
                for kt in range(depth):
                    steps.append((pair, c, row, size, kt))
                row += size

        def push(s):
            pair, _, _, _, kt = steps[s]
            for q in range(2):
                lo = pair * 512 + q * 256
                pltpu.matmul_push_rhs(b[kt * 256:kt * 256 + 256, lo:lo + 256], s % 2, q)

        def pop(pair, c, row, size):
            for q in range(2):
                lo = pair * 512 + q * 256
                stage[slot, row:row + size, lo:lo + 256] = pltpu.matmul_pop(accs[q][c])
            put(i, j, pl.ds(row, size), 512, pair).start()

        late = None
        for s, (pair, c, row, size, kt) in enumerate(steps):
            if s == 0 or (kt == 0 and (pair, c) in waits):
                for w in waits.get((pair, c), ()):
                    w.wait()
                push(s)
            if s + 1 < len(steps) and not (steps[s + 1][4] == 0 and steps[s + 1][:2] in waits):
                push(s + 1)
            block = a[row:row + size, kt * 256:kt * 256 + 256]
            for q in range(2):
                pltpu.matmul_acc_lhs(accs[q][c], block, load_staged_rhs=s % 2)
            if kt == 0 and late is not None:
                pop(*late)
            if kt == depth - 1:
                late = (pair, c, row, size)
        pop(*late)

    def take(p):
        return pltpu.make_async_copy(part_ref.at[:, p * 512:p * 512 + 512], cv.at[p], ci.at[p])

    def give(p):
        return pltpu.make_async_copy(cv.at[p], dd_ref.at[:, p * 512:p * 512 + 512], co.at[p])

    zl, ul = (pltpu.make_async_copy(src, dst, ls.at[i]) for i, (src, dst) in enumerate(((zt_ref, zv), (dut_ref, duv))))
    gl = [pltpu.make_async_copy(dgt_ref.at[rows, :], dgv.at[rows, :], ls.at[2 + i])
          for i, rows in enumerate((pl.ds(0, sizes[0]), pl.ds(sizes[0], ff - sizes[0])))]
    parts = range(nb // 512)
    first = x_loads(0)
    for c in (gl[0], first[0], gl[1], *first[1:], ul):
        c.start()
    zl.start()
    for c in y_loads(1) + x_loads(1):
        c.start()

    def body(*flat):
        h = len(flat) // 2
        accs = [[part[2] if i == len(sizes) - 1 else part[i % 2] for i in range(len(sizes))]
                for part in (flat[:h], flat[h:])]
        product(1, 0, accs, {(0, 0): [gl[0], first[0]], (0, 1): gl[1:], (1, 0): first[1:]})
        product(2, 0, accs, {(0, 0): [ul]})
        zl.wait()

        def rest(j, carry):
            for c in y_loads(j) + x_loads(j):
                c.wait()

            @pl.when(j + 1 < n)
            def _():
                for c in y_loads(j + 1) + x_loads(j + 1):
                    c.start()

            @pl.when(j == 1)
            def _():
                for p in parts:
                    take(p).start()

            @pl.when(j == 2)
            def _():
                for p in parts:
                    take(p).wait()
                    give(p).start()

            @pl.when(j >= 2)
            def _():
                put_all(0, j - 1).wait()
                put_all(2, j - 2).wait()

            put_all(1, j - 1).wait()
            for i in range(3):
                product(i, j, accs, {})
            return carry

        lax.fori_loop(1, n, rest, 0)

    pl.run_scoped(body, *[pltpu.ACC(q)((size, 256), F32) for q in range(2) for size in (sizes[0], sizes[0], sizes[-1])])
    put_all(0, n - 1).wait()
    put_all(1, n - 1).wait()
    put_all(2, n - 2).wait()
    put_all(2, n - 1).wait()
    for p in parts:
        give(p).wait()


def _weight_grads(zt, dgt, dut, dy, x, part):
    ff, tall = zt.shape
    hid = x.shape[1]
    nb = 1024
    sem = pltpu.SemaphoreType.DMA
    any_ = pl.BlockSpec(memory_space=pltpu.HBM)
    return pl.pallas_call(
        _weight_kernel,
        out_shape=(jax.ShapeDtypeStruct((ff, hid), F32),) * 3,
        in_specs=[any_] * 6,
        out_specs=(any_,) * 3,
        scratch_shapes=[pltpu.VMEM((ff, tall), BF16)] * 3 + [pltpu.VMEM((2, tall, nb), BF16)] * 2
        + [pltpu.VMEM((k, ff, nb), F32) for k in (1, 1, 2)] + [pltpu.VMEM((nb // 512, ff, 512), F32)]
        + [sem((4,)), sem((2, 2)), sem((2, 2)), sem((3, 2)), sem((2,)), sem((2,))],
        compiler_params=pltpu.CompilerParams(vmem_limit_bytes=54 * 2 ** 20),
        cost_estimate=pl.CostEstimate(flops=6 * ff * tall * hid, bytes_accessed=12 * ff * hid, transcendentals=0),
        name="weight_grads",
    )(zt, dgt, dut, dy, x, part)


def solution(mesh):
    def local_backward(x, wg, wu, wd, ug, uu, dy):
        tok, hid = dy.shape
        ff = wd.shape[0]
        fp = _lanes(ff)
        tall = 8 * tok
        hc = hid // NH
        any_ = pl.BlockSpec(memory_space=pl.ANY)
        sem = pltpu.SemaphoreType.DMA
        full = jax.ShapeDtypeStruct((4, 2, tok, hid), BF16)
        act = jax.ShapeDtypeStruct((ff, tall), BF16)
        own = jax.ShapeDtypeStruct((tok, hid), BF16)
        rest = jax.ShapeDtypeStruct((tok, hid - HOPS * hc), BF16)
        so, sx, sy, sd, zt, dgt, dut, dya, xa, ddp = pl.pallas_call(
            _comm_kernel,
            out_shape=(own, own, own, rest, act, act, act, full, full,
                       jax.ShapeDtypeStruct((ff, DOWN * hc), F32)),
            in_specs=[any_] * 7,
            out_specs=(any_,) * 10,
            scratch_shapes=[
                pltpu.VMEM((4, 2, tok, hid), BF16),
                pltpu.VMEM((tall, fp), F32),
                pltpu.VMEM((tall, fp), F32),
                pltpu.VMEM((tall, fp), F32),
                pltpu.VMEM((tall, fp), BF16),
                pltpu.VMEM((tall, 2 * fp), BF16),
                pltpu.VMEM((2, 2 * fp, hc), BF16),
                pltpu.VMEM((fp + 128, tall), BF16),
                pltpu.VMEM((fp + 128, tall), BF16),
                pltpu.VMEM((NH, 4, tok, hc), BF16),
                pltpu.VMEM((HOPS, tok, hc), BF16),
                pltpu.VMEM((tok, hid), BF16),
                pltpu.VMEM((2, ff, hc), F32),
                sem((7,)), sem((NY, 3)), sem((7,)), sem((NH, 3)), sem((2,)), sem((NH,)), sem((HOPS,)),
                sem((NY // AHEAD,)), sem((2,)), sem((2, 2)), sem((2,)), sem((2,)), sem((1,)), sem((4,)), sem((2,)),
            ],
            compiler_params=pltpu.CompilerParams(collective_id=0, has_side_effects=True, vmem_limit_bytes=67043328),
            name="gather_partial",
        )(x, dy, wd, wg.T, wu.T, ug.T, uu.T)
        dya = dya.reshape(tall, hid)
        xa = xa.reshape(tall, hid)

        def to(v, flip):
            return lax.ppermute(v, 'tp', [(i, i ^ flip) for i in range(8)])

        fx, fy, fd = to(sx, 2), to(sy, 4), to(sd, 6)
        zt, dgt, dut, ddp = (pltpu.with_memory_space_constraint(v, pltpu.HBM) for v in (zt, dgt, dut, ddp))
        dwd, dwg, dwu = _weight_grads(zt, dgt, dut, dya, xa, ddp)
        fx, fy, fd, dwd, dwg, dwu = lax.optimization_barrier((fx, fy, fd, dwd, dwg, dwu))
        right = jnp.pad(fd, ((0, 0), (HOPS * hc, 0)))
        dx = sum(v.astype(F32) for v in (so, fx, fy, right)).astype(BF16)
        return dx, dwg.T, dwu.T, dwd

    tok_spec = P(('dp', 'tp'), None)
    col_spec = P(None, 'tp')
    act_spec = P('dp', 'tp')
    return jax.shard_map(local_backward, mesh=mesh,
                         in_specs=(tok_spec, col_spec, col_spec, P('tp', None), act_spec, act_spec, tok_spec),
                         out_specs=(tok_spec, act_spec, act_spec, tok_spec),
                         check_vma=False)
```

```python
import functools

import jax
import jax.numpy as jnp
from jax import lax
from jax.experimental import pallas as pl
from jax.experimental.pallas import tpu as pltpu
from jax.sharding import PartitionSpec as P

MESH = pl.DeviceIdType.MESH
BF16 = jnp.bfloat16
F32 = jnp.float32
NH = 8
HOPS = 6
DOWN = 4
NY = 16
AHEAD, LAG, TAKE = 4, 4, 6
NT = (((1,), (1,)), ((), ()))


def _lanes(n):
    return (n + 127) // 128 * 128


def _comm_kernel(x_ref, dy_ref, wd_ref, wg_ref, wu_ref, ug_ref, uu_ref,
                 so_ref, sx_ref, sy_ref, sd_ref, zt_ref, dgt_ref, dut_ref, dya_ref, xa_ref, dd_ref,
                 dyv, gv, av, spv, utv, duv, wbuf, ugv, uuv, r0v, r1v, xov, ddv,
                 ys, yr, xs, xr, rs, rr, r1r, yl, xl, wl, ul, ol, dl, po, pd):
    tok, hid = dy_ref.shape
    ff = wd_ref.shape[0]
    fp = _lanes(ff)
    nfull, rest = ff // 128, ff % 128
    hc = hid // NH
    tall = 8 * tok

    t = lax.axis_index("tp")
    ty, tx, tc = t // 4, (t // 2) % 2, t % 2
    xn = t + 2 - 4 * tx
    yn = t + 4 - 8 * ty
    dg = xn + yn - t
    pn = t + 1 - 2 * tc

    def n1(k):
        return xn + (yn - xn) * (k % 2)

    def n2(k):
        return yn + (xn - yn) * (k % 2)

    hy = hid // NY
    per_h = NY // NH

    def cols(k, w=hc):
        return pl.ds(pl.multiple_of(k * w, w), w)

    def blk(ref, owner, k, w=hc):
        return ref.at[owner // 2, owner % 2, :, cols(k, w)]

    def rcopy(src, dst, ss, rs_, dev):
        return pltpu.make_async_remote_copy(src_ref=src, dst_ref=dst, send_sem=ss, recv_sem=rs_,
                                            device_id={"tp": dev}, device_id_type=MESH)

    def ag(buf, ss, sr, k, j, owner, dev):
        w = hid // sr.shape[0]
        return rcopy(blk(buf, owner, k, w), blk(buf, owner, k, w), ss.at[j], sr.at[k, (0, 1, 1, 2, 2, 2, 2)[j]], dev)

    def arrived(ref, sem):
        rcopy(ref, ref, sem, sem, t).wait_recv()

    def left(ref, sem):
        rcopy(ref, ref, sem, sem, t).wait_send()

    def ag_own(buf, ss, sr, k):
        ag(buf, ss, sr, k, 0, t, n1(k)).start()
        ag(buf, ss, sr, k, 1, t, n2(k)).start()
        ag(buf, ss, sr, k, 3, t, pn).start()

    def x_own(k, j, dev):
        return rcopy(xov.at[:, cols(k)], blk(xa_ref, t, k), xs.at[j], xr.at[k, (0, 1, 1, 2)[j]], dev)

    def x_send(k):
        x_own(k, 0, n1(k)).start()
        x_own(k, 1, n2(k)).start()
        x_own(k, 3, pn).start()

    def ag_mid(buf, ss, sr, k):
        ag(buf, ss, sr, k, 0, n1(k), n1(k)).wait_recv()
        ag(buf, ss, sr, k, 2, n1(k), n2(k)).start()
        ag(buf, ss, sr, k, 4, n1(k), pn).start()

    def ag_last(buf, ss, sr, k):
        w = hid // sr.shape[0]
        arrived(buf.at[pl.ds(0, 2), 0, :, cols(k, w)], sr.at[k, 1])
        ag(buf, ss, sr, k, 5, n2(k), pn).start()
        ag(buf, ss, sr, k, 6, dg, pn).start()

    def ag_end(buf, ss, sr, k):
        w = hid // sr.shape[0]
        arrived(buf.at[:, 0, :, cols(k, w)], sr.at[k, 2])

    def y_local(g):
        w = AHEAD * hy
        return pltpu.make_async_copy(dy_ref.at[:, cols(g, w)], blk(dyv, t, g, w), yl.at[g])

    x_local = pltpu.make_async_copy(x_ref, xov, xl.at[0])
    x_put = pltpu.make_async_copy(xov, xa_ref.at[t // 2, t % 2], xl.at[1])

    def down_out(k):
        return pltpu.make_async_copy(ddv.at[k % 2], dd_ref.at[:, cols(k)], pd.at[k % 2])

    def wd_load(k):
        return pltpu.make_async_copy(wd_ref.at[:, cols(k)], wbuf.at[0, pl.ds(pl.multiple_of(k % 2 * fp, fp), ff), :], wl.at[0, k % 2])

    def w_load(k, j):
        src = (wg_ref, wu_ref)[j]
        return pltpu.make_async_copy(src.at[:, cols(k)], wbuf.at[(k + 1) % 2, pl.ds(j * fp, ff), :],
                                     wl.at[(k + 1) % 2, j])

    def dy_out(k):
        return pltpu.make_async_copy(dyv.at[:, :, :, cols(k)], dya_ref.at[:, :, :, cols(k)], dl.at[0])

    ug_in = pltpu.make_async_copy(ug_ref, ugv.at[pl.ds(0, ff), :], ul.at[0])
    uu_in = pltpu.make_async_copy(uu_ref, uuv.at[pl.ds(0, ff), :], ul.at[1])
    for g in range(NY // AHEAD):
        y_local(g).start()
    wd_load(0).start()
    wd_load(1).start()
    ug_in.start()
    uu_in.start()
    x_local.start()

    barrier = pltpu.get_barrier_semaphore()
    for dev in (xn, yn, pn):
        pl.semaphore_signal(barrier, inc=1, device_id={"tp": dev}, device_id_type=MESH)
    pl.semaphore_wait(barrier, 3)

    y_local(0).wait()
    for k in range(AHEAD):
        ag_own(dyv, ys, yr, k)

    for a in range(2):
        for b in range(2):
            wbuf[a, b * fp + ff:b * fp + fp, :] = jnp.zeros((fp - ff, hc), BF16)
    gv[...] = jnp.zeros_like(gv)
    ug_in.wait()
    uu_in.wait()

    def u_block(r0, n):
        rows = pl.ds(r0, n)
        ug = ugv[rows, :].astype(F32)
        ub = uuv[rows, :]
        uu = ub.astype(F32)
        s = jax.nn.sigmoid(ug)
        a = ug * s
        sp = s * (1.0 + ug * (1.0 - s))
        ugv[rows, :] = (a * uu).astype(BF16)
        if n < 128:
            pad = jnp.zeros((128 - n, tall), F32)
            a = jnp.concatenate([a, pad], axis=0)
            sp = jnp.concatenate([sp, pad], axis=0)
            uu = jnp.concatenate([uu, pad], axis=0)
        lanes = pl.ds(r0, 128)
        av[:, lanes] = a.T
        spv[:, lanes] = sp.T
        utv[:, lanes] = uu.T.astype(BF16)

    down0 = fp // 128

    def phase1(i, carry):
        @pl.when((i < NY - AHEAD) & (i % AHEAD == 0))
        def _():
            y_local(i // AHEAD + 1).wait()

        @pl.when(i < NY - AHEAD)
        def _():
            ag_own(dyv, ys, yr, i + AHEAD)

        @pl.when(i < NY)
        def _():
            ag_mid(dyv, ys, yr, i)

        @pl.when(i >= NY + TAKE - NH)
        def _():
            x_send(i - (NY + TAKE - NH))

        @pl.when(i < nfull)
        def _():
            u_block(pl.multiple_of(i * 128, 128), 128)

        if rest:
            @pl.when(i == nfull)
            def _():
                u_block(nfull * 128, rest)

        @pl.when((i >= LAG) & (i < NY + LAG))
        def _():
            ag_last(dyv, ys, yr, i - LAG)

        @pl.when(i >= TAKE)
        def _():
            ag_end(dyv, ys, yr, i - TAKE)

        @pl.when((i >= TAKE) & ((i - TAKE) % per_h == per_h - 1))
        def _():
            k = (i - TAKE) // per_h
            dy_out(k).start()
            wd_load(k).wait()
            dyc = dyv[:, :, :, cols(k)].reshape(tall, hc)
            for n in range(0, fp, 256):
                w = min(256, fp - n)
                gv[:, n:n + w] += lax.dot_general(dyc, wbuf[0, pl.ds(pl.multiple_of(k % 2 * fp + n, 128), w), :], NT, preferred_element_type=F32)

            @pl.when(k + 2 < NH)
            def _():
                wd_load(k + 2).start()

        @pl.when((i >= down0) & (i < down0 + DOWN))
        def _():
            k = i - down0

            @pl.when(k >= 2)
            def _():
                down_out(k - 2).wait()

            dyc = dyv[:, :, :, cols(k)].reshape(tall, hc)
            ddv[k % 2] = jnp.dot(ugv[:ff, :], dyc, preferred_element_type=F32)
            down_out(k).start()

        return carry

    w_load(0, 0).start()
    w_load(0, 1).start()
    x_local.wait()
    x_put.start()
    lax.fori_loop(0, NY + TAKE, phase1, 0)
    w_load(1, 0).start()
    w_load(1, 1).start()
    zt_out = pltpu.make_async_copy(ugv.at[pl.ds(0, ff), :], zt_ref, ol.at[0])
    zt_out.start()
    def gates(i, carry):
        rows = pl.ds(pl.multiple_of(i * 128, 128), 128)
        g = gv[rows, :]
        duv[rows, :fp] = (g * utv[rows, :].astype(F32) * spv[rows, :]).astype(BF16)
        duv[rows, fp:] = (g * av[rows, :]).astype(BF16)
        return carry

    lax.fori_loop(0, tall // 128, gates, 0)

    for n in range(7):
        left(dyv.at[0, 0], ys.at[n])
    pltpu.make_async_copy(dyv, dya_ref, dl.at[0]).wait()
    zt_out.wait()
    for k in range(DOWN - 2, DOWN):
        down_out(k).wait()

    def rs0(k, c):
        return rcopy(dyv.at[:, c, :, cols(k)], r0v.at[k], rs.at[0], rr.at[k], pn)

    def rs1(k):
        return rcopy(blk(dyv, dg, k), r1v.at[k], rs.at[1], r1r.at[k], n1(k))

    def sums_out(k, diagonal):
        outs = [(so_ref, t, k), (sx_ref, xn, k), (sy_ref, yn, k)] + ([(sd_ref, dg, k - HOPS)] if diagonal else [])
        return [pltpu.make_async_copy(blk(dyv, owner, k), ref.at[:, cols(c)], po.at[i])
                for i, (ref, owner, c) in enumerate(outs)]

    def add(owner, k, other):
        b = blk(dyv, owner, k)
        b[...] = (b[...].astype(F32) + other.astype(F32)).astype(BF16)

    def t_block(b):
        src = pl.multiple_of(jnp.minimum(b, blocks - 1) * 128, 128)
        rows = pl.ds(pl.multiple_of(jnp.minimum(b, blocks) * 128, 128), 128)
        ugv[rows, :] = duv[:, pl.ds(src, 128)].T
        uuv[rows, :] = duv[:, pl.ds(fp + src, 128)].T

    blocks = fp // 128
    per = -(-blocks // NH)

    outs = [pltpu.make_async_copy(v.at[pl.ds(0, ff), :], ref, ol.at[i])
            for i, (v, ref) in enumerate(((ugv, dgt_ref), (uuv, dut_ref)))]

    def hop_end(k):
        rs1(k).wait_recv()
        add(n2(k), k, r1v[k])
        for o in sums_out(k, False):
            o.start()

    def phase2(i, carry):
        for first, ks in ((NH - 1, range(0, 3)),):
            @pl.when(i == first)
            def _():
                for k in ks:
                    ag_last(xa_ref, xs, xr, k)

        @pl.when(i < NH - 1)
        def _():
            ag_mid(xa_ref, xs, xr, i + 1)

        @pl.when(i < NH)
        def _():
            w_load(i, 0).wait()
            w_load(i, 1).wait()
            slot = (i + 1) % 2
            for b in range(per):
                t_block(per * i + b)
            p = jnp.dot(duv[...], wbuf[slot], preferred_element_type=F32)
            dyv[:, :, :, cols(i)] = p.astype(BF16).reshape(4, 2, tok, hc)

            @pl.when(i + 2 < NH)
            def _():
                w_load(i + 2, 0).start()
                w_load(i + 2, 1).start()

        @pl.when(i == -(-blocks // per))
        def _():
            for o in outs:
                o.start()

        @pl.when(i < NH)
        def _():
            rs0(i, 1 - tc).start()

        @pl.when((i >= 1) & (i <= NH))
        def _():
            k = i - 1
            rs0(k, tc).wait_recv()
            for q in range(4):
                add(2 * q + tc, k, r0v[k, q])

            @pl.when(k < HOPS)
            def _():
                rs1(k).start()

            @pl.when(k >= HOPS)
            def _():
                for o in sums_out(k, True):
                    o.start()

        @pl.when((i >= 5) & (i < 5 + HOPS))
        def _():
            hop_end(i - 5)

        return carry

    ag_mid(xa_ref, xs, xr, 0)
    lax.fori_loop(0, NH + 1, phase2, 0)
    for k in range(NH - 4, HOPS):
        hop_end(k)
    for k in range(3, NH):
        ag_last(xa_ref, xs, xr, k)

    def drain(k, carry):
        ag_end(xa_ref, xs, xr, k)
        return carry

    lax.fori_loop(0, NH, drain, 0)
    for n in range(7):
        left(xa_ref.at[0, 0], xs.at[n])
    left(dyv.at[:, 0], rs.at[0])
    left(dyv.at[0, 0, :, pl.ds(0, HOPS * hc)], rs.at[1])
    x_put.wait()
    for n, ref in enumerate((so_ref, sx_ref, sy_ref, sd_ref)):
        pltpu.make_async_copy(ref, ref, po.at[n]).wait()
    for o in outs:
        o.wait()


def _row_chunks(ff):
    n = ff // 16
    size = -(-n // 4)
    return [16 * min(size, n - i) for i in range(0, n, size)]


def _weight_kernel(zt_ref, dgt_ref, dut_ref, dy_ref, x_ref, part_ref, dd_ref, dg_ref, du_ref,
                   zv, dgv, duv, yv, xv, o0, o1, o2, cv, ls, ysem, xsem, os, ci, co):
    ff, tall = zt_ref.shape
    hid = dy_ref.shape[1]
    nb = yv.shape[-1]
    n = hid // nb
    sizes = _row_chunks(ff)
    depth = tall // 256

    def load(src, dst, sem, j, p):
        lo = pl.ds(pl.multiple_of(j * nb + p * 512, 512), 512)
        return pltpu.make_async_copy(src.at[:, lo], dst.at[j % 2, :, p * 512:p * 512 + 512], sem.at[j % 2, p])

    def y_loads(j):
        return [load(dy_ref, yv, ysem, j, p) for p in range(nb // 512)]

    def x_loads(j):
        return [load(x_ref, xv, xsem, j, p) for p in range(nb // 512)]

    def put(i, j, rows, width, p):
        stage, out = ((o0, dd_ref), (o1, dg_ref), (o2, du_ref))[i]
        lo = pl.ds(pl.multiple_of(j * nb + p * 512, 512), width)
        slot = j % stage.shape[0]
        return pltpu.make_async_copy(stage.at[slot, rows, p * 512:p * 512 + width], out.at[rows, lo], os.at[i, slot])

    def put_all(i, j):
        return put(i, j, pl.ds(0, ff), nb, 0)

    def product(i, j, accs, waits):
        a = (zv, dgv, duv)[i]
        b = (yv, xv, xv)[i].at[j % 2]
        stage = (o0, o1, o2)[i]
        slot = j % stage.shape[0]
        steps = []
        for pair in range(nb // 512):
            row = 0
            for c, size in enumerate(sizes):
                for kt in range(depth):
                    steps.append((pair, c, row, size, kt))
                row += size

        def push(s):
            pair, _, _, _, kt = steps[s]
            for q in range(2):
                lo = pair * 512 + q * 256
                pltpu.matmul_push_rhs(b[kt * 256:kt * 256 + 256, lo:lo + 256], s % 2, q)

        def pop(pair, c, row, size):
            for q in range(2):
                lo = pair * 512 + q * 256
                stage[slot, row:row + size, lo:lo + 256] = pltpu.matmul_pop(accs[q][c])
            put(i, j, pl.ds(row, size), 512, pair).start()

        late = None
        for s, (pair, c, row, size, kt) in enumerate(steps):
            if s == 0 or (kt == 0 and (pair, c) in waits):
                for w in waits.get((pair, c), ()):
                    w.wait()
                push(s)
            if s + 1 < len(steps) and not (steps[s + 1][4] == 0 and steps[s + 1][:2] in waits):
                push(s + 1)
            block = a[row:row + size, kt * 256:kt * 256 + 256]
            for q in range(2):
                pltpu.matmul_acc_lhs(accs[q][c], block, load_staged_rhs=s % 2)
            if kt == 0 and late is not None:
                pop(*late)
            if kt == depth - 1:
                late = (pair, c, row, size)
        pop(*late)

    def take(p):
        return pltpu.make_async_copy(part_ref.at[:, p * 512:p * 512 + 512], cv.at[p], ci.at[p])

    def give(p):
        return pltpu.make_async_copy(cv.at[p], dd_ref.at[:, p * 512:p * 512 + 512], co.at[p])

    zl, ul = (pltpu.make_async_copy(src, dst, ls.at[i]) for i, (src, dst) in enumerate(((zt_ref, zv), (dut_ref, duv))))
    gl = [pltpu.make_async_copy(dgt_ref.at[rows, :], dgv.at[rows, :], ls.at[2 + i])
          for i, rows in enumerate((pl.ds(0, sizes[0]), pl.ds(sizes[0], ff - sizes[0])))]
    parts = range(part_ref.shape[1] // 512)
    early, late = parts[:len(parts) // 2], parts[len(parts) // 2:]
    start = part_ref.shape[1] // nb
    first = x_loads(0)
    for c in (gl[0], first[0], gl[1], *first[1:], ul, *x_loads(1), zl, *y_loads(start)):
        c.start()

    def body(*flat):
        h = len(flat) // 2
        accs = [[part[2] if i == len(sizes) - 1 else part[i % 2] for i in range(len(sizes))]
                for part in (flat[:h], flat[h:])]
        product(1, 0, accs, {(0, 0): [gl[0], first[0]], (0, 1): gl[1:], (1, 0): first[1:]})
        product(2, 0, accs, {(0, 0): [ul]})
        for c in x_loads(1):
            c.wait()
        for c in x_loads(2):
            c.start()
        for p in early:
            take(p).start()
        put_all(1, 0).wait()
        product(1, 1, accs, {})
        product(2, 1, accs, {})
        zl.wait()

        def rest(j, carry):
            for c in y_loads(j) + x_loads(j):
                c.wait()

            @pl.when(j + 1 < n)
            def _():
                for c in y_loads(j + 1) + x_loads(j + 1):
                    c.start()

            @pl.when(j > start)
            def _():
                put_all(0, j - 1).wait()

            put_all(1, j - 1).wait()
            put_all(2, j - 2).wait()
            product(0, j, accs, {})

            @pl.when(j == start)
            def _():
                for p in early:
                    take(p).wait()
                    give(p).start()
                for p in late:
                    take(p).start()

            @pl.when(j == start + 1)
            def _():
                for p in late:
                    take(p).wait()
                    give(p).start()

            product(1, j, accs, {})
            product(2, j, accs, {})
            return carry

        lax.fori_loop(start, n, rest, 0)

    pl.run_scoped(body, *[pltpu.ACC(q)((size, 256), F32) for q in range(2) for size in (sizes[0], sizes[0], sizes[-1])])
    put_all(0, n - 1).wait()
    put_all(1, n - 1).wait()
    put_all(2, n - 2).wait()
    put_all(2, n - 1).wait()
    for p in parts:
        give(p).wait()


def _weight_grads(zt, dgt, dut, dy, x, part):
    ff, tall = zt.shape
    hid = x.shape[1]
    nb = 1024
    sem = pltpu.SemaphoreType.DMA
    any_ = pl.BlockSpec(memory_space=pltpu.HBM)
    return pl.pallas_call(
        _weight_kernel,
        out_shape=(jax.ShapeDtypeStruct((ff, hid), F32),) * 3,
        in_specs=[any_] * 6,
        out_specs=(any_,) * 3,
        scratch_shapes=[pltpu.VMEM((ff, tall), BF16)] * 3 + [pltpu.VMEM((2, tall, nb), BF16)] * 2
        + [pltpu.VMEM((k, ff, nb), F32) for k in (1, 1, 2)] + [pltpu.VMEM((DOWN, ff, 512), F32)]
        + [sem((4,)), sem((2, 2)), sem((2, 2)), sem((3, 2)), sem((DOWN,)), sem((DOWN,))],
        compiler_params=pltpu.CompilerParams(vmem_limit_bytes=54 * 2 ** 20),
        cost_estimate=pl.CostEstimate(flops=6 * ff * tall * hid, bytes_accessed=12 * ff * hid, transcendentals=0),
        name="weight_grads",
    )(zt, dgt, dut, dy, x, part)


def solution(mesh):
    def local_backward(x, wg, wu, wd, ug, uu, dy):
        tok, hid = dy.shape
        ff = wd.shape[0]
        fp = _lanes(ff)
        tall = 8 * tok
        hc = hid // NH
        any_ = pl.BlockSpec(memory_space=pl.ANY)
        sem = pltpu.SemaphoreType.DMA
        full = jax.ShapeDtypeStruct((4, 2, tok, hid), BF16)
        act = jax.ShapeDtypeStruct((ff, tall), BF16)
        own = jax.ShapeDtypeStruct((tok, hid), BF16)
        rest = jax.ShapeDtypeStruct((tok, hid - HOPS * hc), BF16)
        so, sx, sy, sd, zt, dgt, dut, dya, xa, ddp = pl.pallas_call(
            _comm_kernel,
            out_shape=(own, own, own, rest, act, act, act, full, full,
                       jax.ShapeDtypeStruct((ff, DOWN * hc), F32)),
            in_specs=[any_] * 7,
            out_specs=(any_,) * 10,
            scratch_shapes=[
                pltpu.VMEM((4, 2, tok, hid), BF16),
                pltpu.VMEM((tall, fp), F32),
                pltpu.VMEM((tall, fp), F32),
                pltpu.VMEM((tall, fp), F32),
                pltpu.VMEM((tall, fp), BF16),
                pltpu.VMEM((tall, 2 * fp), BF16),
                pltpu.VMEM((2, 2 * fp, hc), BF16),
                pltpu.VMEM((fp + 128, tall), BF16),
                pltpu.VMEM((fp + 128, tall), BF16),
                pltpu.VMEM((NH, 4, tok, hc), BF16),
                pltpu.VMEM((HOPS, tok, hc), BF16),
                pltpu.VMEM((tok, hid), BF16),
                pltpu.VMEM((2, ff, hc), F32),
                sem((7,)), sem((NY, 3)), sem((7,)), sem((NH, 3)), sem((2,)), sem((NH,)), sem((HOPS,)),
                sem((NY // AHEAD,)), sem((2,)), sem((2, 2)), sem((2,)), sem((2,)), sem((1,)), sem((4,)), sem((2,)),
            ],
            compiler_params=pltpu.CompilerParams(collective_id=0, has_side_effects=True, vmem_limit_bytes=67043328),
            name="gather_partial",
        )(x, dy, wd, wg.T, wu.T, ug.T, uu.T)
        dya = dya.reshape(tall, hid)
        xa = xa.reshape(tall, hid)

        def to(v, flip):
            return lax.ppermute(v, 'tp', [(i, i ^ flip) for i in range(8)])

        fx, fy, fd = to(sx, 2), to(sy, 4), to(sd, 6)
        zt, dgt, dut, ddp = (pltpu.with_memory_space_constraint(v, pltpu.HBM) for v in (zt, dgt, dut, ddp))
        dwd, dwg, dwu = _weight_grads(zt, dgt, dut, dya, xa, ddp)
        fx, fy, fd, dwd, dwg, dwu = lax.optimization_barrier((fx, fy, fd, dwd, dwg, dwu))
        right = jnp.pad(fd, ((0, 0), (HOPS * hc, 0)))
        dx = sum(v.astype(F32) for v in (so, fx, fy, right)).astype(BF16)
        return dx, dwg.T, dwu.T, dwd

    tok_spec = P(('dp', 'tp'), None)
    col_spec = P(None, 'tp')
    act_spec = P('dp', 'tp')
    return jax.shard_map(local_backward, mesh=mesh,
                         in_specs=(tok_spec, col_spec, col_spec, P('tp', None), act_spec, act_spec, tok_spec),
                         out_specs=(tok_spec, act_spec, act_spec, tok_spec),
                         check_vma=False)
```

```python
import functools

import jax
import jax.numpy as jnp
from jax import lax
from jax.experimental import pallas as pl
from jax.experimental.pallas import tpu as pltpu
from jax.sharding import PartitionSpec as P

MESH = pl.DeviceIdType.MESH
BF16 = jnp.bfloat16
F32 = jnp.float32
NH = 8
HOPS = 4
DOWN = 2
NY = 16
AHEAD, LAG, TAKE = 4, 4, 6
NT = (((1,), (1,)), ((), ()))


def _lanes(n):
    return (n + 127) // 128 * 128


def _comm_kernel(x_ref, dy_ref, wd_ref, wg_ref, wu_ref, ug_ref, uu_ref,
                 so_ref, sx_ref, sy_ref, sd_ref, zt_ref, dgt_ref, dut_ref, dya_ref, xa_ref, dd_ref,
                 dyv, gv, av, spv, utv, duv, wbuf, ugv, uuv, r0v, r1v, xov, ddv,
                 ys, yr, xs, xr, rs, rr, r1r, yl, xl, wl, ul, ol, dl, po, pd):
    tok, hid = dy_ref.shape
    ff = wd_ref.shape[0]
    fp = _lanes(ff)
    nfull, rest = ff // 128, ff % 128
    hc = hid // NH
    tall = 8 * tok

    t = lax.axis_index("tp")
    ty, tx, tc = t // 4, (t // 2) % 2, t % 2
    xn = t + 2 - 4 * tx
    yn = t + 4 - 8 * ty
    dg = xn + yn - t
    pn = t + 1 - 2 * tc

    def n1(k):
        return xn + (yn - xn) * (k % 2)

    def n2(k):
        return yn + (xn - yn) * (k % 2)

    hy = hid // NY
    per_h = NY // NH

    def cols(k, w=hc):
        return pl.ds(pl.multiple_of(k * w, w), w)

    def blk(ref, owner, k, w=hc):
        return ref.at[owner // 2, owner % 2, :, cols(k, w)]

    def rcopy(src, dst, ss, rs_, dev):
        return pltpu.make_async_remote_copy(src_ref=src, dst_ref=dst, send_sem=ss, recv_sem=rs_,
                                            device_id={"tp": dev}, device_id_type=MESH)

    def ag(buf, ss, sr, k, j, owner, dev):
        w = hid // sr.shape[0]
        return rcopy(blk(buf, owner, k, w), blk(buf, owner, k, w), ss.at[j], sr.at[k, (0, 1, 1, 2, 2, 2, 2)[j]], dev)

    def arrived(ref, sem):
        rcopy(ref, ref, sem, sem, t).wait_recv()

    def left(ref, sem):
        rcopy(ref, ref, sem, sem, t).wait_send()

    def ag_own(buf, ss, sr, k):
        ag(buf, ss, sr, k, 0, t, n1(k)).start()
        ag(buf, ss, sr, k, 1, t, n2(k)).start()
        ag(buf, ss, sr, k, 3, t, pn).start()

    def x_own(k, j, dev):
        return rcopy(xov.at[:, cols(k)], blk(xa_ref, t, k), xs.at[j], xr.at[k, (0, 1, 1, 2)[j]], dev)

    def x_send(k):
        x_own(k, 0, n1(k)).start()
        x_own(k, 1, n2(k)).start()
        x_own(k, 3, pn).start()

    def ag_mid(buf, ss, sr, k):
        ag(buf, ss, sr, k, 0, n1(k), n1(k)).wait_recv()
        ag(buf, ss, sr, k, 2, n1(k), n2(k)).start()
        ag(buf, ss, sr, k, 4, n1(k), pn).start()

    def ag_last(buf, ss, sr, k):
        w = hid // sr.shape[0]
        arrived(buf.at[pl.ds(0, 2), 0, :, cols(k, w)], sr.at[k, 1])
        ag(buf, ss, sr, k, 5, n2(k), pn).start()
        ag(buf, ss, sr, k, 6, dg, pn).start()

    def ag_end(buf, ss, sr, k):
        w = hid // sr.shape[0]
        arrived(buf.at[:, 0, :, cols(k, w)], sr.at[k, 2])

    def y_local(g):
        w = AHEAD * hy
        return pltpu.make_async_copy(dy_ref.at[:, cols(g, w)], blk(dyv, t, g, w), yl.at[g])

    x_local = pltpu.make_async_copy(x_ref, xov, xl.at[0])
    x_put = pltpu.make_async_copy(xov, xa_ref.at[t // 2, t % 2], xl.at[1])

    def down_out(k):
        return pltpu.make_async_copy(ddv.at[k % 2], dd_ref.at[:, cols(k)], pd.at[k % 2])

    def wd_load(k):
        return pltpu.make_async_copy(wd_ref.at[:, cols(k)], wbuf.at[0, pl.ds(pl.multiple_of(k % 2 * fp, fp), ff), :], wl.at[0, k % 2])

    def w_load(k, j):
        src = (wg_ref, wu_ref)[j]
        return pltpu.make_async_copy(src.at[:, cols(k)], wbuf.at[(k + 1) % 2, pl.ds(j * fp, ff), :],
                                     wl.at[(k + 1) % 2, j])

    def dy_out(k):
        return pltpu.make_async_copy(dyv.at[:, :, :, cols(k)], dya_ref.at[:, :, :, cols(k)], dl.at[0])

    ug_in = pltpu.make_async_copy(ug_ref, ugv.at[pl.ds(0, ff), :], ul.at[0])
    uu_in = pltpu.make_async_copy(uu_ref, uuv.at[pl.ds(0, ff), :], ul.at[1])
    for g in range(NY // AHEAD):
        y_local(g).start()
    wd_load(0).start()
    wd_load(1).start()
    ug_in.start()
    uu_in.start()
    x_local.start()

    barrier = pltpu.get_barrier_semaphore()
    for dev in (xn, yn, pn):
        pl.semaphore_signal(barrier, inc=1, device_id={"tp": dev}, device_id_type=MESH)
    pl.semaphore_wait(barrier, 3)

    y_local(0).wait()
    for k in range(AHEAD):
        ag_own(dyv, ys, yr, k)

    for a in range(2):
        for b in range(2):
            wbuf[a, b * fp + ff:b * fp + fp, :] = jnp.zeros((fp - ff, hc), BF16)
    gv[...] = jnp.zeros_like(gv)
    ug_in.wait()
    uu_in.wait()

    def u_block(r0, n):
        rows = pl.ds(r0, n)
        ug = ugv[rows, :].astype(F32)
        ub = uuv[rows, :]
        uu = ub.astype(F32)
        s = jax.nn.sigmoid(ug)
        a = ug * s
        sp = s * (1.0 + ug * (1.0 - s))
        ugv[rows, :] = (a * uu).astype(BF16)
        if n < 128:
            pad = jnp.zeros((128 - n, tall), F32)
            a = jnp.concatenate([a, pad], axis=0)
            sp = jnp.concatenate([sp, pad], axis=0)
            uu = jnp.concatenate([uu, pad], axis=0)
        lanes = pl.ds(r0, 128)
        av[:, lanes] = a.T
        spv[:, lanes] = sp.T
        utv[:, lanes] = uu.T.astype(BF16)

    down0 = fp // 128

    def phase1(i, carry):
        @pl.when((i < NY - AHEAD) & (i % AHEAD == 0))
        def _():
            y_local(i // AHEAD + 1).wait()

        @pl.when(i < NY - AHEAD)
        def _():
            ag_own(dyv, ys, yr, i + AHEAD)

        @pl.when(i < NY)
        def _():
            ag_mid(dyv, ys, yr, i)

        @pl.when(i >= NY + TAKE - NH)
        def _():
            x_send(i - (NY + TAKE - NH))

        @pl.when(i < nfull)
        def _():
            u_block(pl.multiple_of(i * 128, 128), 128)

        if rest:
            @pl.when(i == nfull)
            def _():
                u_block(nfull * 128, rest)

        @pl.when((i >= LAG) & (i < NY + LAG))
        def _():
            ag_last(dyv, ys, yr, i - LAG)

        @pl.when(i >= TAKE)
        def _():
            ag_end(dyv, ys, yr, i - TAKE)

        @pl.when((i >= TAKE) & ((i - TAKE) % per_h == per_h - 1))
        def _():
            k = (i - TAKE) // per_h
            dy_out(k).start()
            wd_load(k).wait()
            dyc = dyv[:, :, :, cols(k)].reshape(tall, hc)
            for n in range(0, fp, 256):
                w = min(256, fp - n)
                gv[:, n:n + w] += lax.dot_general(dyc, wbuf[0, pl.ds(pl.multiple_of(k % 2 * fp + n, 128), w), :], NT, preferred_element_type=F32)

            @pl.when(k + 2 < NH)
            def _():
                wd_load(k + 2).start()

        @pl.when((i >= down0) & (i < down0 + DOWN))
        def _():
            k = i - down0

            @pl.when(k >= 2)
            def _():
                down_out(k - 2).wait()

            dyc = dyv[:, :, :, cols(k)].reshape(tall, hc)
            ddv[k % 2] = jnp.dot(ugv[:ff, :], dyc, preferred_element_type=F32)
            down_out(k).start()

        return carry

    w_load(0, 0).start()
    w_load(0, 1).start()
    x_local.wait()
    x_put.start()
    lax.fori_loop(0, NY + TAKE, phase1, 0)
    w_load(1, 0).start()
    w_load(1, 1).start()
    zt_out = pltpu.make_async_copy(ugv.at[pl.ds(0, ff), :], zt_ref, ol.at[0])
    zt_out.start()
    def gates(i, carry):
        rows = pl.ds(pl.multiple_of(i * 128, 128), 128)
        g = gv[rows, :]
        duv[rows, :fp] = (g * utv[rows, :].astype(F32) * spv[rows, :]).astype(BF16)
        duv[rows, fp:] = (g * av[rows, :]).astype(BF16)
        return carry

    lax.fori_loop(0, tall // 128, gates, 0)

    for n in range(7):
        left(dyv.at[0, 0], ys.at[n])
    pltpu.make_async_copy(dyv, dya_ref, dl.at[0]).wait()
    zt_out.wait()
    for k in range(DOWN - 2, DOWN):
        down_out(k).wait()

    def rs0(k, c):
        return rcopy(dyv.at[:, c, :, cols(k)], r0v.at[k], rs.at[0], rr.at[k], pn)

    def rs1(k):
        return rcopy(blk(dyv, dg, k), r1v.at[k], rs.at[1], r1r.at[k], n1(k))

    def sums_out(k, diagonal):
        outs = [(so_ref, t, k), (sx_ref, xn, k), (sy_ref, yn, k)] + ([(sd_ref, dg, k - HOPS)] if diagonal else [])
        return [pltpu.make_async_copy(blk(dyv, owner, k), ref.at[:, cols(c)], po.at[i])
                for i, (ref, owner, c) in enumerate(outs)]

    def add(owner, k, other):
        b = blk(dyv, owner, k)
        b[...] = (b[...].astype(F32) + other.astype(F32)).astype(BF16)

    def t_block(b):
        src = pl.multiple_of(jnp.minimum(b, blocks - 1) * 128, 128)
        rows = pl.ds(pl.multiple_of(jnp.minimum(b, blocks) * 128, 128), 128)
        ugv[rows, :] = duv[:, pl.ds(src, 128)].T
        uuv[rows, :] = duv[:, pl.ds(fp + src, 128)].T

    blocks = fp // 128
    per = -(-blocks // NH)

    outs = [pltpu.make_async_copy(v.at[pl.ds(0, ff), :], ref, ol.at[i])
            for i, (v, ref) in enumerate(((ugv, dgt_ref), (uuv, dut_ref)))]

    def phase2(i, carry):
        for first, ks in ((NH - 1, range(0, 3)),):
            @pl.when(i == first)
            def _():
                for k in ks:
                    ag_last(xa_ref, xs, xr, k)

        @pl.when(i < NH - 1)
        def _():
            ag_mid(xa_ref, xs, xr, i + 1)

        @pl.when(i < NH)
        def _():
            w_load(i, 0).wait()
            w_load(i, 1).wait()
            slot = (i + 1) % 2
            for b in range(per):
                t_block(per * i + b)
            p = jnp.dot(duv[...], wbuf[slot], preferred_element_type=F32)
            dyv[:, :, :, cols(i)] = p.astype(BF16).reshape(4, 2, tok, hc)

            @pl.when(i + 2 < NH)
            def _():
                w_load(i + 2, 0).start()
                w_load(i + 2, 1).start()

        @pl.when(i == -(-blocks // per))
        def _():
            for o in outs:
                o.start()

        @pl.when(i < NH)
        def _():
            rs0(i, 1 - tc).start()

        @pl.when((i >= 1) & (i <= NH))
        def _():
            k = i - 1
            rs0(k, tc).wait_recv()
            for q in range(4):
                add(2 * q + tc, k, r0v[k, q])

            @pl.when(k < HOPS)
            def _():
                rs1(k).start()

            @pl.when(k >= HOPS)
            def _():
                for o in sums_out(k, True):
                    o.start()

        @pl.when((i >= 5) & (i < 5 + HOPS))
        def _():
            k = i - 5
            rs1(k).wait_recv()
            add(n2(k), k, r1v[k])
            for o in sums_out(k, False):
                o.start()

        return carry

    ag_mid(xa_ref, xs, xr, 0)
    lax.fori_loop(0, NH + 1, phase2, 0)
    for k in range(3, NH):
        ag_last(xa_ref, xs, xr, k)

    def drain(k, carry):
        ag_end(xa_ref, xs, xr, k)
        return carry

    lax.fori_loop(0, NH, drain, 0)
    for n in range(7):
        left(xa_ref.at[0, 0], xs.at[n])
    left(dyv.at[:, 0], rs.at[0])
    left(dyv.at[0, 0, :, pl.ds(0, HOPS * hc)], rs.at[1])
    x_put.wait()
    for n, ref in enumerate((so_ref, sx_ref, sy_ref, sd_ref)):
        pltpu.make_async_copy(ref, ref, po.at[n]).wait()
    for o in outs:
        o.wait()


def _row_chunks(ff):
    n = ff // 16
    size = -(-n // 4)
    return [16 * min(size, n - i) for i in range(0, n, size)]


def _weight_kernel(zt_ref, dgt_ref, dut_ref, dy_ref, x_ref, part_ref, dd_ref, dg_ref, du_ref,
                   zv, dgv, duv, yv, xv, o0, o1, o2, cv, ls, ysem, xsem, os, ci, co):
    ff, tall = zt_ref.shape
    hid = dy_ref.shape[1]
    nb = yv.shape[-1]
    n = hid // nb
    sizes = _row_chunks(ff)
    depth = tall // 256

    def load(src, dst, sem, j, p):
        lo = pl.ds(pl.multiple_of(j * nb + p * 512, 512), 512)
        return pltpu.make_async_copy(src.at[:, lo], dst.at[j % 2, :, p * 512:p * 512 + 512], sem.at[j % 2, p])

    def y_loads(j):
        return [load(dy_ref, yv, ysem, j, p) for p in range(nb // 512)]

    def x_loads(j):
        return [load(x_ref, xv, xsem, j, p) for p in range(nb // 512)]

    def put(i, j, rows, width, p):
        stage, out = ((o0, dd_ref), (o1, dg_ref), (o2, du_ref))[i]
        lo = pl.ds(pl.multiple_of(j * nb + p * 512, 512), width)
        slot = j % stage.shape[0]
        return pltpu.make_async_copy(stage.at[slot, rows, p * 512:p * 512 + width], out.at[rows, lo], os.at[i, slot])

    def put_all(i, j):
        return put(i, j, pl.ds(0, ff), nb, 0)

    def product(i, j, accs, waits):
        a = (zv, dgv, duv)[i]
        b = (yv, xv, xv)[i].at[j % 2]
        stage = (o0, o1, o2)[i]
        slot = j % stage.shape[0]
        steps = []
        for pair in range(nb // 512):
            row = 0
            for c, size in enumerate(sizes):
                for kt in range(depth):
                    steps.append((pair, c, row, size, kt))
                row += size

        def push(s):
            pair, _, _, _, kt = steps[s]
            for q in range(2):
                lo = pair * 512 + q * 256
                pltpu.matmul_push_rhs(b[kt * 256:kt * 256 + 256, lo:lo + 256], s % 2, q)

        def pop(pair, c, row, size):
            for q in range(2):
                lo = pair * 512 + q * 256
                stage[slot, row:row + size, lo:lo + 256] = pltpu.matmul_pop(accs[q][c])
            put(i, j, pl.ds(row, size), 512, pair).start()

        late = None
        for s, (pair, c, row, size, kt) in enumerate(steps):
            if s == 0 or (kt == 0 and (pair, c) in waits):
                for w in waits.get((pair, c), ()):
                    w.wait()
                push(s)
            if s + 1 < len(steps) and not (steps[s + 1][4] == 0 and steps[s + 1][:2] in waits):
                push(s + 1)
            block = a[row:row + size, kt * 256:kt * 256 + 256]
            for q in range(2):
                pltpu.matmul_acc_lhs(accs[q][c], block, load_staged_rhs=s % 2)
            if kt == 0 and late is not None:
                pop(*late)
            if kt == depth - 1:
                late = (pair, c, row, size)
        pop(*late)

    def take(p):
        return pltpu.make_async_copy(part_ref.at[:, p * 512:p * 512 + 512], cv.at[p], ci.at[p])

    def give(p):
        return pltpu.make_async_copy(cv.at[p], dd_ref.at[:, p * 512:p * 512 + 512], co.at[p])

    zl, ul = (pltpu.make_async_copy(src, dst, ls.at[i]) for i, (src, dst) in enumerate(((zt_ref, zv), (dut_ref, duv))))
    gl = [pltpu.make_async_copy(dgt_ref.at[rows, :], dgv.at[rows, :], ls.at[2 + i])
          for i, rows in enumerate((pl.ds(0, sizes[0]), pl.ds(sizes[0], ff - sizes[0])))]
    parts = range(nb // 512)
    first = x_loads(0)
    for c in (gl[0], first[0], gl[1], *first[1:], ul):
        c.start()
    zl.start()
    for c in y_loads(1) + x_loads(1):
        c.start()

    def body(*flat):
        h = len(flat) // 2
        accs = [[part[2] if i == len(sizes) - 1 else part[i % 2] for i in range(len(sizes))]
                for part in (flat[:h], flat[h:])]
        product(1, 0, accs, {(0, 0): [*gl, first[0]], (1, 0): first[1:]})
        product(2, 0, accs, {(0, 0): [ul]})
        zl.wait()

        def rest(j, carry):
            for c in y_loads(j) + x_loads(j):
                c.wait()

            @pl.when(j + 1 < n)
            def _():
                for c in y_loads(j + 1) + x_loads(j + 1):
                    c.start()

            @pl.when(j == 1)
            def _():
                for p in parts:
                    take(p).start()

            @pl.when(j == 2)
            def _():
                for p in parts:
                    take(p).wait()
                    give(p).start()

            @pl.when(j >= 2)
            def _():
                put_all(0, j - 1).wait()
                put_all(2, j - 2).wait()

            put_all(1, j - 1).wait()
            for i in range(3):
                product(i, j, accs, {})
            return carry

        lax.fori_loop(1, n, rest, 0)

    pl.run_scoped(body, *[pltpu.ACC(q)((size, 256), F32) for q in range(2) for size in (sizes[0], sizes[0], sizes[-1])])
    put_all(0, n - 1).wait()
    put_all(1, n - 1).wait()
    put_all(2, n - 2).wait()
    put_all(2, n - 1).wait()
    for p in parts:
        give(p).wait()


def _weight_grads(zt, dgt, dut, dy, x, part):
    ff, tall = zt.shape
    hid = x.shape[1]
    nb = 1024
    sem = pltpu.SemaphoreType.DMA
    any_ = pl.BlockSpec(memory_space=pltpu.HBM)
    return pl.pallas_call(
        _weight_kernel,
        out_shape=(jax.ShapeDtypeStruct((ff, hid), F32),) * 3,
        in_specs=[any_] * 6,
        out_specs=(any_,) * 3,
        scratch_shapes=[pltpu.VMEM((ff, tall), BF16)] * 3 + [pltpu.VMEM((2, tall, nb), BF16)] * 2
        + [pltpu.VMEM((k, ff, nb), F32) for k in (1, 1, 2)] + [pltpu.VMEM((nb // 512, ff, 512), F32)]
        + [sem((4,)), sem((2, 2)), sem((2, 2)), sem((3, 2)), sem((2,)), sem((2,))],
        compiler_params=pltpu.CompilerParams(vmem_limit_bytes=54 * 2 ** 20),
        cost_estimate=pl.CostEstimate(flops=6 * ff * tall * hid, bytes_accessed=12 * ff * hid, transcendentals=0),
        name="weight_grads",
    )(zt, dgt, dut, dy, x, part)


def solution(mesh):
    def local_backward(x, wg, wu, wd, ug, uu, dy):
        tok, hid = dy.shape
        ff = wd.shape[0]
        fp = _lanes(ff)
        tall = 8 * tok
        hc = hid // NH
        any_ = pl.BlockSpec(memory_space=pl.ANY)
        sem = pltpu.SemaphoreType.DMA
        full = jax.ShapeDtypeStruct((4, 2, tok, hid), BF16)
        act = jax.ShapeDtypeStruct((ff, tall), BF16)
        own = jax.ShapeDtypeStruct((tok, hid), BF16)
        rest = jax.ShapeDtypeStruct((tok, hid - HOPS * hc), BF16)
        so, sx, sy, sd, zt, dgt, dut, dya, xa, ddp = pl.pallas_call(
            _comm_kernel,
            out_shape=(own, own, own, rest, act, act, act, full, full,
                       jax.ShapeDtypeStruct((ff, DOWN * hc), F32)),
            in_specs=[any_] * 7,
            out_specs=(any_,) * 10,
            scratch_shapes=[
                pltpu.VMEM((4, 2, tok, hid), BF16),
                pltpu.VMEM((tall, fp), F32),
                pltpu.VMEM((tall, fp), F32),
                pltpu.VMEM((tall, fp), F32),
                pltpu.VMEM((tall, fp), BF16),
                pltpu.VMEM((tall, 2 * fp), BF16),
                pltpu.VMEM((2, 2 * fp, hc), BF16),
                pltpu.VMEM((fp + 128, tall), BF16),
                pltpu.VMEM((fp + 128, tall), BF16),
                pltpu.VMEM((NH, 4, tok, hc), BF16),
                pltpu.VMEM((HOPS, tok, hc), BF16),
                pltpu.VMEM((tok, hid), BF16),
                pltpu.VMEM((2, ff, hc), F32),
                sem((7,)), sem((NY, 3)), sem((7,)), sem((NH, 3)), sem((2,)), sem((NH,)), sem((HOPS,)),
                sem((NY // AHEAD,)), sem((2,)), sem((2, 2)), sem((2,)), sem((2,)), sem((1,)), sem((4,)), sem((2,)),
            ],
            compiler_params=pltpu.CompilerParams(collective_id=0, has_side_effects=True, vmem_limit_bytes=67043328),
            name="gather_partial",
        )(x, dy, wd, wg.T, wu.T, ug.T, uu.T)
        dya = dya.reshape(tall, hid)
        xa = xa.reshape(tall, hid)

        def to(v, flip):
            return lax.ppermute(v, 'tp', [(i, i ^ flip) for i in range(8)])

        fx, fy, fd = to(sx, 2), to(sy, 4), to(sd, 6)
        zt, dgt, dut, ddp = (pltpu.with_memory_space_constraint(v, pltpu.HBM) for v in (zt, dgt, dut, ddp))
        dwd, dwg, dwu = _weight_grads(zt, dgt, dut, dya, xa, ddp)
        fx, fy, fd, dwd, dwg, dwu = lax.optimization_barrier((fx, fy, fd, dwd, dwg, dwu))
        right = jnp.pad(fd, ((0, 0), (HOPS * hc, 0)))
        dx = sum(v.astype(F32) for v in (so, fx, fy, right)).astype(BF16)
        return dx, dwg.T, dwu.T, dwd

    tok_spec = P(('dp', 'tp'), None)
    col_spec = P(None, 'tp')
    act_spec = P('dp', 'tp')
    return jax.shard_map(local_backward, mesh=mesh,
                         in_specs=(tok_spec, col_spec, col_spec, P('tp', None), act_spec, act_spec, tok_spec),
                         out_specs=(tok_spec, act_spec, act_spec, tok_spec),
                         check_vma=False)
```
